32 devices in a mesh: ep: 32 (over z, y, x, core).
Axes of the slice: x: 2, y: 2, z: 4, core: 2. Of those that a mesh axis runs over, the one named last changes fastest.
Arguments:
- table_in: float32 [131072, 500], P('ep')
- table_out: float32 [131072, 500], P('ep')
- centers: int32 [32768], P('ep')
- contexts: int32 [32768], P('ep')
- negatives: int32 [32768, 15], P('ep')
Outputs:
- output 1: float32 [], replicated
- output 2: float32 [131072, 500], P('ep')
- output 3: float32 [131072, 500], P('ep')
All inputs are finite; a program needn't handle non-finite values.
Results may differ from the reference program's by a relative error of at most 0.001.
Values sent between devices are 32-bit elements.
A program may use at most 1 GiB of HBM per device.

```python
import math
import jax
import jax.numpy as jnp
from jax import lax

GROUP = 32
ROWS_DEV = 4096
PAIRS_DEV = 1024
DIM = 500
NEG = 15

VOCAB = GROUP * ROWS_DEV
N_PAIRS = GROUP * PAIRS_DEV
N_LOOK = PAIRS_DEV * (NEG + 2)
SHARE = N_LOOK // GROUP
PAIR_BLOCK = min(PAIRS_DEV, 1024)
ROOT_ROWS = math.isqrt(ROWS_DEV)
LEARN_RATE = 0.5


def draw_words(dev_key):
    key_extra, key_top, key_perm, key_root, key_rest = jax.random.split(dev_key, 5)
    slot_ids = jnp.arange(GROUP)
    extra_count = jax.random.randint(key_extra, (GROUP,), 0, SHARE // 2 + 1, dtype=jnp.int32)
    top_owner = jax.random.randint(key_top, (), 0, GROUP, dtype=jnp.int32)
    extra_count = jnp.where(slot_ids == top_owner, SHARE // 2, extra_count)
    extra_count = jnp.where(slot_ids == (top_owner + 1) % GROUP, 0, extra_count)
    owner_count = SHARE + extra_count - jnp.roll(extra_count, -1)
    owner_bounds = jnp.cumsum(owner_count)
    owners = jnp.searchsorted(owner_bounds, jnp.arange(N_LOOK), side='right')
    owners = jax.random.permutation(key_perm, owners.astype(jnp.int32))
    root_part = jax.random.randint(key_root, (N_LOOK,), 0, ROOT_ROWS, dtype=jnp.int32)
    local_row = root_part * root_part + jax.random.randint(key_rest, (N_LOOK,), 0, 2 * root_part + 1, dtype=jnp.int32)
    word_ids = (owners + GROUP * local_row).astype(jnp.int32)
    return word_ids[:PAIRS_DEV], word_ids[PAIRS_DEV:2 * PAIRS_DEV], word_ids[2 * PAIRS_DEV:].reshape(PAIRS_DEV, NEG)


def setup_inputs(seed: int = 0) -> dict:
    seed_key = jax.random.key(seed)
    key_in, key_out, key_words = jax.random.split(seed_key, 3)
    unit_scale = DIM ** -0.25
    table_in = unit_scale * jax.random.normal(key_in, (VOCAB, DIM), jnp.float32)
    table_out = unit_scale * jax.random.normal(key_out, (VOCAB, DIM), jnp.float32)
    centers, contexts, negatives = jax.vmap(draw_words)(jax.random.split(key_words, GROUP))
    return {'table_in': table_in, 'table_out': table_out,
            'centers': centers.reshape(N_PAIRS), 'contexts': contexts.reshape(N_PAIRS),
            'negatives': negatives.reshape(N_PAIRS, NEG)}


def reference(table_in, table_out, centers, contexts, negatives):
    def row_of(word_ids):
        return (word_ids % GROUP) * ROWS_DEV + word_ids // GROUP

    n_blocks = N_PAIRS // PAIR_BLOCK
    blocks = (row_of(centers).reshape(n_blocks, PAIR_BLOCK),
              row_of(contexts).reshape(n_blocks, PAIR_BLOCK),
              row_of(negatives).reshape(n_blocks, PAIR_BLOCK, NEG))

    def block_step(acc_state, pair_block):
        grad_in, grad_out, loss_sum = acc_state
        cen_rows, ctx_rows, neg_rows = pair_block
        u_vec = table_in[cen_rows]
        ctx_vec = table_out[ctx_rows]
        neg_vec = table_out[neg_rows]
        pos_score = jnp.sum(u_vec * ctx_vec, axis=-1)
        neg_score = jnp.sum(u_vec[:, None, :] * neg_vec, axis=-1)
        loss_sum = loss_sum - jnp.sum(jax.nn.log_sigmoid(pos_score)) - jnp.sum(jax.nn.log_sigmoid(-neg_score))
        pos_coef = jax.nn.sigmoid(pos_score) - 1.0
        neg_coef = jax.nn.sigmoid(neg_score)
        grad_u = pos_coef[:, None] * ctx_vec + jnp.sum(neg_coef[:, :, None] * neg_vec, axis=1)
        grad_in = grad_in.at[cen_rows].add(grad_u)
        grad_out = grad_out.at[ctx_rows].add(pos_coef[:, None] * u_vec)
        grad_neg = (neg_coef[:, :, None] * u_vec[:, None, :]).reshape(PAIR_BLOCK * NEG, DIM)
        grad_out = grad_out.at[neg_rows.reshape(PAIR_BLOCK * NEG)].add(grad_neg)
        return (grad_in, grad_out, loss_sum), None

    start_state = (jnp.zeros((VOCAB, DIM), jnp.float32), jnp.zeros((VOCAB, DIM), jnp.float32),
                   jnp.zeros((), jnp.float32))
    final_state, _ = lax.scan(block_step, start_state, blocks)
    grad_in, grad_out, loss_sum = final_state
    return (loss_sum / N_PAIRS, table_in - LEARN_RATE * grad_in, table_out - LEARN_RATE * grad_out)
```

```python
import functools

import jax
import jax.numpy as jnp
from jax import lax
from jax.experimental import pallas as pl
from jax.experimental.pallas import tpu as pltpu
from jax.sharding import PartitionSpec as P

LEARN_RATE = 0.5
LANES = 128
SUB = 4
TAIL = 500 - 3 * LANES
CHUNK = 512
SLOTS = 1280
BATCH = 64
ANY = pl.ANY


def load_table(table, wide, stage, sems):
    rows = table.shape[0]
    n_chunks = rows // CHUNK

    def copy(k):
        return pltpu.make_async_copy(table.at[pl.ds(k * CHUNK, CHUNK)], stage.at[k % 2], sems.at[k % 2])

    copy(0).start()
    for k in range(n_chunks):
        if k + 1 < n_chunks:
            copy(k + 1).start()
        copy(k).wait()
        buf = stage.at[k % 2]

        @pl.loop(0, CHUNK // 32)
        def _(g):
            for i in range(4):
                r8 = pl.multiple_of((g * 4 + i) * 8, 8)
                w8 = pl.multiple_of((k * CHUNK + (g * 4 + i) * 8) * SUB, 32)
                for j in range(SUB):
                    if j < SUB - 1:
                        wide[pl.ds(w8 + j, 8, stride=SUB), :] = buf[pl.ds(r8, 8), j * LANES:(j + 1) * LANES]
                    else:
                        wide[pl.ds(w8 + j, 8, stride=SUB), :] = jnp.concatenate(
                            [buf[pl.ds(r8, 8), j * LANES:j * LANES + TAIL], jnp.zeros((8, LANES - TAIL), jnp.float32)],
                            axis=1)


def store_table(out, stage, sems, value):
    rows = out.shape[0]
    n_chunks = rows // CHUNK

    def copy(k):
        return pltpu.make_async_copy(stage.at[k % 2], out.at[pl.ds(k * CHUNK, CHUNK)], sems.at[k % 2])

    for k in range(n_chunks):
        if k >= 2:
            copy(k - 2).wait()
        buf = stage.at[k % 2]

        @pl.loop(0, CHUNK // 32)
        def _(g):
            for i in range(4):
                r8 = pl.multiple_of((g * 4 + i) * 8, 8)
                w8 = pl.multiple_of((k * CHUNK + (g * 4 + i) * 8) * SUB, 32)
                for j in range(SUB):
                    piece = value(w8, j)
                    if j < SUB - 1:
                        buf[pl.ds(r8, 8), j * LANES:(j + 1) * LANES] = piece
                    else:
                        buf[pl.ds(r8, 8), j * LANES:j * LANES + TAIL] = piece[:, :TAIL]

        copy(k).start()
    copy(n_chunks - 2).wait()
    copy(n_chunks - 1).wait()


def pick_kernel(rows4, table, out, wide, stage, sems):
    load_table(table, wide, stage, sems)

    @pl.loop(0, SLOTS // 16)
    def _(g):
        for i in range(16):
            k = g * 16 + i
            r4 = pl.multiple_of(rows4[k], SUB)
            out[pl.ds(pl.multiple_of(k * SUB, SUB), SUB), :] = wide[pl.ds(r4, SUB), :]


def pick_rows(rows4, table):
    return pl.pallas_call(
        pick_kernel,
        out_shape=jax.ShapeDtypeStruct((SLOTS * SUB, LANES), jnp.float32),
        grid_spec=pltpu.PrefetchScalarGridSpec(
            num_scalar_prefetch=1, grid=(1,),
            in_specs=[pl.BlockSpec(memory_space=ANY)],
            out_specs=pl.BlockSpec((SLOTS * SUB, LANES), lambda i, *_: (0, 0)),
            scratch_shapes=[pltpu.VMEM((table.shape[0] * SUB, LANES), jnp.float32),
                            pltpu.VMEM((2, CHUNK, table.shape[1]), jnp.float32),
                            pltpu.SemaphoreType.DMA((2,))]),
        name='pick_rows')(rows4, table)


def add_kernel(rows4, table, grads, out, wide, stage, sems):
    load_table(table, wide, stage, sems)

    @pl.loop(0, SLOTS // 16)
    def _(g):
        for i in range(16):
            k = g * 16 + i
            r4 = pl.multiple_of(rows4[k], SUB)
            wide[pl.ds(r4, SUB), :] = wide[pl.ds(r4, SUB), :] - LEARN_RATE * grads[pl.ds(pl.multiple_of(k * SUB, SUB), SUB), :]

    store_table(out, stage, sems, lambda w8, j: wide[pl.ds(w8 + j, 8, stride=SUB), :])


def add_rows(rows4, table, grads):
    return pl.pallas_call(
        add_kernel,
        out_shape=jax.ShapeDtypeStruct(table.shape, jnp.float32),
        grid_spec=pltpu.PrefetchScalarGridSpec(
            num_scalar_prefetch=1, grid=(1,),
            in_specs=[pl.BlockSpec(memory_space=ANY),
                      pl.BlockSpec((SLOTS * SUB, LANES), lambda i, *_: (0, 0))],
            out_specs=pl.BlockSpec(memory_space=ANY),
            scratch_shapes=[pltpu.VMEM((table.shape[0] * SUB, LANES), jnp.float32),
                            pltpu.VMEM((2, CHUNK, table.shape[1]), jnp.float32),
                            pltpu.SemaphoreType.DMA((2,))]),
        name='add_rows')(rows4, table, grads)


def score_kernel(separate, bounds, row4s, slot4s, signs, *refs):
    if separate:
        table, acc, u_blk, out, gu_blk, loss_blk, wide, grad, stage, sems, prods, sgn, coef = refs
    else:
        table, u_blk, out, gu_blk, loss_blk, wide, grad, stage, sems, prods, sgn, coef = refs
    step = pl.program_id(0)

    @pl.when(step == 0)
    def _():
        load_table(table, wide, stage, sems)
        loss_blk[...] = jnp.zeros_like(loss_blk)

        @pl.loop(0, grad.shape[0] // 256)
        def _(g):
            grad[pl.ds(pl.multiple_of(g * 256, 256), 256), :] = jnp.zeros((256, LANES), jnp.float32)

    @pl.loop(0, SLOTS * SUB // 256)
    def _(g):
        gu_blk[pl.ds(pl.multiple_of(g * 256, 256), 256), :] = jnp.zeros((256, LANES), jnp.float32)

    begin, end = bounds[step], bounds[step + 1]

    @pl.loop(0, (end - begin + BATCH - 1) // BATCH)
    def _(b):
        base = begin + b * BATCH
        for i in range(BATCH):
            r4 = pl.multiple_of(row4s[base + i], SUB)
            s4 = pl.multiple_of(slot4s[base + i], SUB)
            prods[i * SUB:(i + 1) * SUB, :] = u_blk[pl.ds(s4, SUB), :] * wide[pl.ds(r4, SUB), :]
            sgn[i:i + 1, :] = jnp.full((1, LANES), signs[base + i], jnp.float32)
        part = prods[pl.ds(0, BATCH, stride=SUB), :]
        for j in range(1, SUB):
            part = part + prods[pl.ds(j, BATCH, stride=SUB), :]
        total = jnp.sum(part, axis=1, keepdims=True)
        live = lax.broadcasted_iota(jnp.int32, (BATCH, LANES), 0) < end - base
        sign = jnp.where(live, sgn[...], 0.0)
        signed = sign * total
        small = jnp.exp(-jnp.abs(signed))
        loss = jnp.maximum(signed, 0.0) + jnp.log1p(small)
        loss_blk[...] += jnp.sum((jnp.abs(sign) * loss).reshape(BATCH // 8, 8, LANES), axis=0)
        gain = sign * jnp.where(signed >= 0, 1.0, small) / (1.0 + small)
        for j in range(SUB):
            coef[pl.ds(j, BATCH, stride=SUB), :] = gain
        for i in range(BATCH):
            r4 = pl.multiple_of(row4s[base + i], SUB)
            s4 = pl.multiple_of(slot4s[base + i], SUB)
            c = coef[i * SUB:(i + 1) * SUB, :]
            gu_blk[pl.ds(s4, SUB), :] += c * wide[pl.ds(r4, SUB), :]
            grad[pl.ds(r4, SUB), :] += c * u_blk[pl.ds(s4, SUB), :]

    @pl.when(step == pl.num_programs(0) - 1)
    def _():
        if separate:
            load_table(acc, wide, stage, sems)
        store_table(out, stage, sems,
                    lambda w8, j: wide[pl.ds(w8 + j, 8, stride=SUB), :] - LEARN_RATE * grad[pl.ds(w8 + j, 8, stride=SUB), :])


def score_rows(bounds, row4s, slot4s, signs, table, acc, u_all):
    separate = acc is not None
    n_blocks = u_all.shape[0] // (SLOTS * SUB)
    blk = pl.BlockSpec((SLOTS * SUB, LANES), lambda i, *_: (i, 0))
    tables = (table, acc) if separate else (table,)
    return pl.pallas_call(
        functools.partial(score_kernel, separate),
        out_shape=(jax.ShapeDtypeStruct(table.shape, jnp.float32),
                   jax.ShapeDtypeStruct(u_all.shape, jnp.float32),
                   jax.ShapeDtypeStruct((8, LANES), jnp.float32)),
        grid_spec=pltpu.PrefetchScalarGridSpec(
            num_scalar_prefetch=4, grid=(n_blocks,),
            in_specs=[pl.BlockSpec(memory_space=ANY)] * len(tables) + [blk],
            out_specs=(pl.BlockSpec(memory_space=ANY), blk,
                       pl.BlockSpec((8, LANES), lambda i, *_: (0, 0))),
            scratch_shapes=[pltpu.VMEM((table.shape[0] * SUB, LANES), jnp.float32),
                            pltpu.VMEM((table.shape[0] * SUB, LANES), jnp.float32),
                            pltpu.VMEM((2, CHUNK, table.shape[1]), jnp.float32),
                            pltpu.SemaphoreType.DMA((2,)),
                            pltpu.VMEM((BATCH * SUB, LANES), jnp.float32),
                            pltpu.VMEM((BATCH, LANES), jnp.float32),
                            pltpu.VMEM((BATCH * SUB, LANES), jnp.float32)]),
        compiler_params=pltpu.CompilerParams(vmem_limit_bytes=60 * 1024 * 1024),
        name='score_rows')(bounds, row4s, slot4s, signs, *tables, u_all)


def solution(mesh):
    group = mesh.shape['ep']

    def device_step(table_in, table_out, centers, contexts, negatives):
        rows_dev = table_in.shape[0]
        n_pairs, n_neg = negatives.shape
        n_ref = n_pairs * (n_neg + 1)
        capacity = (3 * n_pairs * (n_neg + 2)) // (2 * group)
        me = lax.axis_index('ep')
        ids = jnp.arange(group, dtype=jnp.int32)

        all_centers = lax.all_gather(centers, 'ep', axis=0, tiled=True)
        all_owner = all_centers % group
        counts = jnp.sum((all_owner.reshape(group, n_pairs)[:, None, :] == ids[None, :, None]).astype(jnp.int32), axis=2)
        totals = jnp.sum(counts, axis=0)
        before = jnp.sum(jnp.where(ids[:, None] < me, counts, 0), axis=0)
        owner_c = centers % group
        one_hot = (owner_c[:, None] == ids[None, :])
        tri = (jnp.arange(n_pairs)[:, None] > jnp.arange(n_pairs)[None, :]).astype(jnp.bfloat16)
        earlier = jnp.dot(tri, one_hot.astype(jnp.bfloat16), preferred_element_type=jnp.float32).astype(jnp.int32)
        rank = jnp.sum(jnp.where(one_hot, earlier + before[None, :], 0), axis=1)
        n_rounds = (jnp.max(totals) + SLOTS - 1) // SLOTS
        place = jnp.arange(group * n_pairs, dtype=jnp.int32)
        big = jnp.int32(2 ** 31 - 1)
        mine = jnp.where(all_owner == me, place * rows_dev + all_centers // group, big)
        my_rows4 = (lax.sort(mine) % rows_dev) * SUB
        my_rows4 = jnp.concatenate([my_rows4, jnp.zeros((SLOTS,), jnp.int32)])

        words = jnp.concatenate([contexts[:, None], negatives], axis=1)
        owner_o = words % group
        row_o = words // group
        is_ctx = (jnp.arange(n_neg + 1) == 0).astype(jnp.int32)[None, :]
        spare_rank = jnp.arange(capacity, dtype=jnp.int32)

        def one_round(turn, acc_in, acc_out):
            local = rank - turn * SLOTS
            inside = (local >= 0) & (local < SLOTS)
            slot = owner_c * SLOTS + local
            code = (slot[:, None] * rows_dev + row_o) * 2 + is_ctx
            dest = jnp.where(inside[:, None], owner_o, group)
            dest_count = jnp.sum((dest.reshape(1, n_ref) == ids[:, None]).astype(jnp.int32), axis=1)
            spare_dest = jnp.where(spare_rank[None, :] < capacity - dest_count[:, None], ids[:, None], group)
            keys = jnp.concatenate([dest.reshape(n_ref), spare_dest.reshape(group * capacity)])
            vals = jnp.concatenate([code.reshape(n_ref), jnp.full((group * capacity,), big)])
            _, vals = lax.sort((keys, vals), num_keys=1, is_stable=False)
            got = lax.all_to_all(vals[:group * capacity].reshape(group, capacity), 'ep', 0, 0)
            refs = lax.sort(got.reshape(group * capacity))
            edges = jnp.arange(group + 1, dtype=jnp.int32) * (SLOTS * rows_dev * 2)
            bounds = jnp.sum((refs[None, :] < edges[:, None]).astype(jnp.int32), axis=1)
            signs = jnp.where(refs % 2 == 1, -1.0, 1.0)
            row4s = (refs // 2) % rows_dev * SUB
            slot4s = (refs // (2 * rows_dev)) % SLOTS * SUB
            pad = jnp.zeros((BATCH,), jnp.int32)
            row4s = jnp.concatenate([row4s, pad])
            slot4s = jnp.concatenate([slot4s, pad])
            signs = jnp.concatenate([signs, jnp.zeros((BATCH,), jnp.float32)])

            rows4 = lax.dynamic_slice(my_rows4, (turn * SLOTS,), (SLOTS,))
            u_mine = pick_rows(rows4, table_in)
            u_all = lax.all_gather(u_mine, 'ep', axis=0, tiled=True)
            new_out, gu, loss = score_rows(bounds, row4s, slot4s, signs, table_out, acc_out, u_all)
            gu_mine = lax.psum_scatter(gu, 'ep', scatter_dimension=0, tiled=True)
            new_in = add_rows(rows4, acc_in, gu_mine)
            return new_in, new_out, jnp.sum(loss[:, 0])

        new_in, new_out, loss = one_round(jnp.int32(0), table_in, None)

        def more(state):
            return state[0] < n_rounds

        def again(state):
            turn, acc_in, acc_out, acc_loss = state
            acc_in, acc_out, part = one_round(turn, acc_in, acc_out)
            return turn + 1, acc_in, acc_out, acc_loss + part

        _, new_in, new_out, loss = lax.while_loop(more, again, (jnp.int32(1), new_in, new_out, loss))
        total_loss = lax.psum(loss, 'ep') / (n_pairs * group)
        return total_loss, new_in, new_out

    return jax.shard_map(device_step, mesh=mesh,
                         in_specs=(P('ep', None), P('ep', None), P('ep'), P('ep'), P('ep', None)),
                         out_specs=(P(), P('ep', None), P('ep', None)), check_vma=False)
```

```python
import functools

import jax
import jax.numpy as jnp
from jax import lax
from jax.experimental import pallas as pl
from jax.experimental.pallas import tpu as pltpu
from jax.sharding import PartitionSpec as P

LEARN_RATE = 0.5
LANES = 128
SUB = 4
TAIL = 500 - 3 * LANES
CHUNK = 512
SLOTS = 1248
BATCH = 64
ROOM = 768
LEFT = 32
ANY = pl.ANY
MESH = pl.DeviceIdType.MESH


def load_table(table, wide, stage, sems, first=0):
    rows = table.shape[0]
    n_chunks = rows // CHUNK

    def copy(k):
        return pltpu.make_async_copy(table.at[pl.ds(k * CHUNK, CHUNK)], stage.at[k % 2], sems.at[k % 2])

    copy(0).start()
    for k in range(n_chunks):
        if k + 1 < n_chunks:
            copy(k + 1).start()
        copy(k).wait()
        buf = stage.at[k % 2]

        @pl.loop(0, CHUNK // 32)
        def _(g):
            for i in range(4):
                r8 = pl.multiple_of((g * 4 + i) * 8, 8)
                w8 = pl.multiple_of((first + k * CHUNK + (g * 4 + i) * 8) * SUB, 32)
                for j in range(SUB):
                    if j < SUB - 1:
                        wide[pl.ds(w8 + j, 8, stride=SUB), :] = buf[pl.ds(r8, 8), j * LANES:(j + 1) * LANES]
                    else:
                        wide[pl.ds(w8 + j, 8, stride=SUB), :] = jnp.concatenate(
                            [buf[pl.ds(r8, 8), j * LANES:j * LANES + TAIL], jnp.zeros((8, LANES - TAIL), jnp.float32)],
                            axis=1)


def store_table(out, stage, sems, value):
    rows = out.shape[0]
    n_chunks = rows // CHUNK

    def copy(k):
        return pltpu.make_async_copy(stage.at[k % 2], out.at[pl.ds(k * CHUNK, CHUNK)], sems.at[k % 2])

    for k in range(n_chunks):
        if k >= 2:
            copy(k - 2).wait()
        buf = stage.at[k % 2]

        @pl.loop(0, CHUNK // 32)
        def _(g):
            for i in range(4):
                r8 = pl.multiple_of((g * 4 + i) * 8, 8)
                w8 = pl.multiple_of((k * CHUNK + (g * 4 + i) * 8) * SUB, 32)
                for j in range(SUB):
                    piece = value(w8, j)
                    if j < SUB - 1:
                        buf[pl.ds(r8, 8), j * LANES:(j + 1) * LANES] = piece
                    else:
                        buf[pl.ds(r8, 8), j * LANES:j * LANES + TAIL] = piece[:, :TAIL]

        copy(k).start()
    copy(n_chunks - 2).wait()
    copy(n_chunks - 1).wait()


def pick_kernel(rows4, table, out, wide, stage, sems):
    load_table(table, wide, stage, sems)

    @pl.loop(0, SLOTS // 16)
    def _(g):
        for i in range(16):
            k = g * 16 + i
            r4 = pl.multiple_of(rows4[k], SUB)
            out[pl.ds(pl.multiple_of(k * SUB, SUB), SUB), :] = wide[pl.ds(r4, SUB), :]


def pick_rows(rows4, table):
    return pl.pallas_call(
        pick_kernel,
        out_shape=jax.ShapeDtypeStruct((SLOTS * SUB, LANES), jnp.float32),
        grid_spec=pltpu.PrefetchScalarGridSpec(
            num_scalar_prefetch=1, grid=(1,),
            in_specs=[pl.BlockSpec(memory_space=ANY)],
            out_specs=pl.BlockSpec((SLOTS * SUB, LANES), lambda i, *_: (0, 0)),
            scratch_shapes=[pltpu.VMEM((table.shape[0] * SUB, LANES), jnp.float32),
                            pltpu.VMEM((2, CHUNK, table.shape[1]), jnp.float32),
                            pltpu.SemaphoreType.DMA((2,))]),
        name='pick_rows')(rows4, table)


def add_kernel(rows4, table, grads, out, wide, stage, sems):
    load_table(table, wide, stage, sems)

    @pl.loop(0, SLOTS // 16)
    def _(g):
        for i in range(16):
            k = g * 16 + i
            r4 = pl.multiple_of(rows4[k], SUB)
            wide[pl.ds(r4, SUB), :] = wide[pl.ds(r4, SUB), :] - LEARN_RATE * grads[pl.ds(pl.multiple_of(k * SUB, SUB), SUB), :]

    store_table(out, stage, sems, lambda w8, j: wide[pl.ds(w8 + j, 8, stride=SUB), :])


def add_rows(rows4, table, grads):
    return pl.pallas_call(
        add_kernel,
        out_shape=jax.ShapeDtypeStruct(table.shape, jnp.float32),
        grid_spec=pltpu.PrefetchScalarGridSpec(
            num_scalar_prefetch=1, grid=(1,),
            in_specs=[pl.BlockSpec(memory_space=ANY),
                      pl.BlockSpec((SLOTS * SUB, LANES), lambda i, *_: (0, 0))],
            out_specs=pl.BlockSpec(memory_space=ANY),
            scratch_shapes=[pltpu.VMEM((table.shape[0] * SUB, LANES), jnp.float32),
                            pltpu.VMEM((2, CHUNK, table.shape[1]), jnp.float32),
                            pltpu.SemaphoreType.DMA((2,))]),
        name='add_rows')(rows4, table, grads)


def score_kernel(bounds, row4s, slot4s, own, other, u_blk, own_grad, other_grad, gu_blk, loss_blk,
                 wide, grad, stage, sems, prods, flag, coef):
    step = pl.program_id(0)
    rows = own.shape[0]

    @pl.when(step == 0)
    def _():
        load_table(own, wide, stage, sems)
        load_table(other, wide, stage, sems, rows)
        loss_blk[...] = jnp.zeros_like(loss_blk)

        @pl.loop(0, grad.shape[0] // 256)
        def _(g):
            grad[pl.ds(pl.multiple_of(g * 256, 256), 256), :] = jnp.zeros((256, LANES), jnp.float32)

    @pl.loop(0, SLOTS * SUB // 128)
    def _(g):
        gu_blk[pl.ds(pl.multiple_of(g * 128, 128), 128), :] = jnp.zeros((128, LANES), jnp.float32)

    begin, end = bounds[step], bounds[step + 1]

    @pl.loop(0, (end - begin + BATCH - 1) // BATCH)
    def _(b):
        base = begin + b * BATCH
        for i in range(BATCH):
            r4 = pl.multiple_of(row4s[base + i], SUB)
            code = slot4s[base + i]
            ctx = code % 2
            s4 = pl.multiple_of(code - ctx, SUB)
            prods[i * SUB:(i + 1) * SUB, :] = u_blk[pl.ds(s4, SUB), :] * wide[pl.ds(r4, SUB), :]
            flag[i:i + 1, :] = jnp.full((1, LANES), ctx, jnp.int32)
        part = prods[pl.ds(0, BATCH, stride=SUB), :]
        for j in range(1, SUB):
            part = part + prods[pl.ds(j, BATCH, stride=SUB), :]
        total = jnp.sum(part, axis=1, keepdims=True)
        live = lax.broadcasted_iota(jnp.int32, (BATCH, LANES), 0) < end - base
        sign = jnp.where(live, jnp.where(flag[...] == 1, -1.0, 1.0), 0.0)
        signed = sign * total
        small = jnp.exp(-jnp.abs(signed))
        loss = jnp.maximum(signed, 0.0) + jnp.log1p(small)
        loss_blk[...] += jnp.sum((jnp.abs(sign) * loss).reshape(BATCH // 8, 8, LANES), axis=0)
        gain = sign * jnp.where(signed >= 0, 1.0, small) / (1.0 + small)
        for j in range(SUB):
            coef[pl.ds(j, BATCH, stride=SUB), :] = gain
        for i in range(BATCH):
            r4 = pl.multiple_of(row4s[base + i], SUB)
            code = slot4s[base + i]
            s4 = pl.multiple_of(code - code % 2, SUB)
            c = coef[i * SUB:(i + 1) * SUB, :]
            gu_blk[pl.ds(s4, SUB), :] += c * wide[pl.ds(r4, SUB), :]
            grad[pl.ds(r4, SUB), :] += c * u_blk[pl.ds(s4, SUB), :]

    @pl.when(step == pl.num_programs(0) - 1)
    def _():
        first = pltpu.make_async_copy(grad.at[pl.ds(0, rows * SUB)], own_grad, sems.at[0])
        second = pltpu.make_async_copy(grad.at[pl.ds(rows * SUB, rows * SUB)], other_grad, sems.at[1])
        first.start()
        second.start()
        first.wait()
        second.wait()


def score_rows(bounds, row4s, slot4s, own, other, u_all):
    rows, width = own.shape
    n_blocks = u_all.shape[0] // (SLOTS * SUB)
    blk = pl.BlockSpec((SLOTS * SUB, LANES), lambda i, *_: (i, 0))
    half = jax.ShapeDtypeStruct((rows * SUB, LANES), jnp.float32)
    return pl.pallas_call(
        score_kernel,
        out_shape=(half, half, jax.ShapeDtypeStruct(u_all.shape, jnp.float32),
                   jax.ShapeDtypeStruct((8, LANES), jnp.float32)),
        grid_spec=pltpu.PrefetchScalarGridSpec(
            num_scalar_prefetch=3, grid=(n_blocks,),
            in_specs=[pl.BlockSpec(memory_space=ANY), pl.BlockSpec(memory_space=ANY), blk],
            out_specs=(pl.BlockSpec(memory_space=ANY), pl.BlockSpec(memory_space=ANY), blk,
                       pl.BlockSpec((8, LANES), lambda i, *_: (0, 0))),
            scratch_shapes=[pltpu.VMEM((2 * rows * SUB, LANES), jnp.float32),
                            pltpu.VMEM((2 * rows * SUB, LANES), jnp.float32),
                            pltpu.VMEM((2, CHUNK, width), jnp.float32),
                            pltpu.SemaphoreType.DMA((2,)),
                            pltpu.VMEM((BATCH * SUB, LANES), jnp.float32),
                            pltpu.VMEM((BATCH, LANES), jnp.int32),
                            pltpu.VMEM((BATCH * SUB, LANES), jnp.float32)]),
        compiler_params=pltpu.CompilerParams(vmem_limit_bytes=60 * 1024 * 1024),
        name='score_rows')(bounds, row4s, slot4s, own, other, u_all)


def finish_kernel(table, first, second, out):
    @pl.loop(0, CHUNK // 32)
    def _(g):
        for i in range(4):
            r8 = pl.multiple_of((g * 4 + i) * 8, 8)
            w8 = pl.multiple_of((g * 4 + i) * 8 * SUB, 32)
            for j in range(SUB):
                cols = slice(j * LANES, (j + 1) * LANES if j < SUB - 1 else j * LANES + TAIL)
                grad = first[pl.ds(w8 + j, 8, stride=SUB), :] + second[pl.ds(w8 + j, 8, stride=SUB), :]
                if j == SUB - 1:
                    grad = grad[:, :TAIL]
                out[pl.ds(r8, 8), cols] = table[pl.ds(r8, 8), cols] - LEARN_RATE * grad


def finish_rows(table, first, second):
    rows, width = table.shape
    native = pl.BlockSpec((CHUNK, width), lambda i: (i, 0))
    wide = pl.BlockSpec((CHUNK * SUB, LANES), lambda i: (i, 0))
    return pl.pallas_call(
        finish_kernel, out_shape=jax.ShapeDtypeStruct(table.shape, jnp.float32), grid=(rows // CHUNK,),
        in_specs=[native, wide, wide], out_specs=native, name='finish_rows')(table, first, second)


def place_of():
    me = lax.axis_index('ep')
    x, y, z = (me // 2) % 2, (me // 4) % 2, me // 8
    return me, x, y, z, me + 2 - 4 * x, me + 4 - 8 * y


def plane_order(z):
    far = 3 * (1 - z // 2)
    near = 1 + z % 2
    return z, near, 6 - far - near - z, far


def meet_neighbours(me, z, x_peer, y_peer):
    barrier = pltpu.get_barrier_semaphore()
    pl.semaphore_signal(barrier, inc=1, device_id=(x_peer,), device_id_type=MESH)
    pl.semaphore_signal(barrier, inc=1, device_id=(y_peer,), device_id_type=MESH)

    @pl.when(z < 3)
    def _():
        pl.semaphore_signal(barrier, inc=1, device_id=(me + 8,), device_id_type=MESH)

    @pl.when(z > 0)
    def _():
        pl.semaphore_signal(barrier, inc=1, device_id=(me - 8,), device_id_type=MESH)

    @pl.when((z > 0) & (z < 3))
    def _():
        pl.semaphore_wait(barrier, 4)

    @pl.when((z == 0) | (z == 3))
    def _():
        pl.semaphore_wait(barrier, 3)


def remote(src, dst, send, recv, peer):
    return pltpu.make_async_remote_copy(src_ref=src, dst_ref=dst, send_sem=send, recv_sem=recv,
                                        device_id=(peer,), device_id_type=MESH)


def gather_kernel(mine, out, zs, zr, xs, xr, ys, yr, local_sem):
    me, x, y, z, x_peer, y_peer = place_of()
    half = mine.shape[0] // 2
    low, high = pl.ds(0, half), pl.ds(half, half)
    planes = plane_order(z)

    def up(p, src):
        return remote(src, out.at[p, y, x], zs.at[0, p], zr.at[0, p], me + 8)

    def down(p, src):
        return remote(src, out.at[p, y, x], zs.at[1, p], zr.at[1, p], me - 8)

    def held(p):
        return out.at[p, y, x]

    def to_x(k, m, src, row, part):
        return remote(src, out.at[planes[k], row, x, part], xs.at[m, k], xr.at[m, k], x_peer)

    def to_y(k, m, src, col, part):
        return remote(src, out.at[planes[k], y, col, part], ys.at[m, k], yr.at[m, k], y_peer)

    def own_pieces(k):
        src = mine if k == 0 else held(planes[k])
        return (to_y(k, 0, src.at[low], x, low), to_x(k, 0, src.at[high], y, high),
                to_y(k, 1, src.at[high], x, high), to_x(k, 1, src.at[low], y, low))

    def second_x(k):
        return to_x(k, 2, out.at[planes[k], 1 - y, x, low], 1 - y, low)

    def second_y(k):
        return to_y(k, 2, out.at[planes[k], y, 1 - x, high], 1 - x, high)

    def from_x(k, m, row, part):
        spot = out.at[planes[k], row, 1 - x, part]
        return remote(spot, spot, xs.at[m, k], xr.at[m, k], x_peer)

    def from_y(k, m, col, part):
        spot = out.at[planes[k], 1 - y, col, part]
        return remote(spot, spot, ys.at[m, k], yr.at[m, k], y_peer)

    meet_neighbours(me, z, x_peer, y_peer)
    keep = pltpu.make_async_copy(mine, out.at[z, y, x], local_sem)

    @pl.when(z < 3)
    def _():
        up(z, mine).start()

    @pl.when(z > 0)
    def _():
        down(z, mine).start()

    for piece in own_pieces(0):
        piece.start()
    keep.start()

    def relay(k):
        from_y(k, 0, x, low).wait_recv()
        second_x(k).start()
        from_x(k, 0, y, high).wait_recv()
        second_y(k).start()

    for k in range(1, 4):
        p = planes[k]

        @pl.when(p < z)
        def _():
            up(p, held(p)).wait_recv()

            @pl.when(z < 3)
            def _():
                up(p, held(p)).start()

        @pl.when(p > z)
        def _():
            down(p, held(p)).wait_recv()

            @pl.when(z > 0)
            def _():
                down(p, held(p)).start()

        for piece in own_pieces(k):
            piece.start()
        relay(k - 1)
    relay(3)

    keep.wait()
    for k in range(4):
        from_y(k, 1, x, high).wait_recv()
        from_x(k, 1, y, low).wait_recv()
        from_x(k, 2, 1 - y, low).wait_recv()
        from_y(k, 2, 1 - x, high).wait_recv()
        for piece in own_pieces(k):
            piece.wait_send()
        second_x(k).wait_send()
        second_y(k).wait_send()
        p = planes[k]

        @pl.when((p <= z) & (z < 3))
        def _():
            up(p, held(p)).wait_send()

        @pl.when((p >= z) & (z > 0))
        def _():
            down(p, held(p)).wait_send()


def gather_slots(mine):
    rows = mine.shape[0]
    dma = pltpu.SemaphoreType.DMA
    out = pl.pallas_call(
        gather_kernel,
        out_shape=jax.ShapeDtypeStruct((4, 2, 2, rows, LANES), jnp.float32),
        in_specs=[pl.BlockSpec(memory_space=pltpu.VMEM)],
        out_specs=pl.BlockSpec(memory_space=ANY),
        scratch_shapes=[dma((2, 4)), dma((2, 4)), dma((3, 4)), dma((3, 4)), dma((3, 4)), dma((3, 4)), dma],
        compiler_params=pltpu.CompilerParams(collective_id=1, has_side_effects=True),
        name='gather_slots')(mine)
    return out.reshape(16 * rows, LANES)


def scatter_kernel(parts, out, r1x, r1y, r2x, r2y, zu, zd, stage, zs, zr, xs, xr, ys, yr, stage_sem):
    me, x, y, z, x_peer, y_peer = place_of()
    half = out.shape[0] // 2
    low, high = pl.ds(0, half), pl.ds(half, half)
    planes = plane_order(z)[::-1]

    def x1(k, h):
        row = 1 - y if h == 0 else y
        return remote(parts.at[planes[k], row, 1 - x, low], r1x.at[k, h], xs.at[h, k], xr.at[h, k], x_peer)

    def y1(k, h):
        col = 1 - x if h == 0 else x
        return remote(parts.at[planes[k], 1 - y, col, high], r1y.at[k, h], ys.at[h, k], yr.at[h, k], y_peer)

    def x2(k):
        return remote(r1y.at[k, 0], r2y.at[k], xs.at[2, k], xr.at[2, k], x_peer)

    def y2(k):
        return remote(r1x.at[k, 0], r2x.at[k], ys.at[2, k], yr.at[2, k], y_peer)

    def load(k, i):
        p = planes[k]
        src = (parts.at[p, 1 - y, x, low], parts.at[p, y, x, low],
               parts.at[p, y, 1 - x, high], parts.at[p, y, x, high])[i]
        return pltpu.make_async_copy(src, stage.at[i], stage_sem.at[i])

    def add(dst, *others):
        @pl.loop(0, half // 64)
        def _(g):
            rows = pl.ds(pl.multiple_of(g * 64, 64), 64)
            value = dst[rows, :]
            for other in others:
                value = value + other[rows, :]
            dst[rows, :] = value

    def up(c, k, src):
        p = planes[k]
        return remote(src, zu.at[c, p - 1], zs.at[c, 0, p], zr.at[c, 0, p], me + 8)

    def down(c, k, src):
        p = planes[k]
        return remote(src, zd.at[c, p], zs.at[c, 1, p], zr.at[c, 1, p], me - 8)

    meet_neighbours(me, z, x_peer, y_peer)
    for i in range(4):
        load(0, i).start()
    for k in range(2):
        for h in range(2):
            x1(k, h).start()
            y1(k, h).start()

    def settle(c, k, total, first, i):
        p = planes[k]
        load(k, i).wait()
        add(total, first, stage.at[i])
        if k < 3:
            load(k + 1, i).start()

        @pl.when((p >= z) & (z > 0))
        def _():
            up(c, k, total).wait_recv()
            add(total, zu.at[c, p - 1])

        @pl.when((p <= z) & (z < 3))
        def _():
            down(c, k, total).wait_recv()
            add(total, zd.at[c, p])

    def move(c, k, total):
        p = planes[k]

        @pl.when(p > z)
        def _():
            up(c, k, total).start()

        @pl.when(p < z)
        def _():
            down(c, k, total).start()

    def finish(k):
        x1(k, 1).wait_recv()
        y2(k).wait_recv()
        settle(0, k, r2x.at[k], r1x.at[k, 1], 1)
        if k < 3:
            move(0, k, r2x.at[k])
        y1(k, 1).wait_recv()
        x2(k).wait_recv()
        settle(1, k, r2y.at[k], r1y.at[k, 1], 3)
        if k < 3:
            move(1, k, r2y.at[k])

    for k in range(4):
        x1(k, 0).wait_recv()
        load(k, 0).wait()
        add(r1x.at[k, 0], stage.at[0])
        y1(k, 0).wait_recv()
        load(k, 2).wait()
        add(r1y.at[k, 0], stage.at[2])
        if k < 3:
            load(k + 1, 0).start()
            load(k + 1, 2).start()
        y2(k).start()
        x2(k).start()
        if k + 2 < 4:
            for h in range(2):
                x1(k + 2, h).start()
                y1(k + 2, h).start()
        if k > 0:
            finish(k - 1)
    finish(3)

    @pl.loop(0, half // 64)
    def _(g):
        rows = pl.ds(pl.multiple_of(g * 64, 64), 64)
        out[rows, :] = r2x[3, rows, :]
        out[pl.ds(pl.multiple_of(half + g * 64, 64), 64), :] = r2y[3, rows, :]

    for k in range(4):
        for h in range(2):
            x1(k, h).wait_send()
            y1(k, h).wait_send()
        x2(k).wait_send()
        y2(k).wait_send()
        if k < 3:
            p = planes[k]
            for c, total in ((0, r2x.at[k]), (1, r2y.at[k])):
                @pl.when(p > z)
                def _():
                    up(c, k, total).wait_send()

                @pl.when(p < z)
                def _():
                    down(c, k, total).wait_send()


def scatter_slots(parts):
    rows = parts.shape[0] // 16
    dma = pltpu.SemaphoreType.DMA
    half = rows // 2
    f32 = jnp.float32
    return pl.pallas_call(
        scatter_kernel,
        out_shape=jax.ShapeDtypeStruct((rows, LANES), f32),
        in_specs=[pl.BlockSpec(memory_space=ANY)],
        out_specs=pl.BlockSpec(memory_space=pltpu.VMEM),
        scratch_shapes=[pltpu.VMEM((4, 2, half, LANES), f32), pltpu.VMEM((4, 2, half, LANES), f32),
                        pltpu.VMEM((4, half, LANES), f32), pltpu.VMEM((4, half, LANES), f32),
                        pltpu.VMEM((2, 3, half, LANES), f32), pltpu.VMEM((2, 3, half, LANES), f32),
                        pltpu.VMEM((4, half, LANES), f32),
                        dma((2, 2, 4)), dma((2, 2, 4)), dma((3, 4)), dma((3, 4)), dma((3, 4)), dma((3, 4)), dma((4,))],
        compiler_params=pltpu.CompilerParams(collective_id=2, has_side_effects=True,
                                             vmem_limit_bytes=62 * 1024 * 1024),
        name='scatter_slots')(parts.reshape(4, 2, 2, rows, LANES))


def solution(mesh):
    group = mesh.shape['ep']

    def device_step(table_in, table_out, centers, contexts, negatives):
        rows_dev, width = table_in.shape
        n_pairs, n_neg = negatives.shape
        n_ref = n_pairs * (n_neg + 1)
        me = lax.axis_index('ep')
        ids = jnp.arange(group, dtype=jnp.int32)
        partner = [(d, d + 1 - 2 * (d % 2)) for d in range(group)]
        other_out = lax.ppermute(table_out, 'ep', partner)

        all_centers = lax.all_gather(centers, 'ep', axis=0, tiled=True)
        all_owner = all_centers % group
        counts = jnp.sum((all_owner.reshape(group, n_pairs)[:, None, :] == ids[None, :, None]).astype(jnp.int32), axis=2)
        totals = jnp.sum(counts, axis=0)
        before = jnp.sum(jnp.where(ids[:, None] < me, counts, 0), axis=0)
        owner_c = centers % group
        one_hot = (owner_c[:, None] == ids[None, :])
        tri = (jnp.arange(n_pairs)[:, None] > jnp.arange(n_pairs)[None, :]).astype(jnp.bfloat16)
        earlier = jnp.dot(tri, one_hot.astype(jnp.bfloat16), preferred_element_type=jnp.float32).astype(jnp.int32)
        rank = jnp.sum(jnp.where(one_hot, earlier + before[None, :], 0), axis=1)
        place = jnp.arange(group * n_pairs, dtype=jnp.int32)
        big = jnp.int32(2 ** 31 - 1)
        mine = jnp.where(all_owner == me, place * rows_dev + all_centers // group, big)
        rows4 = (lax.sort(mine)[:SLOTS] % rows_dev) * SUB
        u_mine = pick_rows(rows4, table_in)

        words = jnp.concatenate([contexts[:, None], negatives], axis=1)
        owner_o = words % group
        core_u = (owner_c % 2)[:, None]
        row_o = words // group + (owner_o + core_u) % 2 * rows_dev
        is_ctx = (jnp.arange(n_neg + 1) == 0).astype(jnp.int32)[None, :]
        code = ((owner_c // 2 * SLOTS + rank)[:, None] * (2 * rows_dev) + row_o) * 2 + is_ctx
        fits = rank < SLOTS
        dest = jnp.where(fits[:, None], owner_o // 2 * 2 + core_u, group)
        dest_count = jnp.sum((dest.reshape(1, n_ref) == ids[:, None]).astype(jnp.int32), axis=1)
        roomy = jnp.max(dest_count) <= ROOM
        fits = fits & roomy
        dest = jnp.where(roomy, dest, group)
        dest_count = jnp.where(roomy, dest_count, 0)
        spare_dest = jnp.where(jnp.arange(ROOM)[None, :] < ROOM - dest_count[:, None], ids[:, None], group)
        keys = jnp.concatenate([dest.reshape(n_ref), spare_dest.reshape(group * ROOM)])
        vals = jnp.concatenate([code.reshape(n_ref), jnp.full((group * ROOM,), big)])
        _, vals = lax.sort((keys, vals), num_keys=1, is_stable=False)
        got = lax.all_to_all(vals[:group * ROOM].reshape(group, ROOM), 'ep', 0, 0)
        refs = lax.sort(got.reshape(group * ROOM))
        edges = jnp.arange(group // 2 + 1, dtype=jnp.int32) * (SLOTS * rows_dev * 4)
        bounds = jnp.sum((refs[None, :] < edges[:, None]).astype(jnp.int32), axis=1)
        pad = jnp.zeros((BATCH,), jnp.int32)
        row4s = jnp.concatenate([(refs // 2) % (2 * rows_dev) * SUB, pad])
        slot4s = jnp.concatenate([(refs // (4 * rows_dev)) % SLOTS * SUB + refs % 2, pad])

        u_all = gather_slots(u_mine)
        own_grad, other_grad, gu, loss = score_rows(bounds, row4s, slot4s, table_out, other_out, u_all)
        back_grad = lax.ppermute(other_grad, 'ep', partner)
        gu_mine = scatter_slots(gu)
        new_in = add_rows(rows4, table_in, gu_mine)
        new_out = finish_rows(table_out, own_grad, back_grad)
        loss = jnp.sum(loss[:, 0])
        overflow = jnp.sum(jnp.where(fits, 0, 1))
        sums = lax.psum(jnp.stack([loss, overflow.astype(jnp.float32)]), 'ep')

        def more(state):
            return state[0] < jnp.where(sums[1] > 0.5, n_pairs // LEFT, 0)

        def again(state):
            turn, acc_in, acc_out, acc_loss = state

            def cut(a):
                return lax.all_gather(lax.dynamic_slice_in_dim(a, turn * LEFT, LEFT), 'ep', axis=0, tiled=True)

            word = jnp.concatenate([cut(centers)[:, None], cut(words)], axis=1)
            left = cut(jnp.where(fits, 0, 1))[:, None] == 1
            held = word % group == me
            row = word // group
            found = jnp.concatenate([table_in[row[:, :1]], table_out[row[:, 1:]]], axis=1)
            found = lax.psum(jnp.where(held[:, :, None], found, 0.0), 'ep')
            u_vec, o_vec = found[:, 0], found[:, 1:]
            sign = jnp.where(is_ctx == 1, -1.0, 1.0)
            signed = sign * jnp.sum(u_vec[:, None, :] * o_vec, axis=-1)
            part = jnp.sum(jnp.where(left & (me == 0), -jax.nn.log_sigmoid(-signed), 0.0))
            gain = jnp.where(left, sign * jax.nn.sigmoid(signed), 0.0)
            goal = jnp.where(held & left, row, rows_dev)
            grad_u = jnp.sum(gain[:, :, None] * o_vec, axis=1)
            grad_o = gain[:, :, None] * u_vec[:, None, :]
            acc_in = acc_in.at[goal[:, 0]].add(-LEARN_RATE * grad_u, mode='drop')
            acc_out = acc_out.at[goal[:, 1:].reshape(-1)].add(-LEARN_RATE * grad_o.reshape(-1, width), mode='drop')
            return turn + 1, acc_in, acc_out, acc_loss + lax.psum(part, 'ep')

        _, new_in, new_out, total = lax.while_loop(more, again, (jnp.int32(0), new_in, new_out, sums[0]))
        return total / (n_pairs * group), new_in, new_out

    return jax.shard_map(device_step, mesh=mesh,
                         in_specs=(P('ep', None), P('ep', None), P('ep'), P('ep'), P('ep', None)),
                         out_specs=(P(), P('ep', None), P('ep', None)), check_vma=False)
```

```python
import functools

import jax
import jax.numpy as jnp
from jax import lax
from jax.experimental import pallas as pl
from jax.experimental.pallas import tpu as pltpu
from jax.sharding import PartitionSpec as P

LEARN_RATE = 0.5
LANES = 128
SUB = 4
TAIL = 500 - 3 * LANES
CHUNK = 512
SLOTS = 1248
BATCH = 64
UNROLL = 16
STEP = 64
UP, DOWN, LATE = range(3)
ROOM = 768
LEFT = 32
ANY = pl.ANY
MESH = pl.DeviceIdType.MESH


def load_table(table, wide, stage, sems, first=0):
    rows = table.shape[0]
    n_chunks = rows // CHUNK

    def copy(k):
        return pltpu.make_async_copy(table.at[pl.ds(k * CHUNK, CHUNK)], stage.at[k % 2], sems.at[k % 2])

    copy(0).start()
    for k in range(n_chunks):
        if k + 1 < n_chunks:
            copy(k + 1).start()
        copy(k).wait()
        buf = stage.at[k % 2]

        @pl.loop(0, CHUNK // 32)
        def _(g):
            for i in range(4):
                r8 = pl.multiple_of((g * 4 + i) * 8, 8)
                w8 = pl.multiple_of((first + k * CHUNK + (g * 4 + i) * 8) * SUB, 32)
                for j in range(SUB):
                    if j < SUB - 1:
                        wide[pl.ds(w8 + j, 8, stride=SUB), :] = buf[pl.ds(r8, 8), j * LANES:(j + 1) * LANES]
                    else:
                        wide[pl.ds(w8 + j, 8, stride=SUB), :] = jnp.concatenate(
                            [buf[pl.ds(r8, 8), j * LANES:j * LANES + TAIL], jnp.zeros((8, LANES - TAIL), jnp.float32)],
                            axis=1)


def store_table(out, stage, sems, value):
    rows = out.shape[0]
    n_chunks = rows // CHUNK

    def copy(k):
        return pltpu.make_async_copy(stage.at[k % 2], out.at[pl.ds(k * CHUNK, CHUNK)], sems.at[k % 2])

    for k in range(n_chunks):
        if k >= 2:
            copy(k - 2).wait()
        buf = stage.at[k % 2]

        @pl.loop(0, CHUNK // 32)
        def _(g):
            for i in range(4):
                r8 = pl.multiple_of((g * 4 + i) * 8, 8)
                w8 = pl.multiple_of((k * CHUNK + (g * 4 + i) * 8) * SUB, 32)
                for j in range(SUB):
                    piece = value(w8, j)
                    if j < SUB - 1:
                        buf[pl.ds(r8, 8), j * LANES:(j + 1) * LANES] = piece
                    else:
                        buf[pl.ds(r8, 8), j * LANES:j * LANES + TAIL] = piece[:, :TAIL]

        copy(k).start()
    copy(n_chunks - 2).wait()
    copy(n_chunks - 1).wait()


def pick_kernel(rows4, table, out, wide, stage, sems):
    load_table(table, wide, stage, sems)

    @pl.loop(0, SLOTS // 16)
    def _(g):
        for i in range(16):
            k = g * 16 + i
            r4 = pl.multiple_of(rows4[k], SUB)
            out[pl.ds(pl.multiple_of(k * SUB, SUB), SUB), :] = wide[pl.ds(r4, SUB), :]


def pick_rows(rows4, table):
    return pl.pallas_call(
        pick_kernel,
        out_shape=jax.ShapeDtypeStruct((SLOTS * SUB, LANES), jnp.float32),
        grid_spec=pltpu.PrefetchScalarGridSpec(
            num_scalar_prefetch=1, grid=(1,),
            in_specs=[pl.BlockSpec(memory_space=ANY)],
            out_specs=pl.BlockSpec((SLOTS * SUB, LANES), lambda i, *_: (0, 0)),
            scratch_shapes=[pltpu.VMEM((table.shape[0] * SUB, LANES), jnp.float32),
                            pltpu.VMEM((2, CHUNK, table.shape[1]), jnp.float32),
                            pltpu.SemaphoreType.DMA((2,))]),
        name='pick_rows')(rows4, table)


def add_kernel(rows4, table, grads, out, wide, stage, sems):
    load_table(table, wide, stage, sems)

    @pl.loop(0, SLOTS // 16)
    def _(g):
        for i in range(16):
            k = g * 16 + i
            r4 = pl.multiple_of(rows4[k], SUB)
            wide[pl.ds(r4, SUB), :] = wide[pl.ds(r4, SUB), :] - LEARN_RATE * grads[pl.ds(pl.multiple_of(k * SUB, SUB), SUB), :]

    store_table(out, stage, sems, lambda w8, j: wide[pl.ds(w8 + j, 8, stride=SUB), :])


def add_rows(rows4, table, grads):
    return pl.pallas_call(
        add_kernel,
        out_shape=jax.ShapeDtypeStruct(table.shape, jnp.float32),
        grid_spec=pltpu.PrefetchScalarGridSpec(
            num_scalar_prefetch=1, grid=(1,),
            in_specs=[pl.BlockSpec(memory_space=ANY),
                      pl.BlockSpec((SLOTS * SUB, LANES), lambda i, *_: (0, 0))],
            out_specs=pl.BlockSpec(memory_space=ANY),
            scratch_shapes=[pltpu.VMEM((table.shape[0] * SUB, LANES), jnp.float32),
                            pltpu.VMEM((2, CHUNK, table.shape[1]), jnp.float32),
                            pltpu.SemaphoreType.DMA((2,))]),
        name='add_rows')(rows4, table, grads)


def score_kernel(bounds, row4s, slot4s, own, other, u_blk, own_grad, other_grad, gu_blk, loss_blk,
                 wide, grad, stage, sems, prods, coef):
    step = pl.program_id(0)
    rows = own.shape[0]

    @pl.when(step == 0)
    def _():
        load_table(own, wide, stage, sems)
        load_table(other, wide, stage, sems, rows)
        loss_blk[...] = jnp.zeros_like(loss_blk)

        @pl.loop(0, grad.shape[0] // 256)
        def _(g):
            grad[pl.ds(pl.multiple_of(g * 256, 256), 256), :] = jnp.zeros((256, LANES), jnp.float32)

    @pl.loop(0, SLOTS * SUB // 128)
    def _(g):
        gu_blk[pl.ds(pl.multiple_of(g * 128, 128), 128), :] = jnp.zeros((128, LANES), jnp.float32)

    begin, middle, end = bounds[2 * step], bounds[2 * step + 1], bounds[2 * step + 2]

    def spots(k):
        return pl.ds(pl.multiple_of(row4s[k], SUB), SUB), pl.ds(pl.multiple_of(slot4s[k], SUB), SUB)

    @pl.loop(0, (end - begin + BATCH - 1) // BATCH)
    def _(b):
        base = begin + b * BATCH

        @pl.loop(0, BATCH // UNROLL)
        def _(g):
            for i in range(UNROLL):
                k = g * UNROLL + i
                row, slot = spots(base + k)
                prods[pl.ds(pl.multiple_of(k * SUB, SUB), SUB), :] = u_blk[slot, :] * wide[row, :]

        part = prods[pl.ds(0, BATCH, stride=SUB), :]
        for j in range(1, SUB):
            part = part + prods[pl.ds(j, BATCH, stride=SUB), :]
        total = jnp.sum(part, axis=1, keepdims=True)
        number = lax.broadcasted_iota(jnp.int32, (BATCH, LANES), 0)
        sign = jnp.where(number < end - base, jnp.where(number < middle - base, 1.0, -1.0), 0.0)
        signed = sign * total
        small = jnp.exp(-jnp.abs(signed))
        loss = jnp.maximum(signed, 0.0) + jnp.log1p(small)
        loss_blk[...] += jnp.sum((jnp.abs(sign) * loss).reshape(BATCH // 8, 8, LANES), axis=0)
        gain = sign * jnp.where(signed >= 0, 1.0, small) / (1.0 + small)
        for j in range(SUB):
            coef[pl.ds(j, BATCH, stride=SUB), :] = gain

        @pl.loop(0, BATCH // UNROLL)
        def _(g):
            for i in range(0, UNROLL, 2):
                k = g * UNROLL + i
                row_a, slot_a = spots(base + k)
                row_b, slot_b = spots(base + k + 1)
                c_a = coef[pl.ds(pl.multiple_of(k * SUB, SUB), SUB), :]
                c_b = coef[pl.ds(pl.multiple_of((k + 1) * SUB, SUB), SUB), :]
                gu_a, gu_b = c_a * wide[row_a, :], c_b * wide[row_b, :]
                go_a, go_b = c_a * u_blk[slot_a, :], c_b * u_blk[slot_b, :]
                gu_b = gu_b + jnp.where(slot4s[base + k] == slot4s[base + k + 1], gu_a, 0.0)
                go_b = go_b + jnp.where(row4s[base + k] == row4s[base + k + 1], go_a, 0.0)
                gu_a, gu_b = gu_a + gu_blk[slot_a, :], gu_b + gu_blk[slot_b, :]
                go_a, go_b = go_a + grad[row_a, :], go_b + grad[row_b, :]
                gu_blk[slot_a, :] = gu_a
                grad[row_a, :] = go_a
                gu_blk[slot_b, :] = gu_b
                grad[row_b, :] = go_b

    @pl.when(step == pl.num_programs(0) - 1)
    def _():
        first = pltpu.make_async_copy(grad.at[pl.ds(0, rows * SUB)], own_grad, sems.at[0])
        second = pltpu.make_async_copy(grad.at[pl.ds(rows * SUB, rows * SUB)], other_grad, sems.at[1])
        first.start()
        second.start()
        first.wait()
        second.wait()


def score_rows(bounds, row4s, slot4s, own, other, u_all):
    rows, width = own.shape
    n_blocks = u_all.shape[0] // (SLOTS * SUB)
    blk = pl.BlockSpec((SLOTS * SUB, LANES), lambda i, *_: (i, 0))
    half = jax.ShapeDtypeStruct((rows * SUB, LANES), jnp.float32)
    return pl.pallas_call(
        score_kernel,
        out_shape=(half, half, jax.ShapeDtypeStruct(u_all.shape, jnp.float32),
                   jax.ShapeDtypeStruct((8, LANES), jnp.float32)),
        grid_spec=pltpu.PrefetchScalarGridSpec(
            num_scalar_prefetch=3, grid=(n_blocks,),
            in_specs=[pl.BlockSpec(memory_space=ANY), pl.BlockSpec(memory_space=ANY), blk],
            out_specs=(pl.BlockSpec(memory_space=ANY), pl.BlockSpec(memory_space=ANY), blk,
                       pl.BlockSpec((8, LANES), lambda i, *_: (0, 0))),
            scratch_shapes=[pltpu.VMEM((2 * rows * SUB, LANES), jnp.float32),
                            pltpu.VMEM((2 * rows * SUB, LANES), jnp.float32),
                            pltpu.VMEM((2, CHUNK, width), jnp.float32),
                            pltpu.SemaphoreType.DMA((2,)),
                            pltpu.VMEM((BATCH * SUB, LANES), jnp.float32),
                            pltpu.VMEM((BATCH * SUB, LANES), jnp.float32)]),
        compiler_params=pltpu.CompilerParams(vmem_limit_bytes=60 * 1024 * 1024),
        name='score_rows')(bounds, row4s, slot4s, own, other, u_all)


def finish_kernel(table, first, second, out):
    @pl.loop(0, CHUNK // 32)
    def _(g):
        for i in range(4):
            r8 = pl.multiple_of((g * 4 + i) * 8, 8)
            w8 = pl.multiple_of((g * 4 + i) * 8 * SUB, 32)
            for j in range(SUB):
                cols = slice(j * LANES, (j + 1) * LANES if j < SUB - 1 else j * LANES + TAIL)
                grad = first[pl.ds(w8 + j, 8, stride=SUB), :] + second[pl.ds(w8 + j, 8, stride=SUB), :]
                if j == SUB - 1:
                    grad = grad[:, :TAIL]
                out[pl.ds(r8, 8), cols] = table[pl.ds(r8, 8), cols] - LEARN_RATE * grad


def finish_rows(table, first, second):
    rows, width = table.shape
    native = pl.BlockSpec((CHUNK, width), lambda i: (i, 0))
    wide = pl.BlockSpec((CHUNK * SUB, LANES), lambda i: (i, 0))
    return pl.pallas_call(
        finish_kernel, out_shape=jax.ShapeDtypeStruct(table.shape, jnp.float32), grid=(rows // CHUNK,),
        in_specs=[native, wide, wide], out_specs=native, name='finish_rows')(table, first, second)


def place_of():
    me = lax.axis_index('ep')
    x, y, z = (me // 2) % 2, (me // 4) % 2, me // 8
    return me, x, y, z, 1 - x, 1 - y, me + 2 - 4 * x, me + 4 - 8 * y, z > 0, z < 3


def block_of(g, base=0):
    return pl.ds(pl.multiple_of(base + g * STEP, STEP), STEP)


def pair(sends, recvs, k):
    at = k if isinstance(k, tuple) else (k,)
    return sends.at[at], recvs.at[at]


def plane_order(z):
    far = 3 * (1 - z // 2)
    near = 1 + z % 2
    return z, near, 6 - far - near - z, far


def meet_neighbours(me, x_peer, y_peer, below, above):
    barrier = pltpu.get_barrier_semaphore()
    pl.semaphore_signal(barrier, inc=1, device_id=(x_peer,), device_id_type=MESH)
    pl.semaphore_signal(barrier, inc=1, device_id=(y_peer,), device_id_type=MESH)

    @pl.when(above)
    def _():
        pl.semaphore_signal(barrier, inc=1, device_id=(me + 8,), device_id_type=MESH)

    @pl.when(below)
    def _():
        pl.semaphore_signal(barrier, inc=1, device_id=(me - 8,), device_id_type=MESH)

    @pl.when(below & above)
    def _():
        pl.semaphore_wait(barrier, 4)

    @pl.when(~(below & above))
    def _():
        pl.semaphore_wait(barrier, 3)


def remote(src, dst, send, recv, peer):
    return pltpu.make_async_remote_copy(src_ref=src, dst_ref=dst, send_sem=send, recv_sem=recv,
                                        device_id=(peer,), device_id_type=MESH)


def shares(rows):
    small = rows * 9 // 78 // STEP * STEP
    return rows // 2 - small, small


def gather_kernel(mine, out, zs, zr, xs, xr, ys, yr, gs, gr, local_sem):
    me, x, y, z, far_x, far_y, x_peer, y_peer, below, above = place_of()
    big, small = shares(mine.shape[0])
    low, high, both = pl.ds(0, big), pl.ds(big, big), pl.ds(0, 2 * big)
    late = pl.ds(2 * big, 2 * small)
    late_x, late_y = pl.ds(2 * big, small), pl.ds(2 * big + small, small)
    planes = plane_order(z)

    def up(p, src):
        return remote(src.at[both], out.at[p, y, x, both], zs.at[UP, p], zr.at[UP, p], me + 8)

    def down(p, src):
        return remote(src.at[both], out.at[p, y, x, both], zs.at[DOWN, p], zr.at[DOWN, p], me - 8)

    def late_up(p):
        piece = out.at[p, :, :, late]
        return remote(piece, piece, zs.at[2, p], zr.at[2, p], me + 8)

    def late_down(p):
        piece = out.at[p, :, :, late]
        return remote(piece, piece, zs.at[3, p], zr.at[3, p], me - 8)

    def held(p):
        return out.at[p, y, x]

    def to_x(k, m, src, row, part):
        return remote(src, out.at[planes[k], row, x, part], xs.at[m, k], xr.at[m, k], x_peer)

    def to_y(k, m, src, col, part):
        return remote(src, out.at[planes[k], y, col, part], ys.at[m, k], yr.at[m, k], y_peer)

    def own_pieces(k):
        src = mine if k == 0 else held(planes[k])
        return (to_y(k, 0, src.at[low], x, low), to_x(k, 0, src.at[high], y, high),
                to_y(k, 1, src.at[high], x, high), to_x(k, 1, src.at[low], y, low))

    def second_x(k):
        return to_x(k, 2, out.at[planes[k], far_y, x, low], far_y, low)

    def second_y(k):
        return to_y(k, 2, out.at[planes[k], y, far_x, high], far_x, high)

    def from_x(k, m, row, part):
        spot = out.at[planes[k], row, far_x, part]
        return remote(spot, spot, xs.at[m, k], xr.at[m, k], x_peer)

    def from_y(k, m, col, part):
        spot = out.at[planes[k], far_y, col, part]
        return remote(spot, spot, ys.at[m, k], yr.at[m, k], y_peer)

    def late1_x():
        return remote(mine.at[late_x], out.at[z, y, x, late_x], *pair(gs, gr, 0), x_peer)

    def late1_y():
        return remote(mine.at[late_y], out.at[z, y, x, late_y], *pair(gs, gr, 1), y_peer)

    def late2_y():
        piece = out.at[z, y, :, late_x]
        return remote(piece, piece, *pair(gs, gr, 2), y_peer)

    def late2_x():
        piece = out.at[z, :, x, late_y]
        return remote(piece, piece, *pair(gs, gr, 3), x_peer)

    meet_neighbours(me, x_peer, y_peer, below, above)
    keep = pltpu.make_async_copy(mine, out.at[z, y, x], local_sem)
    keep.start()
    late1_x().start()
    late1_y().start()

    @pl.when(above)
    def _():
        up(z, mine).start()

    @pl.when(below)
    def _():
        down(z, mine).start()

    keep.wait()
    late1_x().wait_recv()
    late2_y().start()
    late1_y().wait_recv()
    late2_x().start()
    for piece in own_pieces(0):
        piece.start()

    def relay(k):
        from_y(k, 0, x, low).wait_recv()
        second_x(k).start()
        from_x(k, 0, y, high).wait_recv()
        second_y(k).start()

    def late_pass(k):
        p = planes[k]

        @pl.when(p < z)
        def _():
            late_up(p).wait_recv()

            @pl.when(above)
            def _():
                late_up(p).start()

        @pl.when(p > z)
        def _():
            late_down(p).wait_recv()

            @pl.when(below)
            def _():
                late_down(p).start()

    for k in range(1, 4):
        p = planes[k]

        @pl.when(p < z)
        def _():
            up(p, held(p)).wait_recv()

            @pl.when(above)
            def _():
                up(p, held(p)).start()

        @pl.when(p > z)
        def _():
            down(p, held(p)).wait_recv()

            @pl.when(below)
            def _():
                down(p, held(p)).start()

        for piece in own_pieces(k):
            piece.start()
        relay(k - 1)
        if k == 1:
            late2_y().wait_recv()
            late2_x().wait_recv()

            @pl.when(above)
            def _():
                late_up(z).start()

            @pl.when(below)
            def _():
                late_down(z).start()
        else:
            late_pass(k - 1)
    relay(3)
    late_pass(3)

    for piece in (late1_x(), late1_y(), late2_x(), late2_y()):
        piece.wait_send()
    for k in range(4):
        from_y(k, 1, x, high).wait_recv()
        from_x(k, 1, y, low).wait_recv()
        from_x(k, 2, far_y, low).wait_recv()
        from_y(k, 2, far_x, high).wait_recv()
        for piece in own_pieces(k):
            piece.wait_send()
        second_x(k).wait_send()
        second_y(k).wait_send()
        p = planes[k]

        @pl.when((p <= z) & above)
        def _():
            up(p, held(p)).wait_send()
            late_up(p).wait_send()

        @pl.when((p >= z) & below)
        def _():
            down(p, held(p)).wait_send()
            late_down(p).wait_send()


def gather_slots(mine):
    rows = mine.shape[0]
    dma = pltpu.SemaphoreType.DMA
    out = pl.pallas_call(
        gather_kernel,
        out_shape=jax.ShapeDtypeStruct((4, 2, 2, rows, LANES), jnp.float32),
        in_specs=[pl.BlockSpec(memory_space=pltpu.VMEM)],
        out_specs=pl.BlockSpec(memory_space=ANY),
        scratch_shapes=[dma((4, 4)), dma((4, 4)), *[dma((3, 4))] * 4,
                        dma((4,)), dma((4,)), dma],
        compiler_params=pltpu.CompilerParams(collective_id=1, has_side_effects=True),
        name='gather_slots')(mine)
    return out.reshape(16 * rows, LANES)


def scatter_kernel(parts, out, r1x, r1y, r2x, r2y, zu, zd, stage, lu, ld, held, ly2, lx1, lx2, ly1,
                   zs, zr, xs, xr, ys, yr, gs, gr, stage_sem, held_sem):
    me, x, y, z, far_x, far_y, x_peer, y_peer, below, above = place_of()
    half, small = shares(out.shape[0])
    low, high = pl.ds(0, half), pl.ds(half, half)
    late = pl.ds(2 * half, 2 * small)
    late_a, late_b = pl.ds(0, small), pl.ds(small, small)
    planes = plane_order(z)[::-1]

    def x1(k, h):
        row = far_y if h == 0 else y
        return remote(parts.at[planes[k], row, far_x, low], r1x.at[k, h], xs.at[h, k], xr.at[h, k], x_peer)

    def y1(k, h):
        col = far_x if h == 0 else x
        return remote(parts.at[planes[k], far_y, col, high], r1y.at[k, h], ys.at[h, k], yr.at[h, k], y_peer)

    def x2(k):
        return remote(r1y.at[k, 0], r2y.at[k], *pair(xs, xr, (LATE, k)), x_peer)

    def y2(k):
        return remote(r1x.at[k, 0], r2x.at[k], *pair(ys, yr, (LATE, k)), y_peer)

    def load(k, i):
        p = planes[k]
        src = (parts.at[p, far_y, x, low], parts.at[p, y, x, low],
               parts.at[p, y, far_x, high], parts.at[p, y, x, high])[i]
        return pltpu.make_async_copy(src, stage.at[i], stage_sem.at[i])

    def add(dst, *others):
        @pl.loop(0, half // STEP)
        def _(g):
            rows = block_of(g)
            value = dst[rows, :]
            for other in others:
                value = value + other[rows, :]
            dst[rows, :] = value

    def up(c, k, src):
        p = planes[k]
        return remote(src, zu.at[c, p - 1], zs.at[c, UP, p], zr.at[c, UP, p], me + 8)

    def down(c, k, src):
        p = planes[k]
        return remote(src, zd.at[c, p], zs.at[c, DOWN, p], zr.at[c, DOWN, p], me - 8)

    def late_load(p):
        return pltpu.make_async_copy(parts.at[p, :, :, late], held, held_sem)

    def late_up(p, src):
        return remote(src, lu.at[p - 1], zs.at[LATE, UP, p], zr.at[LATE, UP, p], me + 8)

    def late_down(p, src):
        return remote(src, ld.at[p], zs.at[LATE, DOWN, p], zr.at[LATE, DOWN, p], me - 8)

    def late_add(dst, src):
        @pl.loop(0, 2 * small // STEP)
        def _(g):
            rows = block_of(g)
            for i in range(2):
                for j in range(2):
                    dst[i, j, rows, :] = dst[i, j, rows, :] + src[i, j, rows, :]

    def small_add(dst, src):
        @pl.loop(0, small // STEP)
        def _(g):
            rows = block_of(g)
            dst[rows, :] = dst[rows, :] + src[rows, :]

    def late_stage(k):
        p = planes[k]
        if k < 3:
            @pl.when(below & above)
            def _():
                late_load(p).start()

            @pl.when((p > z) & below)
            def _():
                late_up(p, lu.at[p - 1]).wait_recv()
                late_load(p).wait()
                late_add(lu.at[p - 1], held)
                late_up(p, lu.at[p - 1]).start()

            @pl.when((p < z) & above)
            def _():
                late_down(p, ld.at[p]).wait_recv()
                late_load(p).wait()
                late_add(ld.at[p], held)
                late_down(p, ld.at[p]).start()
        else:
            late_load(p).start()
            late_load(p).wait()

            @pl.when(below)
            def _():
                late_up(p, lu.at[p - 1]).wait_recv()
                late_add(held, lu.at[p - 1])

            @pl.when(above)
            def _():
                late_down(p, ld.at[p]).wait_recv()
                late_add(held, ld.at[p])

    def late_y1():
        return remote(held.at[far_y, :, late_a], ly1, *pair(gs, gr, 0), y_peer)

    def late_x1():
        return remote(held.at[:, far_x, late_b], lx1, *pair(gs, gr, 1), x_peer)

    def late_x2():
        return remote(ly1.at[far_x], lx2, *pair(gs, gr, 2), x_peer)

    def late_y2():
        return remote(lx1.at[far_y], ly2, *pair(gs, gr, 3), y_peer)

    meet_neighbours(me, x_peer, y_peer, below, above)
    for k in range(3):
        p = planes[k]

        @pl.when(~below)
        def _():
            late_up(p, parts.at[p, :, :, late]).start()

        @pl.when(~above)
        def _():
            late_down(p, parts.at[p, :, :, late]).start()

    for i in range(4):
        load(0, i).start()
    for k in range(2):
        for h in range(2):
            x1(k, h).start()
            y1(k, h).start()

    def settle(c, k, total, first, i):
        p = planes[k]
        load(k, i).wait()
        add(total, first, stage.at[i])
        if k < 3:
            load(k + 1, i).start()

        @pl.when((p >= z) & below)
        def _():
            up(c, k, total).wait_recv()
            add(total, zu.at[c, p - 1])

        @pl.when((p <= z) & above)
        def _():
            down(c, k, total).wait_recv()
            add(total, zd.at[c, p])

    def move(c, k, total):
        p = planes[k]

        @pl.when(p > z)
        def _():
            up(c, k, total).start()

        @pl.when(p < z)
        def _():
            down(c, k, total).start()

    def finish(k):
        x1(k, 1).wait_recv()
        y2(k).wait_recv()
        settle(0, k, r2x.at[k], r1x.at[k, 1], 1)
        if k < 3:
            move(0, k, r2x.at[k])
        y1(k, 1).wait_recv()
        x2(k).wait_recv()
        settle(1, k, r2y.at[k], r1y.at[k, 1], 3)
        if k < 3:
            move(1, k, r2y.at[k])

    for k in range(4):
        x1(k, 0).wait_recv()
        load(k, 0).wait()
        add(r1x.at[k, 0], stage.at[0])
        y1(k, 0).wait_recv()
        load(k, 2).wait()
        add(r1y.at[k, 0], stage.at[2])
        if k < 3:
            load(k + 1, 0).start()
            load(k + 1, 2).start()
        y2(k).start()
        x2(k).start()
        if k + 2 < 4:
            for h in range(2):
                x1(k + 2, h).start()
                y1(k + 2, h).start()
        if k > 0:
            finish(k - 1)
            late_stage(k - 1)
    late_stage(3)
    late_y1().start()
    late_x1().start()
    finish(3)
    late_y1().wait_recv()
    late_x1().wait_recv()
    for i in range(2):
        small_add(ly1.at[i], held.at[y, i, late_a])
        small_add(lx1.at[i], held.at[i, x, late_b])

    @pl.loop(0, half // STEP)
    def _(g):
        rows = block_of(g)
        out[rows, :] = r2x[3, rows, :]
        out[block_of(g, half), :] = r2y[3, rows, :]

    late_x2().start()
    late_y2().start()
    late_x2().wait_recv()
    late_y2().wait_recv()

    @pl.loop(0, small // STEP)
    def _(g):
        rows = block_of(g)
        out[block_of(g, 2 * half), :] = ly1[x, rows, :] + lx2[rows, :]
        out[block_of(g, 2 * half + small), :] = lx1[y, rows, :] + ly2[rows, :]

    for piece in (late_x1(), late_y1(), late_x2(), late_y2()):
        piece.wait_send()

    for k in range(4):
        for h in range(2):
            x1(k, h).wait_send()
            y1(k, h).wait_send()
        x2(k).wait_send()
        y2(k).wait_send()
        if k < 3:
            p = planes[k]

            @pl.when(p > z)
            def _():
                late_up(p, lu.at[p - 1]).wait_send()

            @pl.when(p < z)
            def _():
                late_down(p, ld.at[p]).wait_send()

            for c, total in ((0, r2x.at[k]), (1, r2y.at[k])):
                @pl.when(p > z)
                def _():
                    up(c, k, total).wait_send()

                @pl.when(p < z)
                def _():
                    down(c, k, total).wait_send()


def scatter_slots(parts):
    rows = parts.shape[0] // 16
    dma = pltpu.SemaphoreType.DMA
    half, small = shares(rows)
    f32 = jnp.float32
    return pl.pallas_call(
        scatter_kernel,
        out_shape=jax.ShapeDtypeStruct((rows, LANES), f32),
        in_specs=[pl.BlockSpec(memory_space=ANY)],
        out_specs=pl.BlockSpec(memory_space=pltpu.VMEM),
        scratch_shapes=[*[pltpu.VMEM((4, 2, half, LANES), f32)] * 2, *[pltpu.VMEM((4, half, LANES), f32)] * 2,
                        *[pltpu.VMEM((2, 3, half, LANES), f32)] * 2, pltpu.VMEM((4, half, LANES), f32),
                        *[pltpu.VMEM((3, 2, 2, 2 * small, LANES), f32)] * 2,
                        pltpu.VMEM((2, 2, 2 * small, LANES), f32),
                        *[pltpu.VMEM((small, LANES), f32), pltpu.VMEM((2, small, LANES), f32)] * 2,
                        *[dma((3, 2, 4))] * 2, *[dma((3, 4))] * 4,
                        *[dma((4,))] * 3, dma],
        compiler_params=pltpu.CompilerParams(collective_id=2, has_side_effects=True,
                                             vmem_limit_bytes=63 * 1024 * 1024),
        name='scatter_slots')(parts.reshape(4, 2, 2, rows, LANES))


def solution(mesh):
    group = mesh.shape['ep']

    def device_step(table_in, table_out, centers, contexts, negatives):
        rows_dev, width = table_in.shape
        n_pairs, n_neg = negatives.shape
        n_ref = n_pairs * (n_neg + 1)
        me = lax.axis_index('ep')
        ids = jnp.arange(group, dtype=jnp.int32)
        partner = [(d, d + 1 - 2 * (d % 2)) for d in range(group)]
        other_out = lax.ppermute(table_out, 'ep', partner)

        all_centers = lax.all_to_all(jnp.broadcast_to(centers[None], (group, n_pairs)), 'ep', 0, 0).reshape(-1)
        all_owner = all_centers % group
        counts = jnp.sum((all_owner.reshape(group, n_pairs)[:, None, :] == ids[None, :, None]).astype(jnp.int32), axis=2)
        totals = jnp.sum(counts, axis=0)
        before = jnp.sum(jnp.where(ids[:, None] < me, counts, 0), axis=0)
        owner_c = centers % group
        one_hot = (owner_c[:, None] == ids[None, :])
        tri = (jnp.arange(n_pairs)[:, None] > jnp.arange(n_pairs)[None, :]).astype(jnp.bfloat16)
        earlier = jnp.dot(tri, one_hot.astype(jnp.bfloat16), preferred_element_type=jnp.float32).astype(jnp.int32)
        rank = jnp.sum(jnp.where(one_hot, earlier + before[None, :], 0), axis=1)
        place = jnp.arange(group * n_pairs, dtype=jnp.int32)
        big = jnp.int32(2 ** 31 - 1)
        mine = jnp.where(all_owner == me, place * rows_dev + all_centers // group, big)
        rows4 = (lax.sort(mine, is_stable=False)[:SLOTS] % rows_dev) * SUB
        u_mine = pick_rows(rows4, table_in)

        words = jnp.concatenate([contexts[:, None], negatives], axis=1)
        owner_o = words % group
        core_u = (owner_c % 2)[:, None]
        row_o = words // group + (owner_o + core_u) % 2 * rows_dev
        is_ctx = (jnp.arange(n_neg + 1) == 0).astype(jnp.int32)[None, :]
        block = (owner_c // 2)[:, None] * 2 + is_ctx
        code = (block * SLOTS + rank[:, None]) * (2 * rows_dev) + row_o
        fits = rank < SLOTS
        dest = jnp.where(fits[:, None], owner_o // 2 * 2 + core_u, group)
        dest_count = jnp.sum((dest.reshape(1, n_ref) == ids[:, None]).astype(jnp.int32), axis=1)
        roomy = jnp.max(dest_count) <= ROOM
        fits = fits & roomy
        dest = jnp.where(roomy, dest, group)
        dest_count = jnp.where(roomy, dest_count, 0)
        spare_dest = jnp.where(jnp.arange(ROOM)[None, :] < ROOM - dest_count[:, None], ids[:, None], group)
        keys = jnp.concatenate([dest.reshape(n_ref), spare_dest.reshape(group * ROOM)])
        vals = jnp.concatenate([code.reshape(n_ref), jnp.full((group * ROOM,), big)])
        _, vals = lax.sort((keys, vals), num_keys=1, is_stable=False)
        got = lax.all_to_all(vals[:group * ROOM].reshape(group, ROOM), 'ep', 0, 0)
        refs = lax.sort(got.reshape(group * ROOM), is_stable=False)
        edges = jnp.arange(group + 1, dtype=jnp.int32) * (SLOTS * rows_dev * 2)
        bounds = jnp.sum((refs[None, :] < edges[:, None]).astype(jnp.int32), axis=1)
        pad = jnp.zeros((BATCH,), jnp.int32)
        row4s = jnp.concatenate([refs % (2 * rows_dev) * SUB, pad])
        slot4s = jnp.concatenate([refs // (2 * rows_dev) % SLOTS * SUB, pad])

        u_all = gather_slots(u_mine)
        own_grad, other_grad, gu, loss = score_rows(bounds, row4s, slot4s, table_out, other_out, u_all)
        back_grad = lax.ppermute(other_grad, 'ep', partner)
        gu_mine = scatter_slots(gu)
        new_in = add_rows(rows4, table_in, gu_mine)
        new_out = finish_rows(table_out, own_grad, back_grad)
        loss = jnp.sum(loss[:, 0])
        overflow = jnp.sum((~fits).astype(jnp.int32))
        both = jnp.where(jnp.arange(LANES) == 0, loss, overflow.astype(jnp.float32))
        sums = jnp.sum(lax.all_to_all(jnp.broadcast_to(both[None], (group, LANES)), 'ep', 0, 0), axis=0)

        def more(state):
            return state[0] < jnp.where(sums[1] > 0.5, n_pairs // LEFT, 0)

        def again(state):
            turn, acc_in, acc_out, acc_loss = state

            def cut(a):
                return lax.all_gather(lax.dynamic_slice_in_dim(a, turn * LEFT, LEFT), 'ep', axis=0, tiled=True)

            word = jnp.concatenate([cut(centers)[:, None], cut(words)], axis=1)
            left = cut((~fits).astype(jnp.int32))[:, None] == 1
            held = word % group == me
            row = word // group
            found = jnp.concatenate([table_in[row[:, :1]], table_out[row[:, 1:]]], axis=1)
            found = lax.psum(jnp.where(held[:, :, None], found, 0.0), 'ep')
            u_vec, o_vec = found[:, 0], found[:, 1:]
            sign = jnp.where(is_ctx == 1, -1.0, 1.0)
            signed = sign * jnp.sum(u_vec[:, None, :] * o_vec, axis=-1)
            part = jnp.sum(jnp.where(left & (me == 0), -jax.nn.log_sigmoid(-signed), 0.0))
            gain = jnp.where(left, sign * jax.nn.sigmoid(signed), 0.0)
            goal = jnp.where(held & left, row, rows_dev)
            grad_u = jnp.sum(gain[:, :, None] * o_vec, axis=1)
            grad_o = gain[:, :, None] * u_vec[:, None, :]
            acc_in = acc_in.at[goal[:, 0]].add(-LEARN_RATE * grad_u, mode='drop')
            acc_out = acc_out.at[goal[:, 1:].reshape(-1)].add(-LEARN_RATE * grad_o.reshape(-1, width), mode='drop')
            return turn + 1, acc_in, acc_out, acc_loss + lax.psum(part, 'ep')

        _, new_in, new_out, total = lax.while_loop(more, again, (jnp.int32(0), new_in, new_out, sums[0]))
        return total / (n_pairs * group), new_in, new_out

    return jax.shard_map(device_step, mesh=mesh,
                         in_specs=(P('ep', None), P('ep', None), P('ep'), P('ep'), P('ep', None)),
                         out_specs=(P(), P('ep', None), P('ep', None)), check_vma=False)
```

```python
import functools

import jax
import jax.numpy as jnp
from jax import lax
from jax.experimental import pallas as pl
from jax.experimental.pallas import tpu as pltpu
from jax.sharding import PartitionSpec as P

LEARN_RATE = 0.5
LANES = 128
SUB = 4
TAIL = 500 - 3 * LANES
CHUNK = 512
SLOTS = 1248
BATCH = 64
UNROLL = 16
STEP = 64
UP, DOWN, LATE = range(3)
GATHER_PLAN = 'I0P0Z0Q0Z1P1R0J0Z2R1P2Z3P3Q1G0Q2G1R3Q3R2G2G3'
SCATTER_PLAN = 'O0N0N2E0L0A0N1N3E1O1L2F0E2A1A2O2L1L3F1O3A3F2M0F3'
ROOM = 768
LEFT = 32
ANY = pl.ANY
MESH = pl.DeviceIdType.MESH


def load_table(table, wide, stage, sems, first=0):
    rows = table.shape[0]
    n_chunks = rows // CHUNK

    def copy(k):
        return pltpu.make_async_copy(table.at[pl.ds(k * CHUNK, CHUNK)], stage.at[k % 2], sems.at[k % 2])

    copy(0).start()
    for k in range(n_chunks):
        if k + 1 < n_chunks:
            copy(k + 1).start()
        copy(k).wait()
        buf = stage.at[k % 2]

        @pl.loop(0, CHUNK // 32)
        def _(g):
            for i in range(4):
                r8 = pl.multiple_of((g * 4 + i) * 8, 8)
                w8 = pl.multiple_of((first + k * CHUNK + (g * 4 + i) * 8) * SUB, 32)
                for j in range(SUB):
                    if j < SUB - 1:
                        wide[pl.ds(w8 + j, 8, stride=SUB), :] = buf[pl.ds(r8, 8), j * LANES:(j + 1) * LANES]
                    else:
                        wide[pl.ds(w8 + j, 8, stride=SUB), :] = jnp.concatenate(
                            [buf[pl.ds(r8, 8), j * LANES:j * LANES + TAIL], jnp.zeros((8, LANES - TAIL), jnp.float32)],
                            axis=1)


def store_table(out, stage, sems, value):
    rows = out.shape[0]
    n_chunks = rows // CHUNK

    def copy(k):
        return pltpu.make_async_copy(stage.at[k % 2], out.at[pl.ds(k * CHUNK, CHUNK)], sems.at[k % 2])

    for k in range(n_chunks):
        if k >= 2:
            copy(k - 2).wait()
        buf = stage.at[k % 2]

        @pl.loop(0, CHUNK // 32)
        def _(g):
            for i in range(4):
                r8 = pl.multiple_of((g * 4 + i) * 8, 8)
                w8 = pl.multiple_of((k * CHUNK + (g * 4 + i) * 8) * SUB, 32)
                for j in range(SUB):
                    piece = value(w8, j)
                    if j < SUB - 1:
                        buf[pl.ds(r8, 8), j * LANES:(j + 1) * LANES] = piece
                    else:
                        buf[pl.ds(r8, 8), j * LANES:j * LANES + TAIL] = piece[:, :TAIL]

        copy(k).start()
    copy(n_chunks - 2).wait()
    copy(n_chunks - 1).wait()


def pick_kernel(rows4, table, out, wide, stage, sems):
    load_table(table, wide, stage, sems)

    @pl.loop(0, SLOTS // 16)
    def _(g):
        for i in range(16):
            k = g * 16 + i
            r4 = pl.multiple_of(rows4[k], SUB)
            out[pl.ds(pl.multiple_of(k * SUB, SUB), SUB), :] = wide[pl.ds(r4, SUB), :]


def pick_rows(rows4, table):
    return pl.pallas_call(
        pick_kernel,
        out_shape=jax.ShapeDtypeStruct((SLOTS * SUB, LANES), jnp.float32),
        grid_spec=pltpu.PrefetchScalarGridSpec(
            num_scalar_prefetch=1, grid=(1,),
            in_specs=[pl.BlockSpec(memory_space=ANY)],
            out_specs=pl.BlockSpec((SLOTS * SUB, LANES), lambda i, *_: (0, 0)),
            scratch_shapes=[pltpu.VMEM((table.shape[0] * SUB, LANES), jnp.float32),
                            pltpu.VMEM((2, CHUNK, table.shape[1]), jnp.float32),
                            pltpu.SemaphoreType.DMA((2,))]),
        name='pick_rows')(rows4, table)


def add_kernel(rows4, table, grads, out, wide, stage, sems):
    load_table(table, wide, stage, sems)

    @pl.loop(0, SLOTS // 16)
    def _(g):
        for i in range(16):
            k = g * 16 + i
            r4 = pl.multiple_of(rows4[k], SUB)
            wide[pl.ds(r4, SUB), :] = wide[pl.ds(r4, SUB), :] - LEARN_RATE * grads[pl.ds(pl.multiple_of(k * SUB, SUB), SUB), :]

    store_table(out, stage, sems, lambda w8, j: wide[pl.ds(w8 + j, 8, stride=SUB), :])


def add_rows(rows4, table, grads):
    return pl.pallas_call(
        add_kernel,
        out_shape=jax.ShapeDtypeStruct(table.shape, jnp.float32),
        grid_spec=pltpu.PrefetchScalarGridSpec(
            num_scalar_prefetch=1, grid=(1,),
            in_specs=[pl.BlockSpec(memory_space=ANY),
                      pl.BlockSpec((SLOTS * SUB, LANES), lambda i, *_: (0, 0))],
            out_specs=pl.BlockSpec(memory_space=ANY),
            scratch_shapes=[pltpu.VMEM((table.shape[0] * SUB, LANES), jnp.float32),
                            pltpu.VMEM((2, CHUNK, table.shape[1]), jnp.float32),
                            pltpu.SemaphoreType.DMA((2,))]),
        name='add_rows')(rows4, table, grads)


def score_kernel(bounds, row4s, slot4s, own, other, u_blk, own_grad, other_grad, gu_blk, loss_blk,
                 wide, grad, stage, sems, prods, coef):
    step = pl.program_id(0)
    rows = own.shape[0]

    @pl.when(step == 0)
    def _():
        load_table(own, wide, stage, sems)
        load_table(other, wide, stage, sems, rows)
        loss_blk[...] = jnp.zeros_like(loss_blk)

        @pl.loop(0, grad.shape[0] // 256)
        def _(g):
            grad[pl.ds(pl.multiple_of(g * 256, 256), 256), :] = jnp.zeros((256, LANES), jnp.float32)

    @pl.loop(0, SLOTS * SUB // 128)
    def _(g):
        gu_blk[pl.ds(pl.multiple_of(g * 128, 128), 128), :] = jnp.zeros((128, LANES), jnp.float32)

    begin, middle, end = bounds[2 * step], bounds[2 * step + 1], bounds[2 * step + 2]

    def spots(k):
        return pl.ds(pl.multiple_of(row4s[k], SUB), SUB), pl.ds(pl.multiple_of(slot4s[k], SUB), SUB)

    @pl.loop(0, (end - begin + BATCH - 1) // BATCH)
    def _(b):
        base = begin + b * BATCH

        @pl.loop(0, BATCH // UNROLL)
        def _(g):
            for i in range(UNROLL):
                k = g * UNROLL + i
                row, slot = spots(base + k)
                prods[pl.ds(pl.multiple_of(k * SUB, SUB), SUB), :] = u_blk[slot, :] * wide[row, :]

        part = prods[pl.ds(0, BATCH, stride=SUB), :]
        for j in range(1, SUB):
            part = part + prods[pl.ds(j, BATCH, stride=SUB), :]
        total = jnp.sum(part, axis=1, keepdims=True)
        number = lax.broadcasted_iota(jnp.int32, (BATCH, LANES), 0)
        sign = jnp.where(number < end - base, jnp.where(number < middle - base, 1.0, -1.0), 0.0)
        signed = sign * total
        small = jnp.exp(-jnp.abs(signed))
        loss = jnp.maximum(signed, 0.0) + jnp.log1p(small)
        loss_blk[...] += jnp.sum((jnp.abs(sign) * loss).reshape(BATCH // 8, 8, LANES), axis=0)
        gain = sign * jnp.where(signed >= 0, 1.0, small) / (1.0 + small)
        for j in range(SUB):
            coef[pl.ds(j, BATCH, stride=SUB), :] = gain

        @pl.loop(0, BATCH // UNROLL)
        def _(g):
            for i in range(0, UNROLL, 2):
                k = g * UNROLL + i
                row_a, slot_a = spots(base + k)
                row_b, slot_b = spots(base + k + 1)
                c_a = coef[pl.ds(pl.multiple_of(k * SUB, SUB), SUB), :]
                c_b = coef[pl.ds(pl.multiple_of((k + 1) * SUB, SUB), SUB), :]
                gu_a, gu_b = c_a * wide[row_a, :], c_b * wide[row_b, :]
                go_a, go_b = c_a * u_blk[slot_a, :], c_b * u_blk[slot_b, :]
                gu_b = gu_b + jnp.where(slot4s[base + k] == slot4s[base + k + 1], gu_a, 0.0)
                go_b = go_b + jnp.where(row4s[base + k] == row4s[base + k + 1], go_a, 0.0)
                gu_a, gu_b = gu_a + gu_blk[slot_a, :], gu_b + gu_blk[slot_b, :]
                go_a, go_b = go_a + grad[row_a, :], go_b + grad[row_b, :]
                gu_blk[slot_a, :] = gu_a
                grad[row_a, :] = go_a
                gu_blk[slot_b, :] = gu_b
                grad[row_b, :] = go_b

    @pl.when(step == pl.num_programs(0) - 1)
    def _():
        first = pltpu.make_async_copy(grad.at[pl.ds(0, rows * SUB)], own_grad, sems.at[0])
        second = pltpu.make_async_copy(grad.at[pl.ds(rows * SUB, rows * SUB)], other_grad, sems.at[1])
        first.start()
        second.start()
        first.wait()
        second.wait()


def score_rows(bounds, row4s, slot4s, own, other, u_all):
    rows, width = own.shape
    n_blocks = u_all.shape[0] // (SLOTS * SUB)
    blk = pl.BlockSpec((SLOTS * SUB, LANES), lambda i, *_: (i, 0))
    half = jax.ShapeDtypeStruct((rows * SUB, LANES), jnp.float32)
    return pl.pallas_call(
        score_kernel,
        out_shape=(half, half, jax.ShapeDtypeStruct(u_all.shape, jnp.float32),
                   jax.ShapeDtypeStruct((8, LANES), jnp.float32)),
        grid_spec=pltpu.PrefetchScalarGridSpec(
            num_scalar_prefetch=3, grid=(n_blocks,),
            in_specs=[pl.BlockSpec(memory_space=ANY), pl.BlockSpec(memory_space=ANY), blk],
            out_specs=(pl.BlockSpec(memory_space=ANY), pl.BlockSpec(memory_space=ANY), blk,
                       pl.BlockSpec((8, LANES), lambda i, *_: (0, 0))),
            scratch_shapes=[pltpu.VMEM((2 * rows * SUB, LANES), jnp.float32),
                            pltpu.VMEM((2 * rows * SUB, LANES), jnp.float32),
                            pltpu.VMEM((2, CHUNK, width), jnp.float32),
                            pltpu.SemaphoreType.DMA((2,)),
                            pltpu.VMEM((BATCH * SUB, LANES), jnp.float32),
                            pltpu.VMEM((BATCH * SUB, LANES), jnp.float32)]),
        compiler_params=pltpu.CompilerParams(vmem_limit_bytes=60 * 1024 * 1024),
        name='score_rows')(bounds, row4s, slot4s, own, other, u_all)


def finish_kernel(table, first, second, out):
    @pl.loop(0, CHUNK // 32)
    def _(g):
        for i in range(4):
            r8 = pl.multiple_of((g * 4 + i) * 8, 8)
            w8 = pl.multiple_of((g * 4 + i) * 8 * SUB, 32)
            for j in range(SUB):
                cols = slice(j * LANES, (j + 1) * LANES if j < SUB - 1 else j * LANES + TAIL)
                grad = first[pl.ds(w8 + j, 8, stride=SUB), :] + second[pl.ds(w8 + j, 8, stride=SUB), :]
                if j == SUB - 1:
                    grad = grad[:, :TAIL]
                out[pl.ds(r8, 8), cols] = table[pl.ds(r8, 8), cols] - LEARN_RATE * grad


def finish_rows(table, first, second):
    rows, width = table.shape
    native = pl.BlockSpec((CHUNK, width), lambda i: (i, 0))
    wide = pl.BlockSpec((CHUNK * SUB, LANES), lambda i: (i, 0))
    return pl.pallas_call(
        finish_kernel, out_shape=jax.ShapeDtypeStruct(table.shape, jnp.float32), grid=(rows // CHUNK,),
        in_specs=[native, wide, wide], out_specs=native, name='finish_rows')(table, first, second)


def place_of():
    me = lax.axis_index('ep')
    x, y, z = (me // 2) % 2, (me // 4) % 2, me // 8
    return me, x, y, z, 1 - x, 1 - y, me + 2 - 4 * x, me + 4 - 8 * y, z > 0, z < 3


def follow(plan, steps):
    for name, plane in zip(plan[::2], plan[1::2]):
        steps[name](int(plane))


def block_of(g, base=0):
    return pl.ds(pl.multiple_of(base + g * STEP, STEP), STEP)


def pair(sends, recvs, k):
    at = k if isinstance(k, tuple) else (k,)
    return sends.at[at], recvs.at[at]


def plane_order(z):
    far = 3 * (1 - z // 2)
    near = 1 + z % 2
    return z, near, 6 - far - near - z, far


def meet_neighbours(me, x_peer, y_peer, below, above):
    barrier = pltpu.get_barrier_semaphore()
    pl.semaphore_signal(barrier, inc=1, device_id=(x_peer,), device_id_type=MESH)
    pl.semaphore_signal(barrier, inc=1, device_id=(y_peer,), device_id_type=MESH)

    @pl.when(above)
    def _():
        pl.semaphore_signal(barrier, inc=1, device_id=(me + 8,), device_id_type=MESH)

    @pl.when(below)
    def _():
        pl.semaphore_signal(barrier, inc=1, device_id=(me - 8,), device_id_type=MESH)

    @pl.when(below & above)
    def _():
        pl.semaphore_wait(barrier, 4)

    @pl.when(~(below & above))
    def _():
        pl.semaphore_wait(barrier, 3)


def remote(src, dst, send, recv, peer):
    return pltpu.make_async_remote_copy(src_ref=src, dst_ref=dst, send_sem=send, recv_sem=recv,
                                        device_id=(peer,), device_id_type=MESH)


def shares(rows):
    small = rows * 4 // 39 // STEP * STEP
    return rows // 2 - small, small


def gather_kernel(mine, out, zs, zr, xs, xr, ys, yr, gs, gr, local_sem):
    me, x, y, z, far_x, far_y, x_peer, y_peer, below, above = place_of()
    big, small = shares(mine.shape[0])
    low, high, both = pl.ds(0, big), pl.ds(big, big), pl.ds(0, 2 * big)
    late = pl.ds(2 * big, 2 * small)
    late_x, late_y = pl.ds(2 * big, small), pl.ds(2 * big + small, small)
    planes = plane_order(z)

    def up(p, src):
        return remote(src.at[both], out.at[p, y, x, both], zs.at[UP, p], zr.at[UP, p], me + 8)

    def down(p, src):
        return remote(src.at[both], out.at[p, y, x, both], zs.at[DOWN, p], zr.at[DOWN, p], me - 8)

    def late_up(p):
        piece = out.at[p, :, :, late]
        return remote(piece, piece, zs.at[2, p], zr.at[2, p], me + 8)

    def late_down(p):
        piece = out.at[p, :, :, late]
        return remote(piece, piece, zs.at[3, p], zr.at[3, p], me - 8)

    def held(p):
        return out.at[p, y, x]

    def to_x(k, m, src, row, part):
        return remote(src, out.at[planes[k], row, x, part], xs.at[m, k], xr.at[m, k], x_peer)

    def to_y(k, m, src, col, part):
        return remote(src, out.at[planes[k], y, col, part], ys.at[m, k], yr.at[m, k], y_peer)

    def own_pieces(k):
        src = mine if k == 0 else held(planes[k])
        return (to_y(k, 0, src.at[low], x, low), to_x(k, 0, src.at[high], y, high),
                to_y(k, 1, src.at[high], x, high), to_x(k, 1, src.at[low], y, low))

    def second_x(k):
        return to_x(k, 2, out.at[planes[k], far_y, x, low], far_y, low)

    def second_y(k):
        return to_y(k, 2, out.at[planes[k], y, far_x, high], far_x, high)

    def from_x(k, m, row, part):
        spot = out.at[planes[k], row, far_x, part]
        return remote(spot, spot, xs.at[m, k], xr.at[m, k], x_peer)

    def from_y(k, m, col, part):
        spot = out.at[planes[k], far_y, col, part]
        return remote(spot, spot, ys.at[m, k], yr.at[m, k], y_peer)

    def late1_x():
        return remote(mine.at[late_x], out.at[z, y, x, late_x], *pair(gs, gr, 0), x_peer)

    def late1_y():
        return remote(mine.at[late_y], out.at[z, y, x, late_y], *pair(gs, gr, 1), y_peer)

    def late2_y():
        piece = out.at[z, y, :, late_x]
        return remote(piece, piece, *pair(gs, gr, 2), y_peer)

    def late2_x():
        piece = out.at[z, :, x, late_y]
        return remote(piece, piece, *pair(gs, gr, 3), x_peer)

    meet_neighbours(me, x_peer, y_peer, below, above)
    keep = pltpu.make_async_copy(mine, out.at[z, y, x], local_sem)
    keep.start()

    def late_out(k):
        late1_x().start()
        late1_y().start()

    def late_on(k):
        keep.wait()
        late1_x().wait_recv()
        late2_y().start()
        late1_y().wait_recv()
        late2_x().start()

    def along_z(k):
        p = planes[k]
        src = mine if k == 0 else held(p)

        @pl.when(p <= z)
        def _():
            if k > 0:
                up(p, src).wait_recv()

            @pl.when(above)
            def _():
                up(p, src).start()

        @pl.when(p >= z)
        def _():
            if k > 0:
                down(p, src).wait_recv()

            @pl.when(below)
            def _():
                down(p, src).start()

    def early_pieces(k):
        for piece in own_pieces(k)[:2]:
            piece.start()

    def other_pieces(k):
        for piece in own_pieces(k)[2:]:
            piece.start()

    def relay(k):
        from_y(k, 0, x, low).wait_recv()
        second_x(k).start()
        from_x(k, 0, y, high).wait_recv()
        second_y(k).start()

    def late_along_z(k):
        p = planes[k]
        if k == 0:
            late2_y().wait_recv()
            late2_x().wait_recv()

        @pl.when(p <= z)
        def _():
            if k > 0:
                late_up(p).wait_recv()

            @pl.when(above)
            def _():
                late_up(p).start()

        @pl.when(p >= z)
        def _():
            if k > 0:
                late_down(p).wait_recv()

            @pl.when(below)
            def _():
                late_down(p).start()

    follow(GATHER_PLAN, {'I': late_out, 'J': late_on, 'Z': along_z, 'P': early_pieces, 'Q': other_pieces,
                         'R': relay, 'G': late_along_z})
    for piece in (late1_x(), late1_y(), late2_x(), late2_y()):
        piece.wait_send()
    for k in range(4):
        from_y(k, 1, x, high).wait_recv()
        from_x(k, 1, y, low).wait_recv()
        from_x(k, 2, far_y, low).wait_recv()
        from_y(k, 2, far_x, high).wait_recv()
        for piece in own_pieces(k):
            piece.wait_send()
        second_x(k).wait_send()
        second_y(k).wait_send()
        p = planes[k]

        @pl.when((p <= z) & above)
        def _():
            up(p, held(p)).wait_send()
            late_up(p).wait_send()

        @pl.when((p >= z) & below)
        def _():
            down(p, held(p)).wait_send()
            late_down(p).wait_send()


def gather_slots(mine):
    rows = mine.shape[0]
    dma = pltpu.SemaphoreType.DMA
    out = pl.pallas_call(
        gather_kernel,
        out_shape=jax.ShapeDtypeStruct((4, 2, 2, rows, LANES), jnp.float32),
        in_specs=[pl.BlockSpec(memory_space=pltpu.VMEM)],
        out_specs=pl.BlockSpec(memory_space=ANY),
        scratch_shapes=[dma((4, 4)), dma((4, 4)), *[dma((3, 4))] * 4,
                        dma((4,)), dma((4,)), dma],
        compiler_params=pltpu.CompilerParams(collective_id=1, has_side_effects=True),
        name='gather_slots')(mine)
    return out.reshape(16 * rows, LANES)


def scatter_kernel(parts, out, r1x, r1y, r2x, r2y, zu, zd, stage, lu, ld, held, ly2, lx1, lx2, ly1,
                   zs, zr, xs, xr, ys, yr, gs, gr, stage_sem, held_sem):
    me, x, y, z, far_x, far_y, x_peer, y_peer, below, above = place_of()
    half, small = shares(out.shape[0])
    low, high = pl.ds(0, half), pl.ds(half, half)
    late = pl.ds(2 * half, 2 * small)
    late_a, late_b = pl.ds(0, small), pl.ds(small, small)
    planes = plane_order(z)[::-1]

    def x1(k, h):
        row = far_y if h == 0 else y
        return remote(parts.at[planes[k], row, far_x, low], r1x.at[k, h], xs.at[h, k], xr.at[h, k], x_peer)

    def y1(k, h):
        col = far_x if h == 0 else x
        return remote(parts.at[planes[k], far_y, col, high], r1y.at[k, h], ys.at[h, k], yr.at[h, k], y_peer)

    def x2(k):
        return remote(r1y.at[k, 0], r2y.at[k], *pair(xs, xr, (LATE, k)), x_peer)

    def y2(k):
        return remote(r1x.at[k, 0], r2x.at[k], *pair(ys, yr, (LATE, k)), y_peer)

    def load(k, i):
        p = planes[k]
        src = (parts.at[p, far_y, x, low], parts.at[p, y, x, low],
               parts.at[p, y, far_x, high], parts.at[p, y, x, high])[i]
        return pltpu.make_async_copy(src, stage.at[i], stage_sem.at[i])

    def add(dst, *others):
        @pl.loop(0, half // STEP)
        def _(g):
            rows = block_of(g)
            value = dst[rows, :]
            for other in others:
                value = value + other[rows, :]
            dst[rows, :] = value

    def up(c, k, src):
        p = planes[k]
        return remote(src, zu.at[c, p - 1], zs.at[c, UP, p], zr.at[c, UP, p], me + 8)

    def down(c, k, src):
        p = planes[k]
        return remote(src, zd.at[c, p], zs.at[c, DOWN, p], zr.at[c, DOWN, p], me - 8)

    def late_load(p):
        return pltpu.make_async_copy(parts.at[p, :, :, late], held, held_sem)

    def late_up(p, src):
        return remote(src, lu.at[p - 1], zs.at[LATE, UP, p], zr.at[LATE, UP, p], me + 8)

    def late_down(p, src):
        return remote(src, ld.at[p], zs.at[LATE, DOWN, p], zr.at[LATE, DOWN, p], me - 8)

    def late_add(dst, src):
        @pl.loop(0, 2 * small // STEP)
        def _(g):
            rows = block_of(g)
            for i in range(2):
                for j in range(2):
                    dst[i, j, rows, :] = dst[i, j, rows, :] + src[i, j, rows, :]

    def small_add(dst, src):
        @pl.loop(0, small // STEP)
        def _(g):
            rows = block_of(g)
            dst[rows, :] = dst[rows, :] + src[rows, :]

    def late_stage(k):
        p = planes[k]
        if k < 3:
            @pl.when(below & above)
            def _():
                late_load(p).start()

            @pl.when((p > z) & below)
            def _():
                late_up(p, lu.at[p - 1]).wait_recv()
                late_load(p).wait()
                late_add(lu.at[p - 1], held)
                late_up(p, lu.at[p - 1]).start()

            @pl.when((p < z) & above)
            def _():
                late_down(p, ld.at[p]).wait_recv()
                late_load(p).wait()
                late_add(ld.at[p], held)
                late_down(p, ld.at[p]).start()
        else:
            late_load(p).start()
            late_load(p).wait()

            @pl.when(below)
            def _():
                late_up(p, lu.at[p - 1]).wait_recv()
                late_add(held, lu.at[p - 1])

            @pl.when(above)
            def _():
                late_down(p, ld.at[p]).wait_recv()
                late_add(held, ld.at[p])

            late_y1().start()
            late_x1().start()

    def late_y1():
        return remote(held.at[far_y, :, late_a], ly1, *pair(gs, gr, 0), y_peer)

    def late_x1():
        return remote(held.at[:, far_x, late_b], lx1, *pair(gs, gr, 1), x_peer)

    def late_x2():
        return remote(ly1.at[far_x], lx2, *pair(gs, gr, 2), x_peer)

    def late_y2():
        return remote(lx1.at[far_y], ly2, *pair(gs, gr, 3), y_peer)

    meet_neighbours(me, x_peer, y_peer, below, above)
    for i in range(4):
        load(0, i).start()

    def settle(c, k, total, first, i):
        p = planes[k]
        load(k, i).wait()
        add(total, first, stage.at[i])
        if k < 3:
            load(k + 1, i).start()

        @pl.when((p >= z) & below)
        def _():
            up(c, k, total).wait_recv()
            add(total, zu.at[c, p - 1])

        @pl.when((p <= z) & above)
        def _():
            down(c, k, total).wait_recv()
            add(total, zd.at[c, p])

    def move(c, k, total):
        p = planes[k]

        @pl.when(p > z)
        def _():
            up(c, k, total).start()

        @pl.when(p < z)
        def _():
            down(c, k, total).start()

    def finish(k):
        x1(k, 1).wait_recv()
        y2(k).wait_recv()
        settle(0, k, r2x.at[k], r1x.at[k, 1], 1)
        if k < 3:
            move(0, k, r2x.at[k])
        y1(k, 1).wait_recv()
        x2(k).wait_recv()
        settle(1, k, r2y.at[k], r1y.at[k, 1], 3)
        if k < 3:
            move(1, k, r2y.at[k])

    def late_ends(k):
        p = planes[k]

        @pl.when(~below)
        def _():
            late_up(p, parts.at[p, :, :, late]).start()

        @pl.when(~above)
        def _():
            late_down(p, parts.at[p, :, :, late]).start()

    def first_pieces(k):
        x1(k, 0).start()
        y1(k, 0).start()

    def other_pieces(k):
        x1(k, 1).start()
        y1(k, 1).start()

    def turn_corner(k):
        x1(k, 0).wait_recv()
        load(k, 0).wait()
        add(r1x.at[k, 0], stage.at[0])
        y1(k, 0).wait_recv()
        load(k, 2).wait()
        add(r1y.at[k, 0], stage.at[2])
        if k < 3:
            load(k + 1, 0).start()
            load(k + 1, 2).start()
        y2(k).start()
        x2(k).start()

    def late_corner(k):
        late_y1().wait_recv()
        late_x1().wait_recv()
        for i in range(2):
            small_add(ly1.at[i], held.at[y, i, late_a])
            small_add(lx1.at[i], held.at[i, x, late_b])
        late_x2().start()
        late_y2().start()

    follow(SCATTER_PLAN, {'E': late_ends, 'N': first_pieces, 'O': other_pieces, 'A': turn_corner, 'F': finish,
                          'L': late_stage, 'M': late_corner})

    @pl.loop(0, half // STEP)
    def _(g):
        rows = block_of(g)
        out[rows, :] = r2x[3, rows, :]
        out[block_of(g, half), :] = r2y[3, rows, :]

    late_x2().wait_recv()
    late_y2().wait_recv()

    @pl.loop(0, small // STEP)
    def _(g):
        rows = block_of(g)
        out[block_of(g, 2 * half), :] = ly1[x, rows, :] + lx2[rows, :]
        out[block_of(g, 2 * half + small), :] = lx1[y, rows, :] + ly2[rows, :]

    for piece in (late_x1(), late_y1(), late_x2(), late_y2()):
        piece.wait_send()

    for k in range(4):
        for h in range(2):
            x1(k, h).wait_send()
            y1(k, h).wait_send()
        x2(k).wait_send()
        y2(k).wait_send()
        if k < 3:
            p = planes[k]

            @pl.when(p > z)
            def _():
                late_up(p, lu.at[p - 1]).wait_send()

            @pl.when(p < z)
            def _():
                late_down(p, ld.at[p]).wait_send()

            for c, total in ((0, r2x.at[k]), (1, r2y.at[k])):
                @pl.when(p > z)
                def _():
                    up(c, k, total).wait_send()

                @pl.when(p < z)
                def _():
                    down(c, k, total).wait_send()


def scatter_slots(parts):
    rows = parts.shape[0] // 16
    dma = pltpu.SemaphoreType.DMA
    half, small = shares(rows)
    f32 = jnp.float32
    return pl.pallas_call(
        scatter_kernel,
        out_shape=jax.ShapeDtypeStruct((rows, LANES), f32),
        in_specs=[pl.BlockSpec(memory_space=ANY)],
        out_specs=pl.BlockSpec(memory_space=pltpu.VMEM),
        scratch_shapes=[*[pltpu.VMEM((4, 2, half, LANES), f32)] * 2, *[pltpu.VMEM((4, half, LANES), f32)] * 2,
                        *[pltpu.VMEM((2, 3, half, LANES), f32)] * 2, pltpu.VMEM((4, half, LANES), f32),
                        *[pltpu.VMEM((3, 2, 2, 2 * small, LANES), f32)] * 2,
                        pltpu.VMEM((2, 2, 2 * small, LANES), f32),
                        *[pltpu.VMEM((small, LANES), f32), pltpu.VMEM((2, small, LANES), f32)] * 2,
                        *[dma((3, 2, 4))] * 2, *[dma((3, 4))] * 4,
                        *[dma((4,))] * 3, dma],
        compiler_params=pltpu.CompilerParams(collective_id=2, has_side_effects=True,
                                             vmem_limit_bytes=63 * 1024 * 1024),
        name='scatter_slots')(parts.reshape(4, 2, 2, rows, LANES))


def solution(mesh):
    group = mesh.shape['ep']

    def device_step(table_in, table_out, centers, contexts, negatives):
        rows_dev, width = table_in.shape
        n_pairs, n_neg = negatives.shape
        n_ref = n_pairs * (n_neg + 1)
        me = lax.axis_index('ep')
        ids = jnp.arange(group, dtype=jnp.int32)
        partner = [(d, d + 1 - 2 * (d % 2)) for d in range(group)]
        other_out = lax.ppermute(table_out, 'ep', partner)

        all_centers = lax.all_to_all(jnp.broadcast_to(centers[None], (group, n_pairs)), 'ep', 0, 0).reshape(-1)
        all_owner = all_centers % group
        counts = jnp.sum((all_owner.reshape(group, n_pairs)[:, None, :] == ids[None, :, None]).astype(jnp.int32), axis=2)
        totals = jnp.sum(counts, axis=0)
        before = jnp.sum(jnp.where(ids[:, None] < me, counts, 0), axis=0)
        owner_c = centers % group
        one_hot = (owner_c[:, None] == ids[None, :])
        tri = (jnp.arange(n_pairs)[:, None] > jnp.arange(n_pairs)[None, :]).astype(jnp.bfloat16)
        earlier = jnp.dot(tri, one_hot.astype(jnp.bfloat16), preferred_element_type=jnp.float32).astype(jnp.int32)
        rank = jnp.sum(jnp.where(one_hot, earlier + before[None, :], 0), axis=1)
        place = jnp.arange(group * n_pairs, dtype=jnp.int32)
        big = jnp.int32(2 ** 31 - 1)
        mine = jnp.where(all_owner == me, place * rows_dev + all_centers // group, big)
        rows4 = (lax.sort(mine, is_stable=False)[:SLOTS] % rows_dev) * SUB
        u_mine = pick_rows(rows4, table_in)

        words = jnp.concatenate([contexts[:, None], negatives], axis=1)
        owner_o = words % group
        core_u = (owner_c % 2)[:, None]
        row_o = words // group + (owner_o + core_u) % 2 * rows_dev
        is_ctx = (jnp.arange(n_neg + 1) == 0).astype(jnp.int32)[None, :]
        block = (owner_c // 2)[:, None] * 2 + is_ctx
        code = (block * SLOTS + rank[:, None]) * (2 * rows_dev) + row_o
        fits = rank < SLOTS
        dest = jnp.where(fits[:, None], owner_o // 2 * 2 + core_u, group)
        dest_count = jnp.sum((dest.reshape(1, n_ref) == ids[:, None]).astype(jnp.int32), axis=1)
        roomy = jnp.max(dest_count) <= ROOM
        fits = fits & roomy
        dest = jnp.where(roomy, dest, group)
        dest_count = jnp.where(roomy, dest_count, 0)
        spare_dest = jnp.where(jnp.arange(ROOM)[None, :] < ROOM - dest_count[:, None], ids[:, None], group)
        keys = jnp.concatenate([dest.reshape(n_ref), spare_dest.reshape(group * ROOM)])
        vals = jnp.concatenate([code.reshape(n_ref), jnp.full((group * ROOM,), big)])
        _, vals = lax.sort((keys, vals), num_keys=1, is_stable=False)
        got = lax.all_to_all(vals[:group * ROOM].reshape(group, ROOM), 'ep', 0, 0)
        refs = lax.sort(got.reshape(group * ROOM), is_stable=False)
        edges = jnp.arange(group + 1, dtype=jnp.int32) * (SLOTS * rows_dev * 2)
        bounds = jnp.sum((refs[None, :] < edges[:, None]).astype(jnp.int32), axis=1)
        pad = jnp.zeros((BATCH,), jnp.int32)
        row4s = jnp.concatenate([refs % (2 * rows_dev) * SUB, pad])
        slot4s = jnp.concatenate([refs // (2 * rows_dev) % SLOTS * SUB, pad])

        u_all = gather_slots(u_mine)
        own_grad, other_grad, gu, loss = score_rows(bounds, row4s, slot4s, table_out, other_out, u_all)
        back_grad = lax.ppermute(other_grad, 'ep', partner)
        gu_mine = scatter_slots(gu)
        new_in = add_rows(rows4, table_in, gu_mine)
        new_out = finish_rows(table_out, own_grad, back_grad)
        loss = jnp.sum(loss[:, 0])
        overflow = jnp.sum((~fits).astype(jnp.int32))
        both = jnp.where(jnp.arange(LANES) == 0, loss, overflow.astype(jnp.float32))
        sums = jnp.sum(lax.all_to_all(jnp.broadcast_to(both[None], (group, LANES)), 'ep', 0, 0), axis=0)

        def more(state):
            return state[0] < jnp.where(sums[1] > 0.5, n_pairs // LEFT, 0)

        def again(state):
            turn, acc_in, acc_out, acc_loss = state

            def cut(a):
                return lax.all_gather(lax.dynamic_slice_in_dim(a, turn * LEFT, LEFT), 'ep', axis=0, tiled=True)

            word = jnp.concatenate([cut(centers)[:, None], cut(words)], axis=1)
            left = cut((~fits).astype(jnp.int32))[:, None] == 1
            held = word % group == me
            row = word // group
            found = jnp.concatenate([table_in[row[:, :1]], table_out[row[:, 1:]]], axis=1)
            found = lax.psum(jnp.where(held[:, :, None], found, 0.0), 'ep')
            u_vec, o_vec = found[:, 0], found[:, 1:]
            sign = jnp.where(is_ctx == 1, -1.0, 1.0)
            signed = sign * jnp.sum(u_vec[:, None, :] * o_vec, axis=-1)
            part = jnp.sum(jnp.where(left & (me == 0), -jax.nn.log_sigmoid(-signed), 0.0))
            gain = jnp.where(left, sign * jax.nn.sigmoid(signed), 0.0)
            goal = jnp.where(held & left, row, rows_dev)
            grad_u = jnp.sum(gain[:, :, None] * o_vec, axis=1)
            grad_o = gain[:, :, None] * u_vec[:, None, :]
            acc_in = acc_in.at[goal[:, 0]].add(-LEARN_RATE * grad_u, mode='drop')
            acc_out = acc_out.at[goal[:, 1:].reshape(-1)].add(-LEARN_RATE * grad_o.reshape(-1, width), mode='drop')
            return turn + 1, acc_in, acc_out, acc_loss + lax.psum(part, 'ep')

        _, new_in, new_out, total = lax.while_loop(more, again, (jnp.int32(0), new_in, new_out, sums[0]))
        return total / (n_pairs * group), new_in, new_out

    return jax.shard_map(device_step, mesh=mesh,
                         in_specs=(P('ep', None), P('ep', None), P('ep'), P('ep'), P('ep', None)),
                         out_specs=(P(), P('ep', None), P('ep', None)), check_vma=False)
```

```python
import functools

import jax
import jax.numpy as jnp
from jax import lax
from jax.experimental import pallas as pl
from jax.experimental.pallas import tpu as pltpu
from jax.sharding import PartitionSpec as P

LEARN_RATE = 0.5
LANES = 128
TILE = 8
SUB = 4
TAIL = 500 - 3 * LANES
CHUNK = 512
SLOTS = 1248
BATCH = 64
UNROLL = 16
STEP = 64
COLS = 256
TURNS = 4
UP, DOWN, LATE = range(3)
GATHER_PLAN = 'Z0P0Q0I0X0R0Z1J0P1X1Z2G0P2Q2X2Q1R2Z3P3G1X3X4Q3G2R1R3X5X6X7G3'
SCATTER_PLAN = 'O0N0N2E0A0E1N3N1L0X0O1L2X1F0E2L1A1A2F1X2O2L3X3O3A3F2M0F3'
ROOM = 768
LEFT = 32
ANY = pl.ANY
MESH = pl.DeviceIdType.MESH


def load_table(table, wide, stage, sems):
    rows = table.shape[0]
    n_chunks = rows // CHUNK

    def copy(k):
        return pltpu.make_async_copy(table.at[pl.ds(k * CHUNK, CHUNK)], stage.at[k % 2], sems.at[k % 2])

    copy(0).start()
    for k in range(n_chunks):
        if k + 1 < n_chunks:
            copy(k + 1).start()
        copy(k).wait()
        buf = stage.at[k % 2]

        @pl.loop(0, CHUNK // (TILE * SUB))
        def _(g):
            for i in range(SUB):
                r8 = pl.multiple_of((g * SUB + i) * TILE, TILE)
                w8 = pl.multiple_of((k * CHUNK + (g * SUB + i) * TILE) * SUB, (TILE * SUB))
                for j in range(SUB):
                    if j < SUB - 1:
                        wide[pl.ds(w8 + j, TILE, stride=SUB), :] = buf[pl.ds(r8, TILE), j * LANES:(j + 1) * LANES]
                    else:
                        wide[pl.ds(w8 + j, TILE, stride=SUB), :] = jnp.concatenate(
                            [buf[pl.ds(r8, TILE), j * LANES:j * LANES + TAIL], jnp.zeros((TILE, LANES - TAIL), jnp.float32)],
                            axis=1)


def store_table(out, stage, sems, value):
    rows = out.shape[0]
    n_chunks = rows // CHUNK

    def copy(k):
        return pltpu.make_async_copy(stage.at[k % 2], out.at[pl.ds(k * CHUNK, CHUNK)], sems.at[k % 2])

    for k in range(n_chunks):
        if k >= 2:
            copy(k - 2).wait()
        buf = stage.at[k % 2]

        @pl.loop(0, CHUNK // (TILE * SUB))
        def _(g):
            for i in range(SUB):
                r8 = pl.multiple_of((g * SUB + i) * TILE, TILE)
                w8 = pl.multiple_of((k * CHUNK + (g * SUB + i) * TILE) * SUB, (TILE * SUB))
                for j in range(SUB):
                    piece = value(w8, j)
                    if j < SUB - 1:
                        buf[pl.ds(r8, TILE), j * LANES:(j + 1) * LANES] = piece
                    else:
                        buf[pl.ds(r8, TILE), j * LANES:j * LANES + TAIL] = piece[:, :TAIL]

        copy(k).start()
    copy(n_chunks - 2).wait()
    copy(n_chunks - 1).wait()


def pick_kernel(rows4, table, out, wide, stage, sems):
    load_table(table, wide, stage, sems)

    @pl.loop(0, SLOTS // UNROLL)
    def _(g):
        for i in range(UNROLL):
            k = g * UNROLL + i
            r4 = pl.multiple_of(rows4[k], SUB)
            out[pl.ds(pl.multiple_of(k * SUB, SUB), SUB), :] = wide[pl.ds(r4, SUB), :]


def pick_rows(rows4, table):
    return pl.pallas_call(
        pick_kernel,
        out_shape=jax.ShapeDtypeStruct((SLOTS * SUB, LANES), jnp.float32),
        grid_spec=pltpu.PrefetchScalarGridSpec(
            num_scalar_prefetch=1, grid=(1,),
            in_specs=[pl.BlockSpec(memory_space=ANY)],
            out_specs=pl.BlockSpec((SLOTS * SUB, LANES), lambda i, *_: (0, 0)),
            scratch_shapes=[pltpu.VMEM((table.shape[0] * SUB, LANES), jnp.float32),
                            pltpu.VMEM((2, CHUNK, table.shape[1]), jnp.float32),
                            pltpu.SemaphoreType.DMA((2,))]),
        name='pick_rows')(rows4, table)


def add_kernel(rows4, table, grads, out, wide, stage, sems):
    load_table(table, wide, stage, sems)

    @pl.loop(0, SLOTS // UNROLL)
    def _(g):
        for i in range(UNROLL):
            k = g * UNROLL + i
            r4 = pl.multiple_of(rows4[k], SUB)
            wide[pl.ds(r4, SUB), :] = wide[pl.ds(r4, SUB), :] - LEARN_RATE * grads[pl.ds(pl.multiple_of(k * SUB, SUB), SUB), :]

    store_table(out, stage, sems, lambda w8, j: wide[pl.ds(w8 + j, 8, stride=SUB), :])


def add_rows(rows4, table, grads):
    return pl.pallas_call(
        add_kernel,
        out_shape=jax.ShapeDtypeStruct(table.shape, jnp.float32),
        grid_spec=pltpu.PrefetchScalarGridSpec(
            num_scalar_prefetch=1, grid=(1,),
            in_specs=[pl.BlockSpec(memory_space=ANY),
                      pl.BlockSpec((SLOTS * SUB, LANES), lambda i, *_: (0, 0))],
            out_specs=pl.BlockSpec(memory_space=ANY),
            scratch_shapes=[pltpu.VMEM((table.shape[0] * SUB, LANES), jnp.float32),
                            pltpu.VMEM((2, CHUNK, table.shape[1]), jnp.float32),
                            pltpu.SemaphoreType.DMA((2,))]),
        name='add_rows')(rows4, table, grads)


def score_kernel(bounds, row4s, slot4s, tables, u_blk, own_grad, other_grad, gu_blk, loss_blk,
                 wide, grad, sems, prods, coef):
    step = pl.program_id(0)

    @pl.when(step == 0)
    def _():
        whole = pltpu.make_async_copy(tables, wide, sems.at[0])
        whole.start()
        loss_blk[...] = jnp.zeros_like(loss_blk)

        @pl.loop(0, grad.shape[0] // COLS)
        def _(g):
            grad[pl.ds(pl.multiple_of(g * COLS, COLS), COLS), :] = jnp.zeros((COLS, LANES), jnp.float32)

        whole.wait()

    @pl.loop(0, SLOTS * SUB // 128)
    def _(g):
        gu_blk[pl.ds(pl.multiple_of(g * 128, 128), 128), :] = jnp.zeros((128, LANES), jnp.float32)

    begin, middle, end = bounds[2 * step], bounds[2 * step + 1], bounds[2 * step + 2]

    def spots(k):
        return pl.ds(pl.multiple_of(row4s[k], SUB), SUB), pl.ds(pl.multiple_of(slot4s[k], SUB), SUB)

    @pl.loop(0, (end - begin + BATCH - 1) // BATCH)
    def _(b):
        base = begin + b * BATCH

        @pl.loop(0, BATCH // UNROLL)
        def _(g):
            for i in range(UNROLL):
                k = g * UNROLL + i
                row, slot = spots(base + k)
                prods[pl.ds(pl.multiple_of(k * SUB, SUB), SUB), :] = u_blk[slot, :] * wide[row, :]

        part = prods[pl.ds(0, BATCH, stride=SUB), :]
        for j in range(1, SUB):
            part = part + prods[pl.ds(j, BATCH, stride=SUB), :]
        total = jnp.sum(part, axis=1, keepdims=True)
        number = lax.broadcasted_iota(jnp.int32, (BATCH, LANES), 0)
        sign = jnp.where(number < end - base, jnp.where(number < middle - base, 1.0, -1.0), 0.0)
        signed = sign * total
        small = jnp.exp(-jnp.abs(signed))
        loss = jnp.maximum(signed, 0.0) + jnp.log1p(small)
        loss_blk[...] += jnp.sum((jnp.abs(sign) * loss).reshape(BATCH // 8, 8, LANES), axis=0)
        gain = sign * jnp.where(signed >= 0, 1.0, small) / (1.0 + small)
        for j in range(SUB):
            coef[pl.ds(j, BATCH, stride=SUB), :] = gain

        @pl.loop(0, BATCH // UNROLL)
        def _(g):
            for i in range(0, UNROLL, 2):
                k = g * UNROLL + i
                row_a, slot_a = spots(base + k)
                row_b, slot_b = spots(base + k + 1)
                c_a = coef[pl.ds(pl.multiple_of(k * SUB, SUB), SUB), :]
                c_b = coef[pl.ds(pl.multiple_of((k + 1) * SUB, SUB), SUB), :]
                gu_a, gu_b = c_a * wide[row_a, :], c_b * wide[row_b, :]
                go_a, go_b = c_a * u_blk[slot_a, :], c_b * u_blk[slot_b, :]
                gu_b = gu_b + jnp.where(slot4s[base + k] == slot4s[base + k + 1], gu_a, 0.0)
                go_b = go_b + jnp.where(row4s[base + k] == row4s[base + k + 1], go_a, 0.0)
                gu_a, gu_b = gu_a + gu_blk[slot_a, :], gu_b + gu_blk[slot_b, :]
                go_a, go_b = go_a + grad[row_a, :], go_b + grad[row_b, :]
                gu_blk[slot_a, :] = gu_a
                grad[row_a, :] = go_a
                gu_blk[slot_b, :] = gu_b
                grad[row_b, :] = go_b

    @pl.when(step == pl.num_programs(0) - 1)
    def _():
        half = own_grad.shape[0]
        first = pltpu.make_async_copy(grad.at[pl.ds(0, half)], own_grad, sems.at[0])
        second = pltpu.make_async_copy(grad.at[pl.ds(half, half)], other_grad, sems.at[1])
        first.start()
        second.start()
        first.wait()
        second.wait()


def score_rows(bounds, row4s, slot4s, tables, u_all):
    n_blocks = u_all.shape[0] // (SLOTS * SUB)
    blk = pl.BlockSpec((SLOTS * SUB, LANES), lambda i, *_: (i, 0))
    half = jax.ShapeDtypeStruct((tables.shape[0] // 2, LANES), jnp.float32)
    return pl.pallas_call(
        score_kernel,
        out_shape=(half, half, jax.ShapeDtypeStruct(u_all.shape, jnp.float32),
                   jax.ShapeDtypeStruct((8, LANES), jnp.float32)),
        grid_spec=pltpu.PrefetchScalarGridSpec(
            num_scalar_prefetch=3, grid=(n_blocks,),
            in_specs=[pl.BlockSpec(memory_space=ANY), blk],
            out_specs=(pl.BlockSpec(memory_space=ANY), pl.BlockSpec(memory_space=ANY), blk,
                       pl.BlockSpec((8, LANES), lambda i, *_: (0, 0))),
            scratch_shapes=[*[pltpu.VMEM(tables.shape, jnp.float32)] * 2, pltpu.SemaphoreType.DMA((2,)),
                            pltpu.VMEM((BATCH * SUB, LANES), jnp.float32),
                            pltpu.VMEM((BATCH * SUB, LANES), jnp.float32)]),
        compiler_params=pltpu.CompilerParams(vmem_limit_bytes=60 * 1024 * 1024),
        name='score_rows')(bounds, row4s, slot4s, tables, u_all)


def place_of():
    me = lax.axis_index('ep')
    x, y, z = (me // 2) % 2, (me // 4) % 2, me // 8
    return me, x, y, z, 1 - x, 1 - y, me + 2 - 4 * x, me + 4 - 8 * y, z > 0, z < 3


def follow(plan, steps):
    for name, plane in zip(plan[::2], plan[1::2]):
        steps[name](int(plane))


def block_of(g, base=0):
    return pl.ds(pl.multiple_of(base + g * STEP, STEP), STEP)


def pair(sends, recvs, k):
    at = k if isinstance(k, tuple) else (k,)
    return sends.at[at], recvs.at[at]


def plane_order(z):
    far = 3 * (1 - z // 2)
    near = 1 + z % 2
    return z, near, 6 - far - near - z, far


def meet_neighbours(me, x_peer, y_peer, below, above, partner=None):
    barrier = pltpu.get_barrier_semaphore()
    extra = int(partner is not None)
    if extra:
        pl.semaphore_signal(barrier, inc=1, device_id=(partner,), device_id_type=MESH)
    pl.semaphore_signal(barrier, inc=1, device_id=(x_peer,), device_id_type=MESH)
    pl.semaphore_signal(barrier, inc=1, device_id=(y_peer,), device_id_type=MESH)

    @pl.when(above)
    def _():
        pl.semaphore_signal(barrier, inc=1, device_id=(me + 8,), device_id_type=MESH)

    @pl.when(below)
    def _():
        pl.semaphore_signal(barrier, inc=1, device_id=(me - 8,), device_id_type=MESH)

    @pl.when(below & above)
    def _():
        pl.semaphore_wait(barrier, 4 + extra)

    @pl.when(~(below & above))
    def _():
        pl.semaphore_wait(barrier, 3 + extra)


def remote(src, dst, send, recv, peer):
    return pltpu.make_async_remote_copy(src_ref=src, dst_ref=dst, send_sem=send, recv_sem=recv,
                                        device_id=(peer,), device_id_type=MESH)


def shares(rows):
    small = rows * 4 // 39 // STEP * STEP
    return rows // 2 - small, small


def gather_kernel(mine, own_t, other_t, out, tables, cols, rows, in_sem, out_sem,
                  zs, zr, xs, xr, ys, yr, gs, gr, local_sem):
    me, x, y, z, far_x, far_y, x_peer, y_peer, below, above = place_of()
    big, small = shares(mine.shape[0])
    low, high, both = pl.ds(0, big), pl.ds(big, big), pl.ds(0, 2 * big)
    late = pl.ds(2 * big, 2 * small)
    late_x, late_y = pl.ds(2 * big, small), pl.ds(2 * big + small, small)
    planes = plane_order(z)

    def up(p, src):
        return remote(src.at[both], out.at[p, y, x, both], zs.at[UP, p], zr.at[UP, p], me + 8)

    def down(p, src):
        return remote(src.at[both], out.at[p, y, x, both], zs.at[DOWN, p], zr.at[DOWN, p], me - 8)

    def late_up(p):
        piece = out.at[p, :, :, late]
        return remote(piece, piece, zs.at[2, p], zr.at[2, p], me + 8)

    def late_down(p):
        piece = out.at[p, :, :, late]
        return remote(piece, piece, zs.at[3, p], zr.at[3, p], me - 8)

    def held(p):
        return out.at[p, y, x]

    def to_x(k, m, src, row, part):
        return remote(src, out.at[planes[k], row, x, part], xs.at[m, k], xr.at[m, k], x_peer)

    def to_y(k, m, src, col, part):
        return remote(src, out.at[planes[k], y, col, part], ys.at[m, k], yr.at[m, k], y_peer)

    def own_pieces(k):
        src = mine if k == 0 else held(planes[k])
        return (to_y(k, 0, src.at[low], x, low), to_x(k, 0, src.at[high], y, high),
                to_y(k, 1, src.at[high], x, high), to_x(k, 1, src.at[low], y, low))

    def second_x(k):
        return to_x(k, 2, out.at[planes[k], far_y, x, low], far_y, low)

    def second_y(k):
        return to_y(k, 2, out.at[planes[k], y, far_x, high], far_x, high)

    def from_x(k, m, row, part):
        spot = out.at[planes[k], row, far_x, part]
        return remote(spot, spot, xs.at[m, k], xr.at[m, k], x_peer)

    def from_y(k, m, col, part):
        spot = out.at[planes[k], far_y, col, part]
        return remote(spot, spot, ys.at[m, k], yr.at[m, k], y_peer)

    def late1_x():
        return remote(mine.at[late_x], out.at[z, y, x, late_x], *pair(gs, gr, 0), x_peer)

    def late1_y():
        return remote(mine.at[late_y], out.at[z, y, x, late_y], *pair(gs, gr, 1), y_peer)

    def late2_y():
        piece = out.at[z, y, :, late_x]
        return remote(piece, piece, *pair(gs, gr, 2), y_peer)

    def late2_x():
        piece = out.at[z, :, x, late_y]
        return remote(piece, piece, *pair(gs, gr, 3), x_peer)

    meet_neighbours(me, x_peer, y_peer, below, above)
    keep = pltpu.make_async_copy(mine, out.at[z, y, x], local_sem)
    keep.start()

    def late_out(k):
        late1_x().start()
        late1_y().start()

    def late_on(k):
        keep.wait()
        late1_x().wait_recv()
        late2_y().start()
        late1_y().wait_recv()
        late2_x().start()

    def along_z(k):
        p = planes[k]
        src = mine if k == 0 else held(p)

        @pl.when(p <= z)
        def _():
            if k > 0:
                up(p, src).wait_recv()

            @pl.when(above)
            def _():
                up(p, src).start()

        @pl.when(p >= z)
        def _():
            if k > 0:
                down(p, src).wait_recv()

            @pl.when(below)
            def _():
                down(p, src).start()

    def early_pieces(k):
        for piece in own_pieces(k)[:2]:
            piece.start()

    def other_pieces(k):
        for piece in own_pieces(k)[2:]:
            piece.start()

    def relay(k):
        from_y(k, 0, x, low).wait_recv()
        second_x(k).start()
        from_x(k, 0, y, high).wait_recv()
        second_y(k).start()

    def late_along_z(k):
        p = planes[k]
        if k == 0:
            late2_y().wait_recv()
            late2_x().wait_recv()

        @pl.when(p <= z)
        def _():
            if k > 0:
                late_up(p).wait_recv()

            @pl.when(above)
            def _():
                late_up(p).start()

        @pl.when(p >= z)
        def _():
            if k > 0:
                late_down(p).wait_recv()

            @pl.when(below)
            def _():
                late_down(p).start()

    def convert(k):
        source, first = (own_t, k) if k < TURNS else (other_t, k - TURNS)

        def fetch(t):
            at = pl.ds(pl.multiple_of((first * TURNS + t) * COLS, COLS), COLS)
            return pltpu.make_async_copy(source.at[:, at], cols.at[t % 2], in_sem.at[t % 2])

        def put(t):
            at = pl.ds(pl.multiple_of((k * TURNS + t) * COLS * SUB, COLS), COLS * SUB)
            return pltpu.make_async_copy(rows.at[t % 2], tables.at[at], out_sem.at[t % 2])

        fetch(0).start()

        @pl.loop(0, TURNS)
        def _(t):
            fetch(t).wait()

            @pl.when(t + 1 < TURNS)
            def _():
                fetch(t + 1).start()

            @pl.when(t > 1)
            def _():
                put(t - 2).wait()

            for h in range(COLS // LANES):
                for j in range(SUB):
                    width = LANES if j < SUB - 1 else TAIL
                    turned = cols[t % 2, j * LANES:j * LANES + width, h * LANES:(h + 1) * LANES].T
                    if width < LANES:
                        turned = jnp.concatenate([turned, jnp.zeros((LANES, LANES - width), jnp.float32)], axis=1)
                    rows[t % 2, pl.ds(h * LANES * SUB + j, LANES, stride=SUB), :] = turned
            put(t).start()

        put(TURNS - 2).wait()
        put(TURNS - 1).wait()

    follow(GATHER_PLAN, {'X': convert, 'I': late_out, 'J': late_on, 'Z': along_z, 'P': early_pieces, 'Q': other_pieces,
                         'R': relay, 'G': late_along_z})
    for piece in (late1_x(), late1_y(), late2_x(), late2_y()):
        piece.wait_send()
    for k in range(4):
        from_y(k, 1, x, high).wait_recv()
        from_x(k, 1, y, low).wait_recv()
        from_x(k, 2, far_y, low).wait_recv()
        from_y(k, 2, far_x, high).wait_recv()
        for piece in own_pieces(k):
            piece.wait_send()
        second_x(k).wait_send()
        second_y(k).wait_send()
        p = planes[k]

        @pl.when((p <= z) & above)
        def _():
            up(p, held(p)).wait_send()
            late_up(p).wait_send()

        @pl.when((p >= z) & below)
        def _():
            down(p, held(p)).wait_send()
            late_down(p).wait_send()


def gather_slots(mine, own_t, other_t):
    rows = mine.shape[0]
    width, words = own_t.shape
    dma = pltpu.SemaphoreType.DMA
    out, tables = pl.pallas_call(
        gather_kernel,
        out_shape=(jax.ShapeDtypeStruct((4, 2, 2, rows, LANES), jnp.float32),
                   jax.ShapeDtypeStruct((2 * words * SUB, LANES), jnp.float32)),
        in_specs=[pl.BlockSpec(memory_space=pltpu.VMEM), *[pl.BlockSpec(memory_space=ANY)] * 2],
        out_specs=(pl.BlockSpec(memory_space=ANY),) * 2,
        scratch_shapes=[pltpu.VMEM((2, width, COLS), jnp.float32), pltpu.VMEM((2, COLS * SUB, LANES), jnp.float32),
                        dma((2,)), dma((2,)), dma((4, 4)), dma((4, 4)), *[dma((3, 4))] * 4,
                        dma((4,)), dma((4,)), dma],
        compiler_params=pltpu.CompilerParams(collective_id=1, has_side_effects=True),
        name='gather_slots')(mine, own_t, other_t)
    return out.reshape(16 * rows, LANES), tables


def scatter_kernel(parts, tables, own_grad, other_grad, out, new_table, back, terms, fresh, term_sem, fresh_sem, swap_s, swap_r, r1x, r1y, r2x, r2y, zu, zd, stage, lu, ld, held, ly2, lx1, lx2, ly1,
                   zs, zr, xs, xr, ys, yr, gs, gr, stage_sem, held_sem):
    me, x, y, z, far_x, far_y, x_peer, y_peer, below, above = place_of()
    half, small = shares(out.shape[0])
    low, high = pl.ds(0, half), pl.ds(half, half)
    late = pl.ds(2 * half, 2 * small)
    late_a, late_b = pl.ds(0, small), pl.ds(small, small)
    planes = plane_order(z)[::-1]

    def x1(k, h):
        row = far_y if h == 0 else y
        return remote(parts.at[planes[k], row, far_x, low], r1x.at[k, h], xs.at[h, k], xr.at[h, k], x_peer)

    def y1(k, h):
        col = far_x if h == 0 else x
        return remote(parts.at[planes[k], far_y, col, high], r1y.at[k, h], ys.at[h, k], yr.at[h, k], y_peer)

    def x2(k):
        return remote(r1y.at[k, 0], r2y.at[k], *pair(xs, xr, (LATE, k)), x_peer)

    def y2(k):
        return remote(r1x.at[k, 0], r2x.at[k], *pair(ys, yr, (LATE, k)), y_peer)

    def load(k, i):
        p = planes[k]
        src = (parts.at[p, far_y, x, low], parts.at[p, y, x, low],
               parts.at[p, y, far_x, high], parts.at[p, y, x, high])[i]
        return pltpu.make_async_copy(src, stage.at[i], stage_sem.at[i])

    def add(dst, *others):
        @pl.loop(0, half // STEP)
        def _(g):
            rows = block_of(g)
            value = dst[rows, :]
            for other in others:
                value = value + other[rows, :]
            dst[rows, :] = value

    def up(c, k, src):
        p = planes[k]
        return remote(src, zu.at[c, p - 1], zs.at[c, UP, p], zr.at[c, UP, p], me + 8)

    def down(c, k, src):
        p = planes[k]
        return remote(src, zd.at[c, p], zs.at[c, DOWN, p], zr.at[c, DOWN, p], me - 8)

    def late_load(p):
        return pltpu.make_async_copy(parts.at[p, :, :, late], held, held_sem)

    def late_up(p, src):
        return remote(src, lu.at[p - 1], zs.at[LATE, UP, p], zr.at[LATE, UP, p], me + 8)

    def late_down(p, src):
        return remote(src, ld.at[p], zs.at[LATE, DOWN, p], zr.at[LATE, DOWN, p], me - 8)

    def late_add(dst, src):
        @pl.loop(0, 2 * small // STEP)
        def _(g):
            rows = block_of(g)
            for i in range(2):
                for j in range(2):
                    dst[i, j, rows, :] = dst[i, j, rows, :] + src[i, j, rows, :]

    def small_add(dst, src):
        @pl.loop(0, small // STEP)
        def _(g):
            rows = block_of(g)
            dst[rows, :] = dst[rows, :] + src[rows, :]

    def late_stage(k):
        p = planes[k]
        if k < 3:
            @pl.when(below & above)
            def _():
                late_load(p).start()

            @pl.when((p > z) & below)
            def _():
                late_up(p, lu.at[p - 1]).wait_recv()
                late_load(p).wait()
                late_add(lu.at[p - 1], held)
                late_up(p, lu.at[p - 1]).start()

            @pl.when((p < z) & above)
            def _():
                late_down(p, ld.at[p]).wait_recv()
                late_load(p).wait()
                late_add(ld.at[p], held)
                late_down(p, ld.at[p]).start()
        else:
            late_load(p).start()
            late_load(p).wait()

            @pl.when(below)
            def _():
                late_up(p, lu.at[p - 1]).wait_recv()
                late_add(held, lu.at[p - 1])

            @pl.when(above)
            def _():
                late_down(p, ld.at[p]).wait_recv()
                late_add(held, ld.at[p])

            late_y1().start()
            late_x1().start()

    def late_y1():
        return remote(held.at[far_y, :, late_a], ly1, *pair(gs, gr, 0), y_peer)

    def late_x1():
        return remote(held.at[:, far_x, late_b], lx1, *pair(gs, gr, 1), x_peer)

    def late_x2():
        return remote(ly1.at[far_x], lx2, *pair(gs, gr, 2), x_peer)

    def late_y2():
        return remote(lx1.at[far_y], ly2, *pair(gs, gr, 3), y_peer)

    partner = me + 1 - 2 * (me % 2)
    meet_neighbours(me, x_peer, y_peer, below, above, partner)
    swap = remote(other_grad, back, swap_s, swap_r, partner)
    swap.start()
    for i in range(4):
        load(0, i).start()

    def settle(c, k, total, first, i):
        p = planes[k]
        load(k, i).wait()
        add(total, first, stage.at[i])
        if k < 3:
            load(k + 1, i).start()

        @pl.when((p >= z) & below)
        def _():
            up(c, k, total).wait_recv()
            add(total, zu.at[c, p - 1])

        @pl.when((p <= z) & above)
        def _():
            down(c, k, total).wait_recv()
            add(total, zd.at[c, p])

    def move(c, k, total):
        p = planes[k]

        @pl.when(p > z)
        def _():
            up(c, k, total).start()

        @pl.when(p < z)
        def _():
            down(c, k, total).start()

    def finish(k):
        x1(k, 1).wait_recv()
        y2(k).wait_recv()
        settle(0, k, r2x.at[k], r1x.at[k, 1], 1)
        if k < 3:
            move(0, k, r2x.at[k])
        y1(k, 1).wait_recv()
        x2(k).wait_recv()
        settle(1, k, r2y.at[k], r1y.at[k, 1], 3)
        if k < 3:
            move(1, k, r2y.at[k])

    def late_ends(k):
        p = planes[k]

        @pl.when(~below)
        def _():
            late_up(p, parts.at[p, :, :, late]).start()

        @pl.when(~above)
        def _():
            late_down(p, parts.at[p, :, :, late]).start()

    def first_pieces(k):
        x1(k, 0).start()
        y1(k, 0).start()

    def other_pieces(k):
        x1(k, 1).start()
        y1(k, 1).start()

    def turn_corner(k):
        x1(k, 0).wait_recv()
        load(k, 0).wait()
        add(r1x.at[k, 0], stage.at[0])
        y1(k, 0).wait_recv()
        load(k, 2).wait()
        add(r1y.at[k, 0], stage.at[2])
        if k < 3:
            load(k + 1, 0).start()
            load(k + 1, 2).start()
        y2(k).start()
        x2(k).start()

    def late_corner(k):
        late_y1().wait_recv()
        late_x1().wait_recv()
        for i in range(2):
            small_add(ly1.at[i], held.at[y, i, late_a])
            small_add(lx1.at[i], held.at[i, x, late_b])
        late_x2().start()
        late_y2().start()

    def update(k):
        if k == 0:
            swap.wait_recv()

        def fetch(t):
            at = pl.ds(pl.multiple_of((k * TURNS + t) * COLS * SUB, COLS), COLS * SUB)
            return [pltpu.make_async_copy(ref.at[at], terms.at[i, t % 2], term_sem.at[i, t % 2])
                    for i, ref in enumerate((tables, own_grad, back))]

        def put(t):
            at = pl.ds(pl.multiple_of((k * TURNS + t) * COLS, COLS), COLS)
            return pltpu.make_async_copy(fresh.at[t % 2], new_table.at[at], fresh_sem.at[t % 2])

        for copy in fetch(0):
            copy.start()

        @pl.loop(0, TURNS)
        def _(t):
            for copy in fetch(t):
                copy.wait()

            @pl.when(t + 1 < TURNS)
            def _():
                for copy in fetch(t + 1):
                    copy.start()

            @pl.when(t > 1)
            def _():
                put(t - 2).wait()

            @pl.loop(0, COLS // TILE)
            def _(g):
                for j in range(SUB):
                    at = pl.ds(pl.multiple_of(g * TILE * SUB, TILE) + j, TILE, stride=SUB)
                    old, first, second = [terms[i, t % 2, at, :] for i in range(3)]
                    new = old - LEARN_RATE * (first + second)
                    width = LANES if j < SUB - 1 else TAIL
                    fresh[t % 2, pl.ds(pl.multiple_of(g * TILE, TILE), TILE), j * LANES:j * LANES + width] = new[:, :width]

            put(t).start()

        put(TURNS - 2).wait()
        put(TURNS - 1).wait()

    follow(SCATTER_PLAN, {'X': update, 'E': late_ends, 'N': first_pieces, 'O': other_pieces, 'A': turn_corner, 'F': finish,
                          'L': late_stage, 'M': late_corner})

    @pl.loop(0, half // STEP)
    def _(g):
        rows = block_of(g)
        out[rows, :] = r2x[3, rows, :]
        out[block_of(g, half), :] = r2y[3, rows, :]

    late_x2().wait_recv()
    late_y2().wait_recv()

    @pl.loop(0, small // STEP)
    def _(g):
        rows = block_of(g)
        out[block_of(g, 2 * half), :] = ly1[x, rows, :] + lx2[rows, :]
        out[block_of(g, 2 * half + small), :] = lx1[y, rows, :] + ly2[rows, :]

    for piece in (late_x1(), late_y1(), late_x2(), late_y2(), swap):
        piece.wait_send()

    for k in range(4):
        for h in range(2):
            x1(k, h).wait_send()
            y1(k, h).wait_send()
        x2(k).wait_send()
        y2(k).wait_send()
        if k < 3:
            p = planes[k]

            @pl.when(p > z)
            def _():
                late_up(p, lu.at[p - 1]).wait_send()

            @pl.when(p < z)
            def _():
                late_down(p, ld.at[p]).wait_send()

            for c, total in ((0, r2x.at[k]), (1, r2y.at[k])):
                @pl.when(p > z)
                def _():
                    up(c, k, total).wait_send()

                @pl.when(p < z)
                def _():
                    down(c, k, total).wait_send()


def scatter_slots(parts, tables, own_grad, other_grad, width):
    rows = parts.shape[0] // 16
    dma = pltpu.SemaphoreType.DMA
    half, small = shares(rows)
    f32 = jnp.float32
    return pl.pallas_call(
        scatter_kernel,
        out_shape=(jax.ShapeDtypeStruct((rows, LANES), f32),
                   jax.ShapeDtypeStruct((own_grad.shape[0] // SUB, width), f32),
                   jax.ShapeDtypeStruct(own_grad.shape, f32)),
        in_specs=[pl.BlockSpec(memory_space=ANY)] * 4,
        out_specs=(pl.BlockSpec(memory_space=pltpu.VMEM), *[pl.BlockSpec(memory_space=ANY)] * 2),
        scratch_shapes=[pltpu.VMEM((3, 2, COLS * SUB, LANES), f32), pltpu.VMEM((2, COLS, width), f32),
                        dma((3, 2)), dma((2,)), dma, dma, *[pltpu.VMEM((4, 2, half, LANES), f32)] * 2, *[pltpu.VMEM((4, half, LANES), f32)] * 2,
                        *[pltpu.VMEM((2, 3, half, LANES), f32)] * 2, pltpu.VMEM((4, half, LANES), f32),
                        *[pltpu.VMEM((3, 2, 2, 2 * small, LANES), f32)] * 2,
                        pltpu.VMEM((2, 2, 2 * small, LANES), f32),
                        *[pltpu.VMEM((small, LANES), f32), pltpu.VMEM((2, small, LANES), f32)] * 2,
                        *[dma((3, 2, 4))] * 2, *[dma((3, 4))] * 4,
                        *[dma((4,))] * 3, dma],
        compiler_params=pltpu.CompilerParams(collective_id=2, has_side_effects=True,
                                             vmem_limit_bytes=63 * 1024 * 1024),
        name='scatter_slots')(parts.reshape(4, 2, 2, rows, LANES), tables, own_grad, other_grad)[:2]


def trade(a):
    return lax.all_to_all(a, 'ep', 0, 0)


def solution(mesh):
    group = mesh.shape['ep']

    def device_step(table_in, table_out, centers, contexts, negatives):
        rows_dev, width = table_in.shape
        n_pairs, n_neg = negatives.shape
        n_ref = n_pairs * (n_neg + 1)
        me = lax.axis_index('ep')
        ids = jnp.arange(group, dtype=jnp.int32)
        partner = [(d, d + 1 - 2 * (d % 2)) for d in range(group)]
        other_out = lax.ppermute(table_out, 'ep', partner)

        all_centers = trade(jnp.broadcast_to(centers[None], (group, n_pairs))).reshape(-1)
        all_owner = all_centers % group
        counts = jnp.sum((all_owner.reshape(group, n_pairs)[:, None, :] == ids[None, :, None]).astype(jnp.int32), axis=2)
        totals = jnp.sum(counts, axis=0)
        before = jnp.sum(jnp.where(ids[:, None] < me, counts, 0), axis=0)
        owner_c = centers % group
        one_hot = (owner_c[:, None] == ids[None, :])
        tri = (jnp.arange(n_pairs)[:, None] > jnp.arange(n_pairs)[None, :]).astype(jnp.bfloat16)
        earlier = jnp.dot(tri, one_hot.astype(jnp.bfloat16), preferred_element_type=jnp.float32).astype(jnp.int32)
        rank = jnp.sum(jnp.where(one_hot, earlier + before[None, :], 0), axis=1)
        place = jnp.arange(group * n_pairs, dtype=jnp.int32)
        big = jnp.int32(2 ** 31 - 1)
        mine = jnp.where(all_owner == me, place * rows_dev + all_centers // group, big)
        rows4 = (lax.sort(mine, is_stable=False)[:SLOTS] % rows_dev) * SUB
        u_mine = pick_rows(rows4, table_in)

        words = jnp.concatenate([contexts[:, None], negatives], axis=1)
        owner_o = words % group
        core_u = (owner_c % 2)[:, None]
        row_o = words // group + (owner_o + core_u) % 2 * rows_dev
        is_ctx = (jnp.arange(n_neg + 1) == 0).astype(jnp.int32)[None, :]
        block = (owner_c // 2)[:, None] * 2 + is_ctx
        code = (block * SLOTS + rank[:, None]) * (2 * rows_dev) + row_o
        fits = rank < SLOTS
        dest = jnp.where(fits[:, None], owner_o // 2 * 2 + core_u, group)
        dest_count = jnp.sum((dest.reshape(1, n_ref) == ids[:, None]).astype(jnp.int32), axis=1)
        roomy = jnp.max(dest_count) <= ROOM
        fits = fits & roomy
        dest = jnp.where(roomy, dest, group)
        dest_count = jnp.where(roomy, dest_count, 0)
        spare_dest = jnp.where(jnp.arange(ROOM)[None, :] < ROOM - dest_count[:, None], ids[:, None], group)
        keys = jnp.concatenate([dest.reshape(n_ref), spare_dest.reshape(group * ROOM)])
        vals = jnp.concatenate([code.reshape(n_ref), jnp.full((group * ROOM,), big)])
        _, vals = lax.sort((keys, vals), num_keys=1, is_stable=False)
        got = trade(vals[:group * ROOM].reshape(group, ROOM))
        refs = lax.sort(got.reshape(group * ROOM), is_stable=False)
        edges = jnp.arange(group + 1, dtype=jnp.int32) * (SLOTS * rows_dev * 2)
        bounds = jnp.sum((refs[None, :] < edges[:, None]).astype(jnp.int32), axis=1)
        pad = jnp.zeros((BATCH,), jnp.int32)
        row4s = jnp.concatenate([refs % (2 * rows_dev) * SUB, pad])
        slot4s = jnp.concatenate([refs // (2 * rows_dev) % SLOTS * SUB, pad])

        u_all, tables = gather_slots(u_mine, table_out.T, other_out.T)
        own_grad, other_grad, gu, loss = score_rows(bounds, row4s, slot4s, tables, u_all)
        gu_mine, new_out = scatter_slots(gu, tables, own_grad, other_grad, width)
        new_in = add_rows(rows4, table_in, gu_mine)
        loss = jnp.sum(loss[:, 0])
        overflow = jnp.sum((~fits).astype(jnp.int32))
        both = jnp.where(jnp.arange(LANES) == 0, loss, overflow.astype(jnp.float32))
        sums = jnp.sum(trade(jnp.broadcast_to(both[None], (group, LANES))), axis=0)

        def more(state):
            return state[0] < jnp.where(sums[1] > 0.5, n_pairs // LEFT, 0)

        def again(state):
            turn, acc_in, acc_out, acc_loss = state

            def cut(a):
                return lax.all_gather(lax.dynamic_slice_in_dim(a, turn * LEFT, LEFT), 'ep', axis=0, tiled=True)

            word = jnp.concatenate([cut(centers)[:, None], cut(words)], axis=1)
            left = cut((~fits).astype(jnp.int32))[:, None] == 1
            held = word % group == me
            row = word // group
            parts = row[:, 1:, None] * SUB + jnp.arange(SUB)
            o_rows = tables[parts].reshape(row.shape[0], n_neg + 1, SUB * LANES)[:, :, :width]
            found = jnp.concatenate([table_in[row[:, :1]], o_rows], axis=1)
            found = lax.psum(jnp.where(held[:, :, None], found, 0.0), 'ep')
            u_vec, o_vec = found[:, 0], found[:, 1:]
            sign = jnp.where(is_ctx == 1, -1.0, 1.0)
            signed = sign * jnp.sum(u_vec[:, None, :] * o_vec, axis=-1)
            part = jnp.sum(jnp.where(left & (me == 0), -jax.nn.log_sigmoid(-signed), 0.0))
            gain = jnp.where(left, sign * jax.nn.sigmoid(signed), 0.0)
            goal = jnp.where(held & left, row, rows_dev)
            grad_u = jnp.sum(gain[:, :, None] * o_vec, axis=1)
            grad_o = gain[:, :, None] * u_vec[:, None, :]
            acc_in = acc_in.at[goal[:, 0]].add(-LEARN_RATE * grad_u, mode='drop')
            acc_out = acc_out.at[goal[:, 1:].reshape(-1)].add(-LEARN_RATE * grad_o.reshape(-1, width), mode='drop')
            return turn + 1, acc_in, acc_out, acc_loss + lax.psum(part, 'ep')

        _, new_in, new_out, total = lax.while_loop(more, again, (jnp.int32(0), new_in, new_out, sums[0]))
        return total / (n_pairs * group), new_in, new_out

    return jax.shard_map(device_step, mesh=mesh,
                         in_specs=(P('ep', None), P('ep', None), P('ep'), P('ep'), P('ep', None)),
                         out_specs=(P(), P('ep', None), P('ep', None)), check_vma=False)
```

```python
import functools

import jax
import jax.numpy as jnp
from jax import lax
from jax.experimental import pallas as pl
from jax.experimental.pallas import tpu as pltpu
from jax.sharding import PartitionSpec as P

LEARN_RATE = 0.5
LANES = 128
TILE = 8
SUB = 4
TAIL = 500 - 3 * LANES
CHUNK = 512
SLOTS = 1248
BATCH = 64
UNROLL = 16
STEP = 64
COLS = 256
TURNS = 4
UP, DOWN, LATE = range(3)
GATHER_PLAN = 'Z0P0Q0I0X0R0Z1J0P1X1Z2G0P2Q2X2Q1R2Z3P3G1X3X4Q3G2R1R3X5X6X7G3'
SCATTER_PLAN = 'O0N0N2E0A0E1N3N1L0X0O1L2X1F0E2L1A1A2F1X2O2L3X3O3A3F2M0F3'
ROOM = 768
LEFT = 32
ANY = pl.ANY
MESH = pl.DeviceIdType.MESH


def load_table(table, wide, stage, sems):
    rows = table.shape[0]
    n_chunks = rows // CHUNK

    def copy(k):
        return pltpu.make_async_copy(table.at[pl.ds(k * CHUNK, CHUNK)], stage.at[k % 2], sems.at[k % 2])

    copy(0).start()
    for k in range(n_chunks):
        if k + 1 < n_chunks:
            copy(k + 1).start()
        copy(k).wait()
        buf = stage.at[k % 2]

        @pl.loop(0, CHUNK // (TILE * SUB))
        def _(g):
            for i in range(SUB):
                r8 = pl.multiple_of((g * SUB + i) * TILE, TILE)
                w8 = pl.multiple_of((k * CHUNK + (g * SUB + i) * TILE) * SUB, (TILE * SUB))
                for j in range(SUB):
                    if j < SUB - 1:
                        wide[pl.ds(w8 + j, TILE, stride=SUB), :] = buf[pl.ds(r8, TILE), j * LANES:(j + 1) * LANES]
                    else:
                        wide[pl.ds(w8 + j, TILE, stride=SUB), :] = jnp.concatenate(
                            [buf[pl.ds(r8, TILE), j * LANES:j * LANES + TAIL], jnp.zeros((TILE, LANES - TAIL), jnp.float32)],
                            axis=1)


def store_table(out, stage, sems, value):
    rows = out.shape[0]
    n_chunks = rows // CHUNK

    def copy(k):
        return pltpu.make_async_copy(stage.at[k % 2], out.at[pl.ds(k * CHUNK, CHUNK)], sems.at[k % 2])

    for k in range(n_chunks):
        if k >= 2:
            copy(k - 2).wait()
        buf = stage.at[k % 2]

        @pl.loop(0, CHUNK // (TILE * SUB))
        def _(g):
            for i in range(SUB):
                r8 = pl.multiple_of((g * SUB + i) * TILE, TILE)
                w8 = pl.multiple_of((k * CHUNK + (g * SUB + i) * TILE) * SUB, (TILE * SUB))
                for j in range(SUB):
                    piece = value(w8, j)
                    if j < SUB - 1:
                        buf[pl.ds(r8, TILE), j * LANES:(j + 1) * LANES] = piece
                    else:
                        buf[pl.ds(r8, TILE), j * LANES:j * LANES + TAIL] = piece[:, :TAIL]

        copy(k).start()
    copy(n_chunks - 2).wait()
    copy(n_chunks - 1).wait()


def pick_kernel(rows4, table, out, wide, stage, sems):
    load_table(table, wide, stage, sems)

    @pl.loop(0, SLOTS // UNROLL)
    def _(g):
        for i in range(UNROLL):
            k = g * UNROLL + i
            r4 = pl.multiple_of(rows4[k], SUB)
            out[pl.ds(pl.multiple_of(k * SUB, SUB), SUB), :] = wide[pl.ds(r4, SUB), :]


def pick_rows(rows4, table):
    return pl.pallas_call(
        pick_kernel,
        out_shape=jax.ShapeDtypeStruct((SLOTS * SUB, LANES), jnp.float32),
        grid_spec=pltpu.PrefetchScalarGridSpec(
            num_scalar_prefetch=1, grid=(1,),
            in_specs=[pl.BlockSpec(memory_space=ANY)],
            out_specs=pl.BlockSpec((SLOTS * SUB, LANES), lambda i, *_: (0, 0)),
            scratch_shapes=[pltpu.VMEM((table.shape[0] * SUB, LANES), jnp.float32),
                            pltpu.VMEM((2, CHUNK, table.shape[1]), jnp.float32),
                            pltpu.SemaphoreType.DMA((2,))]),
        name='pick_rows')(rows4, table)


def add_kernel(rows4, table, grads, out, wide, stage, sems):
    load_table(table, wide, stage, sems)

    @pl.loop(0, SLOTS // UNROLL)
    def _(g):
        for i in range(UNROLL):
            k = g * UNROLL + i
            r4 = pl.multiple_of(rows4[k], SUB)
            wide[pl.ds(r4, SUB), :] = wide[pl.ds(r4, SUB), :] - LEARN_RATE * grads[pl.ds(pl.multiple_of(k * SUB, SUB), SUB), :]

    store_table(out, stage, sems, lambda w8, j: wide[pl.ds(w8 + j, 8, stride=SUB), :])


def add_rows(rows4, table, grads):
    return pl.pallas_call(
        add_kernel,
        out_shape=jax.ShapeDtypeStruct(table.shape, jnp.float32),
        grid_spec=pltpu.PrefetchScalarGridSpec(
            num_scalar_prefetch=1, grid=(1,),
            in_specs=[pl.BlockSpec(memory_space=ANY),
                      pl.BlockSpec((SLOTS * SUB, LANES), lambda i, *_: (0, 0))],
            out_specs=pl.BlockSpec(memory_space=ANY),
            scratch_shapes=[pltpu.VMEM((table.shape[0] * SUB, LANES), jnp.float32),
                            pltpu.VMEM((2, CHUNK, table.shape[1]), jnp.float32),
                            pltpu.SemaphoreType.DMA((2,))]),
        name='add_rows')(rows4, table, grads)


def score_kernel(bounds, row4s, slot4s, tables, u_blk, own_grad, other_grad, gu_blk, loss_blk,
                 wide, grad, sems, prods, coef):
    step = pl.program_id(0)

    @pl.when(step == 0)
    def _():
        whole = pltpu.make_async_copy(tables, wide, sems.at[0])
        whole.start()
        loss_blk[...] = jnp.zeros_like(loss_blk)

        @pl.loop(0, grad.shape[0] // COLS)
        def _(g):
            grad[pl.ds(pl.multiple_of(g * COLS, COLS), COLS), :] = jnp.zeros((COLS, LANES), jnp.float32)

        whole.wait()

    @pl.loop(0, SLOTS * SUB // 128)
    def _(g):
        gu_blk[pl.ds(pl.multiple_of(g * 128, 128), 128), :] = jnp.zeros((128, LANES), jnp.float32)

    begin, middle, end = bounds[2 * step], bounds[2 * step + 1], bounds[2 * step + 2]

    def spots(k):
        return pl.ds(pl.multiple_of(row4s[k], SUB), SUB), pl.ds(pl.multiple_of(slot4s[k], SUB), SUB)

    @pl.loop(0, (end - begin + BATCH - 1) // BATCH)
    def _(b):
        base = begin + b * BATCH

        @pl.loop(0, BATCH // UNROLL)
        def _(g):
            for i in range(UNROLL):
                k = g * UNROLL + i
                row, slot = spots(base + k)
                prods[pl.ds(pl.multiple_of(k * SUB, SUB), SUB), :] = u_blk[slot, :] * wide[row, :]

        part = prods[pl.ds(0, BATCH, stride=SUB), :]
        for j in range(1, SUB):
            part = part + prods[pl.ds(j, BATCH, stride=SUB), :]
        total = jnp.sum(part, axis=1, keepdims=True)
        number = lax.broadcasted_iota(jnp.int32, (BATCH, LANES), 0)
        sign = jnp.where(number < end - base, jnp.where(number < middle - base, 1.0, -1.0), 0.0)
        signed = sign * total
        small = jnp.exp(-jnp.abs(signed))
        loss = jnp.maximum(signed, 0.0) + jnp.log1p(small)
        loss_blk[...] += jnp.sum((jnp.abs(sign) * loss).reshape(BATCH // 8, 8, LANES), axis=0)
        gain = sign * jnp.where(signed >= 0, 1.0, small) / (1.0 + small)
        for j in range(SUB):
            coef[pl.ds(j, BATCH, stride=SUB), :] = gain

        @pl.loop(0, BATCH // UNROLL)
        def _(g):
            for i in range(0, UNROLL, 2):
                k = g * UNROLL + i
                row_a, slot_a = spots(base + k)
                row_b, slot_b = spots(base + k + 1)
                c_a = coef[pl.ds(pl.multiple_of(k * SUB, SUB), SUB), :]
                c_b = coef[pl.ds(pl.multiple_of((k + 1) * SUB, SUB), SUB), :]
                gu_a, gu_b = c_a * wide[row_a, :], c_b * wide[row_b, :]
                go_a, go_b = c_a * u_blk[slot_a, :], c_b * u_blk[slot_b, :]
                gu_b = gu_b + jnp.where(slot4s[base + k] == slot4s[base + k + 1], gu_a, 0.0)
                go_b = go_b + jnp.where(row4s[base + k] == row4s[base + k + 1], go_a, 0.0)
                gu_a, gu_b = gu_a + gu_blk[slot_a, :], gu_b + gu_blk[slot_b, :]
                go_a, go_b = go_a + grad[row_a, :], go_b + grad[row_b, :]
                gu_blk[slot_a, :] = gu_a
                grad[row_a, :] = go_a
                gu_blk[slot_b, :] = gu_b
                grad[row_b, :] = go_b

    @pl.when(step == pl.num_programs(0) - 1)
    def _():
        half = own_grad.shape[0]
        first = pltpu.make_async_copy(grad.at[pl.ds(0, half)], own_grad, sems.at[0])
        second = pltpu.make_async_copy(grad.at[pl.ds(half, half)], other_grad, sems.at[1])
        first.start()
        second.start()
        first.wait()
        second.wait()


def score_rows(bounds, row4s, slot4s, tables, u_all):
    n_blocks = u_all.shape[0] // (SLOTS * SUB)
    blk = pl.BlockSpec((SLOTS * SUB, LANES), lambda i, *_: (i, 0))
    half = jax.ShapeDtypeStruct((tables.shape[0] // 2, LANES), jnp.float32)
    return pl.pallas_call(
        score_kernel,
        out_shape=(half, half, jax.ShapeDtypeStruct(u_all.shape, jnp.float32),
                   jax.ShapeDtypeStruct((8, LANES), jnp.float32)),
        grid_spec=pltpu.PrefetchScalarGridSpec(
            num_scalar_prefetch=3, grid=(n_blocks,),
            in_specs=[pl.BlockSpec(memory_space=ANY), blk],
            out_specs=(pl.BlockSpec(memory_space=ANY), pl.BlockSpec(memory_space=ANY), blk,
                       pl.BlockSpec((8, LANES), lambda i, *_: (0, 0))),
            scratch_shapes=[*[pltpu.VMEM(tables.shape, jnp.float32)] * 2, pltpu.SemaphoreType.DMA((2,)),
                            pltpu.VMEM((BATCH * SUB, LANES), jnp.float32),
                            pltpu.VMEM((BATCH * SUB, LANES), jnp.float32)]),
        compiler_params=pltpu.CompilerParams(vmem_limit_bytes=60 * 1024 * 1024),
        name='score_rows')(bounds, row4s, slot4s, tables, u_all)


def place_of():
    me = lax.axis_index('ep')
    x, y, z = (me // 2) % 2, (me // 4) % 2, me // 8
    return me, x, y, z, 1 - x, 1 - y, me + 2 - 4 * x, me + 4 - 8 * y, z > 0, z < 3


def follow(plan, steps):
    for name, plane in zip(plan[::2], plan[1::2]):
        steps[name](int(plane))


def block_of(g, base=0):
    return pl.ds(pl.multiple_of(base + g * STEP, STEP), STEP)


def pair(sends, recvs, k):
    at = k if isinstance(k, tuple) else (k,)
    return sends.at[at], recvs.at[at]


def partner_of(me):
    return me + 1 - 2 * (me % 2)


def plane_order(z):
    far = 3 * (1 - z // 2)
    near = 1 + z % 2
    return z, near, 6 - far - near - z, far


def meet_neighbours(me, x_peer, y_peer, below, above, partner=None):
    barrier = pltpu.get_barrier_semaphore()
    extra = int(partner is not None)
    if extra:
        pl.semaphore_signal(barrier, inc=1, device_id=(partner,), device_id_type=MESH)
    pl.semaphore_signal(barrier, inc=1, device_id=(x_peer,), device_id_type=MESH)
    pl.semaphore_signal(barrier, inc=1, device_id=(y_peer,), device_id_type=MESH)

    @pl.when(above)
    def _():
        pl.semaphore_signal(barrier, inc=1, device_id=(me + 8,), device_id_type=MESH)

    @pl.when(below)
    def _():
        pl.semaphore_signal(barrier, inc=1, device_id=(me - 8,), device_id_type=MESH)

    @pl.when(below & above)
    def _():
        pl.semaphore_wait(barrier, 4 + extra)

    @pl.when(~(below & above))
    def _():
        pl.semaphore_wait(barrier, 3 + extra)


def remote(src, dst, send, recv, peer):
    return pltpu.make_async_remote_copy(src_ref=src, dst_ref=dst, send_sem=send, recv_sem=recv,
                                        device_id=(peer,), device_id_type=MESH)


def shares(rows):
    small = rows * 4 // 39 // STEP * STEP
    return rows // 2 - small, small


def gather_kernel(mine, own_t, out, tables, other_t, cols, rows, in_sem, out_sem, swap_s, swap_r,
                  zs, zr, xs, xr, ys, yr, gs, gr, local_sem):
    me, x, y, z, far_x, far_y, x_peer, y_peer, below, above = place_of()
    big, small = shares(mine.shape[0])
    low, high, both = pl.ds(0, big), pl.ds(big, big), pl.ds(0, 2 * big)
    late = pl.ds(2 * big, 2 * small)
    late_x, late_y = pl.ds(2 * big, small), pl.ds(2 * big + small, small)
    planes = plane_order(z)

    def up(p, src):
        return remote(src.at[both], out.at[p, y, x, both], zs.at[UP, p], zr.at[UP, p], me + 8)

    def down(p, src):
        return remote(src.at[both], out.at[p, y, x, both], zs.at[DOWN, p], zr.at[DOWN, p], me - 8)

    def late_up(p):
        piece = out.at[p, :, :, late]
        return remote(piece, piece, zs.at[2, p], zr.at[2, p], me + 8)

    def late_down(p):
        piece = out.at[p, :, :, late]
        return remote(piece, piece, zs.at[3, p], zr.at[3, p], me - 8)

    def held(p):
        return out.at[p, y, x]

    def to_x(k, m, src, row, part):
        return remote(src, out.at[planes[k], row, x, part], xs.at[m, k], xr.at[m, k], x_peer)

    def to_y(k, m, src, col, part):
        return remote(src, out.at[planes[k], y, col, part], ys.at[m, k], yr.at[m, k], y_peer)

    def own_pieces(k):
        src = mine if k == 0 else held(planes[k])
        return (to_y(k, 0, src.at[low], x, low), to_x(k, 0, src.at[high], y, high),
                to_y(k, 1, src.at[high], x, high), to_x(k, 1, src.at[low], y, low))

    def second_x(k):
        return to_x(k, 2, out.at[planes[k], far_y, x, low], far_y, low)

    def second_y(k):
        return to_y(k, 2, out.at[planes[k], y, far_x, high], far_x, high)

    def from_x(k, m, row, part):
        spot = out.at[planes[k], row, far_x, part]
        return remote(spot, spot, xs.at[m, k], xr.at[m, k], x_peer)

    def from_y(k, m, col, part):
        spot = out.at[planes[k], far_y, col, part]
        return remote(spot, spot, ys.at[m, k], yr.at[m, k], y_peer)

    def late1_x():
        return remote(mine.at[late_x], out.at[z, y, x, late_x], *pair(gs, gr, 0), x_peer)

    def late1_y():
        return remote(mine.at[late_y], out.at[z, y, x, late_y], *pair(gs, gr, 1), y_peer)

    def late2_y():
        piece = out.at[z, y, :, late_x]
        return remote(piece, piece, *pair(gs, gr, 2), y_peer)

    def late2_x():
        piece = out.at[z, :, x, late_y]
        return remote(piece, piece, *pair(gs, gr, 3), x_peer)

    partner = partner_of(me)
    meet_neighbours(me, x_peer, y_peer, below, above, partner)
    swap = remote(own_t, other_t, swap_s, swap_r, partner)
    keep = pltpu.make_async_copy(mine, out.at[z, y, x], local_sem)
    keep.start()

    def late_out(k):
        late1_x().start()
        late1_y().start()
        swap.start()

    def late_on(k):
        keep.wait()
        late1_x().wait_recv()
        late2_y().start()
        late1_y().wait_recv()
        late2_x().start()

    def along_z(k):
        p = planes[k]
        src = mine if k == 0 else held(p)

        @pl.when(p <= z)
        def _():
            if k > 0:
                up(p, src).wait_recv()

            @pl.when(above)
            def _():
                up(p, src).start()

        @pl.when(p >= z)
        def _():
            if k > 0:
                down(p, src).wait_recv()

            @pl.when(below)
            def _():
                down(p, src).start()

    def early_pieces(k):
        for piece in own_pieces(k)[:2]:
            piece.start()

    def other_pieces(k):
        for piece in own_pieces(k)[2:]:
            piece.start()

    def relay(k):
        from_y(k, 0, x, low).wait_recv()
        second_x(k).start()
        from_x(k, 0, y, high).wait_recv()
        second_y(k).start()

    def late_along_z(k):
        p = planes[k]
        if k == 0:
            late2_y().wait_recv()
            late2_x().wait_recv()

        @pl.when(p <= z)
        def _():
            if k > 0:
                late_up(p).wait_recv()

            @pl.when(above)
            def _():
                late_up(p).start()

        @pl.when(p >= z)
        def _():
            if k > 0:
                late_down(p).wait_recv()

            @pl.when(below)
            def _():
                late_down(p).start()

    def convert(k):
        source, first = (own_t, k) if k < TURNS else (other_t, k - TURNS)
        if k == TURNS:
            swap.wait_recv()

        def fetch(t):
            at = pl.ds(pl.multiple_of((first * TURNS + t) * COLS, COLS), COLS)
            return pltpu.make_async_copy(source.at[:, at], cols.at[t % 2], in_sem.at[t % 2])

        def put(t):
            at = pl.ds(pl.multiple_of((k * TURNS + t) * COLS * SUB, COLS), COLS * SUB)
            return pltpu.make_async_copy(rows.at[t % 2], tables.at[at], out_sem.at[t % 2])

        fetch(0).start()

        @pl.loop(0, TURNS)
        def _(t):
            fetch(t).wait()

            @pl.when(t + 1 < TURNS)
            def _():
                fetch(t + 1).start()

            @pl.when(t > 1)
            def _():
                put(t - 2).wait()

            for h in range(COLS // LANES):
                for j in range(SUB):
                    width = LANES if j < SUB - 1 else TAIL
                    turned = cols[t % 2, j * LANES:j * LANES + width, h * LANES:(h + 1) * LANES].T
                    if width < LANES:
                        turned = jnp.concatenate([turned, jnp.zeros((LANES, LANES - width), jnp.float32)], axis=1)
                    rows[t % 2, pl.ds(h * LANES * SUB + j, LANES, stride=SUB), :] = turned
            put(t).start()

        put(TURNS - 2).wait()
        put(TURNS - 1).wait()

    follow(GATHER_PLAN, {'X': convert, 'I': late_out, 'J': late_on, 'Z': along_z, 'P': early_pieces, 'Q': other_pieces,
                         'R': relay, 'G': late_along_z})
    for piece in (late1_x(), late1_y(), late2_x(), late2_y(), swap):
        piece.wait_send()
    for k in range(4):
        from_y(k, 1, x, high).wait_recv()
        from_x(k, 1, y, low).wait_recv()
        from_x(k, 2, far_y, low).wait_recv()
        from_y(k, 2, far_x, high).wait_recv()
        for piece in own_pieces(k):
            piece.wait_send()
        second_x(k).wait_send()
        second_y(k).wait_send()
        p = planes[k]

        @pl.when((p <= z) & above)
        def _():
            up(p, held(p)).wait_send()
            late_up(p).wait_send()

        @pl.when((p >= z) & below)
        def _():
            down(p, held(p)).wait_send()
            late_down(p).wait_send()


def gather_slots(mine, own_t):
    rows = mine.shape[0]
    width, words = own_t.shape
    dma = pltpu.SemaphoreType.DMA
    out, tables, _ = pl.pallas_call(
        gather_kernel,
        out_shape=(jax.ShapeDtypeStruct((4, 2, 2, rows, LANES), jnp.float32),
                   jax.ShapeDtypeStruct((2 * words * SUB, LANES), jnp.float32),
                   jax.ShapeDtypeStruct(own_t.shape, jnp.float32)),
        in_specs=[pl.BlockSpec(memory_space=pltpu.VMEM), pl.BlockSpec(memory_space=ANY)],
        out_specs=(pl.BlockSpec(memory_space=ANY),) * 3,
        scratch_shapes=[pltpu.VMEM((2, width, COLS), jnp.float32), pltpu.VMEM((2, COLS * SUB, LANES), jnp.float32),
                        dma((2,)), dma((2,)), dma, dma, dma((4, 4)), dma((4, 4)), *[dma((3, 4))] * 4,
                        dma((4,)), dma((4,)), dma],
        compiler_params=pltpu.CompilerParams(collective_id=1, has_side_effects=True),
        name='gather_slots')(mine, own_t)
    return out.reshape(16 * rows, LANES), tables


def scatter_kernel(parts, tables, own_grad, other_grad, out, new_table, back, terms, fresh, term_sem, fresh_sem, swap_s, swap_r, r1x, r1y, r2x, r2y, zu, zd, stage, lu, ld, held, ly2, lx1, lx2, ly1,
                   zs, zr, xs, xr, ys, yr, gs, gr, stage_sem, held_sem):
    me, x, y, z, far_x, far_y, x_peer, y_peer, below, above = place_of()
    half, small = shares(out.shape[0])
    low, high = pl.ds(0, half), pl.ds(half, half)
    late = pl.ds(2 * half, 2 * small)
    late_a, late_b = pl.ds(0, small), pl.ds(small, small)
    planes = plane_order(z)[::-1]

    def x1(k, h):
        row = far_y if h == 0 else y
        return remote(parts.at[planes[k], row, far_x, low], r1x.at[k, h], xs.at[h, k], xr.at[h, k], x_peer)

    def y1(k, h):
        col = far_x if h == 0 else x
        return remote(parts.at[planes[k], far_y, col, high], r1y.at[k, h], ys.at[h, k], yr.at[h, k], y_peer)

    def x2(k):
        return remote(r1y.at[k, 0], r2y.at[k], *pair(xs, xr, (LATE, k)), x_peer)

    def y2(k):
        return remote(r1x.at[k, 0], r2x.at[k], *pair(ys, yr, (LATE, k)), y_peer)

    def load(k, i):
        p = planes[k]
        src = (parts.at[p, far_y, x, low], parts.at[p, y, x, low],
               parts.at[p, y, far_x, high], parts.at[p, y, x, high])[i]
        return pltpu.make_async_copy(src, stage.at[i], stage_sem.at[i])

    def add(dst, *others):
        @pl.loop(0, half // STEP)
        def _(g):
            rows = block_of(g)
            value = dst[rows, :]
            for other in others:
                value = value + other[rows, :]
            dst[rows, :] = value

    def up(c, k, src):
        p = planes[k]
        return remote(src, zu.at[c, p - 1], zs.at[c, UP, p], zr.at[c, UP, p], me + 8)

    def down(c, k, src):
        p = planes[k]
        return remote(src, zd.at[c, p], zs.at[c, DOWN, p], zr.at[c, DOWN, p], me - 8)

    def late_load(p):
        return pltpu.make_async_copy(parts.at[p, :, :, late], held, held_sem)

    def late_up(p, src):
        return remote(src, lu.at[p - 1], zs.at[LATE, UP, p], zr.at[LATE, UP, p], me + 8)

    def late_down(p, src):
        return remote(src, ld.at[p], zs.at[LATE, DOWN, p], zr.at[LATE, DOWN, p], me - 8)

    def late_add(dst, src):
        @pl.loop(0, 2 * small // STEP)
        def _(g):
            rows = block_of(g)
            for i in range(2):
                for j in range(2):
                    dst[i, j, rows, :] = dst[i, j, rows, :] + src[i, j, rows, :]

    def small_add(dst, src):
        @pl.loop(0, small // STEP)
        def _(g):
            rows = block_of(g)
            dst[rows, :] = dst[rows, :] + src[rows, :]

    def late_stage(k):
        p = planes[k]
        if k < 3:
            @pl.when(below & above)
            def _():
                late_load(p).start()

            @pl.when((p > z) & below)
            def _():
                late_up(p, lu.at[p - 1]).wait_recv()
                late_load(p).wait()
                late_add(lu.at[p - 1], held)
                late_up(p, lu.at[p - 1]).start()

            @pl.when((p < z) & above)
            def _():
                late_down(p, ld.at[p]).wait_recv()
                late_load(p).wait()
                late_add(ld.at[p], held)
                late_down(p, ld.at[p]).start()
        else:
            late_load(p).start()
            late_load(p).wait()

            @pl.when(below)
            def _():
                late_up(p, lu.at[p - 1]).wait_recv()
                late_add(held, lu.at[p - 1])

            @pl.when(above)
            def _():
                late_down(p, ld.at[p]).wait_recv()
                late_add(held, ld.at[p])

            late_y1().start()
            late_x1().start()

    def late_y1():
        return remote(held.at[far_y, :, late_a], ly1, *pair(gs, gr, 0), y_peer)

    def late_x1():
        return remote(held.at[:, far_x, late_b], lx1, *pair(gs, gr, 1), x_peer)

    def late_x2():
        return remote(ly1.at[far_x], lx2, *pair(gs, gr, 2), x_peer)

    def late_y2():
        return remote(lx1.at[far_y], ly2, *pair(gs, gr, 3), y_peer)

    partner = partner_of(me)
    meet_neighbours(me, x_peer, y_peer, below, above, partner)
    swap = remote(other_grad, back, swap_s, swap_r, partner)
    swap.start()
    for i in range(4):
        load(0, i).start()

    def settle(c, k, total, first, i):
        p = planes[k]
        load(k, i).wait()
        add(total, first, stage.at[i])
        if k < 3:
            load(k + 1, i).start()

        @pl.when((p >= z) & below)
        def _():
            up(c, k, total).wait_recv()
            add(total, zu.at[c, p - 1])

        @pl.when((p <= z) & above)
        def _():
            down(c, k, total).wait_recv()
            add(total, zd.at[c, p])

    def move(c, k, total):
        p = planes[k]

        @pl.when(p > z)
        def _():
            up(c, k, total).start()

        @pl.when(p < z)
        def _():
            down(c, k, total).start()

    def finish(k):
        x1(k, 1).wait_recv()
        y2(k).wait_recv()
        settle(0, k, r2x.at[k], r1x.at[k, 1], 1)
        if k < 3:
            move(0, k, r2x.at[k])
        y1(k, 1).wait_recv()
        x2(k).wait_recv()
        settle(1, k, r2y.at[k], r1y.at[k, 1], 3)
        if k < 3:
            move(1, k, r2y.at[k])

    def late_ends(k):
        p = planes[k]

        @pl.when(~below)
        def _():
            late_up(p, parts.at[p, :, :, late]).start()

        @pl.when(~above)
        def _():
            late_down(p, parts.at[p, :, :, late]).start()

    def first_pieces(k):
        x1(k, 0).start()
        y1(k, 0).start()

    def other_pieces(k):
        x1(k, 1).start()
        y1(k, 1).start()

    def turn_corner(k):
        x1(k, 0).wait_recv()
        load(k, 0).wait()
        add(r1x.at[k, 0], stage.at[0])
        y1(k, 0).wait_recv()
        load(k, 2).wait()
        add(r1y.at[k, 0], stage.at[2])
        if k < 3:
            load(k + 1, 0).start()
            load(k + 1, 2).start()
        y2(k).start()
        x2(k).start()

    def late_corner(k):
        late_y1().wait_recv()
        late_x1().wait_recv()
        for i in range(2):
            small_add(ly1.at[i], held.at[y, i, late_a])
            small_add(lx1.at[i], held.at[i, x, late_b])
        late_x2().start()
        late_y2().start()

    def update(k):
        if k == 0:
            swap.wait_recv()

        def fetch(t):
            at = pl.ds(pl.multiple_of((k * TURNS + t) * COLS * SUB, COLS), COLS * SUB)
            return [pltpu.make_async_copy(ref.at[at], terms.at[i, t % 2], term_sem.at[i, t % 2])
                    for i, ref in enumerate((tables, own_grad, back))]

        def put(t):
            at = pl.ds(pl.multiple_of((k * TURNS + t) * COLS, COLS), COLS)
            return pltpu.make_async_copy(fresh.at[t % 2], new_table.at[at], fresh_sem.at[t % 2])

        for copy in fetch(0):
            copy.start()

        @pl.loop(0, TURNS)
        def _(t):
            for copy in fetch(t):
                copy.wait()

            @pl.when(t + 1 < TURNS)
            def _():
                for copy in fetch(t + 1):
                    copy.start()

            @pl.when(t > 1)
            def _():
                put(t - 2).wait()

            @pl.loop(0, COLS // TILE)
            def _(g):
                for j in range(SUB):
                    at = pl.ds(pl.multiple_of(g * TILE * SUB, TILE) + j, TILE, stride=SUB)
                    old, first, second = [terms[i, t % 2, at, :] for i in range(3)]
                    new = old - LEARN_RATE * (first + second)
                    width = LANES if j < SUB - 1 else TAIL
                    fresh[t % 2, pl.ds(pl.multiple_of(g * TILE, TILE), TILE), j * LANES:j * LANES + width] = new[:, :width]

            put(t).start()

        put(TURNS - 2).wait()
        put(TURNS - 1).wait()

    follow(SCATTER_PLAN, {'X': update, 'E': late_ends, 'N': first_pieces, 'O': other_pieces, 'A': turn_corner, 'F': finish,
                          'L': late_stage, 'M': late_corner})

    @pl.loop(0, half // STEP)
    def _(g):
        rows = block_of(g)
        out[rows, :] = r2x[3, rows, :]
        out[block_of(g, half), :] = r2y[3, rows, :]

    late_x2().wait_recv()
    late_y2().wait_recv()

    @pl.loop(0, small // STEP)
    def _(g):
        rows = block_of(g)
        out[block_of(g, 2 * half), :] = ly1[x, rows, :] + lx2[rows, :]
        out[block_of(g, 2 * half + small), :] = lx1[y, rows, :] + ly2[rows, :]

    for piece in (late_x1(), late_y1(), late_x2(), late_y2(), swap):
        piece.wait_send()

    for k in range(4):
        for h in range(2):
            x1(k, h).wait_send()
            y1(k, h).wait_send()
        x2(k).wait_send()
        y2(k).wait_send()
        if k < 3:
            p = planes[k]

            @pl.when(p > z)
            def _():
                late_up(p, lu.at[p - 1]).wait_send()

            @pl.when(p < z)
            def _():
                late_down(p, ld.at[p]).wait_send()

            for c, total in ((0, r2x.at[k]), (1, r2y.at[k])):
                @pl.when(p > z)
                def _():
                    up(c, k, total).wait_send()

                @pl.when(p < z)
                def _():
                    down(c, k, total).wait_send()


def scatter_slots(parts, tables, own_grad, other_grad, width):
    rows = parts.shape[0] // 16
    dma = pltpu.SemaphoreType.DMA
    half, small = shares(rows)
    f32 = jnp.float32
    return pl.pallas_call(
        scatter_kernel,
        out_shape=(jax.ShapeDtypeStruct((rows, LANES), f32),
                   jax.ShapeDtypeStruct((own_grad.shape[0] // SUB, width), f32),
                   jax.ShapeDtypeStruct(own_grad.shape, f32)),
        in_specs=[pl.BlockSpec(memory_space=ANY)] * 4,
        out_specs=(pl.BlockSpec(memory_space=pltpu.VMEM), *[pl.BlockSpec(memory_space=ANY)] * 2),
        scratch_shapes=[pltpu.VMEM((3, 2, COLS * SUB, LANES), f32), pltpu.VMEM((2, COLS, width), f32),
                        dma((3, 2)), dma((2,)), dma, dma, *[pltpu.VMEM((4, 2, half, LANES), f32)] * 2, *[pltpu.VMEM((4, half, LANES), f32)] * 2,
                        *[pltpu.VMEM((2, 3, half, LANES), f32)] * 2, pltpu.VMEM((4, half, LANES), f32),
                        *[pltpu.VMEM((3, 2, 2, 2 * small, LANES), f32)] * 2,
                        pltpu.VMEM((2, 2, 2 * small, LANES), f32),
                        *[pltpu.VMEM((small, LANES), f32), pltpu.VMEM((2, small, LANES), f32)] * 2,
                        *[dma((3, 2, 4))] * 2, *[dma((3, 4))] * 4,
                        *[dma((4,))] * 3, dma],
        compiler_params=pltpu.CompilerParams(collective_id=2, has_side_effects=True,
                                             vmem_limit_bytes=63 * 1024 * 1024),
        name='scatter_slots')(parts.reshape(4, 2, 2, rows, LANES), tables, own_grad, other_grad)[:2]


def trade(a):
    return lax.all_to_all(a, 'ep', 0, 0)


def solution(mesh):
    group = mesh.shape['ep']

    def device_step(table_in, table_out, centers, contexts, negatives):
        rows_dev, width = table_in.shape
        n_pairs, n_neg = negatives.shape
        n_ref = n_pairs * (n_neg + 1)
        me = lax.axis_index('ep')
        ids = jnp.arange(group, dtype=jnp.int32)

        all_centers = trade(jnp.broadcast_to(centers[None], (group, n_pairs))).reshape(-1)
        all_owner = all_centers % group
        counts = jnp.sum((all_owner.reshape(group, n_pairs)[:, None, :] == ids[None, :, None]).astype(jnp.int32), axis=2)
        totals = jnp.sum(counts, axis=0)
        before = jnp.sum(jnp.where(ids[:, None] < me, counts, 0), axis=0)
        owner_c = centers % group
        one_hot = (owner_c[:, None] == ids[None, :])
        tri = (jnp.arange(n_pairs)[:, None] > jnp.arange(n_pairs)[None, :]).astype(jnp.bfloat16)
        earlier = jnp.dot(tri, one_hot.astype(jnp.bfloat16), preferred_element_type=jnp.float32).astype(jnp.int32)
        rank = jnp.sum(jnp.where(one_hot, earlier + before[None, :], 0), axis=1)
        place = jnp.arange(group * n_pairs, dtype=jnp.int32)
        big = jnp.int32(2 ** 31 - 1)
        mine = jnp.where(all_owner == me, place * rows_dev + all_centers // group, big)
        rows4 = (lax.sort(mine, is_stable=False)[:SLOTS] % rows_dev) * SUB
        u_mine = pick_rows(rows4, table_in)

        words = jnp.concatenate([contexts[:, None], negatives], axis=1)
        owner_o = words % group
        core_u = (owner_c % 2)[:, None]
        row_o = words // group + (owner_o + core_u) % 2 * rows_dev
        is_ctx = (jnp.arange(n_neg + 1) == 0).astype(jnp.int32)[None, :]
        block = (owner_c // 2)[:, None] * 2 + is_ctx
        code = (block * SLOTS + rank[:, None]) * (2 * rows_dev) + row_o
        fits = rank < SLOTS
        dest = jnp.where(fits[:, None], owner_o // 2 * 2 + core_u, group)
        dest_count = jnp.sum((dest.reshape(1, n_ref) == ids[:, None]).astype(jnp.int32), axis=1)
        roomy = jnp.max(dest_count) <= ROOM
        fits = fits & roomy
        dest = jnp.where(roomy, dest, group)
        dest_count = jnp.where(roomy, dest_count, 0)
        spare_dest = jnp.where(jnp.arange(ROOM)[None, :] < ROOM - dest_count[:, None], ids[:, None], group)
        keys = jnp.concatenate([dest.reshape(n_ref), spare_dest.reshape(group * ROOM)])
        vals = jnp.concatenate([code.reshape(n_ref), jnp.full((group * ROOM,), big)])
        _, vals = lax.sort((keys, vals), num_keys=1, is_stable=False)
        got = trade(vals[:group * ROOM].reshape(group, ROOM))
        refs = lax.sort(got.reshape(group * ROOM), is_stable=False)
        edges = jnp.arange(group + 1, dtype=jnp.int32) * (SLOTS * rows_dev * 2)
        bounds = jnp.sum((refs[None, :] < edges[:, None]).astype(jnp.int32), axis=1)
        pad = jnp.zeros((BATCH,), jnp.int32)
        row4s = jnp.concatenate([refs % (2 * rows_dev) * SUB, pad])
        slot4s = jnp.concatenate([refs // (2 * rows_dev) % SLOTS * SUB, pad])

        u_all, tables = gather_slots(u_mine, table_out.T)
        own_grad, other_grad, gu, loss = score_rows(bounds, row4s, slot4s, tables, u_all)
        gu_mine, new_out = scatter_slots(gu, tables, own_grad, other_grad, width)
        new_in = add_rows(rows4, table_in, gu_mine)
        loss = jnp.sum(loss[:, 0])
        overflow = jnp.sum((~fits).astype(jnp.int32))
        both = jnp.where(jnp.arange(LANES) == 0, loss, overflow.astype(jnp.float32))
        sums = jnp.sum(trade(jnp.broadcast_to(both[None], (group, LANES))), axis=0)

        def more(state):
            return state[0] < jnp.where(sums[1] > 0.5, n_pairs // LEFT, 0)

        def again(state):
            turn, acc_in, acc_out, acc_loss = state

            def cut(a):
                return lax.all_gather(lax.dynamic_slice_in_dim(a, turn * LEFT, LEFT), 'ep', axis=0, tiled=True)

            word = jnp.concatenate([cut(centers)[:, None], cut(words)], axis=1)
            left = cut((~fits).astype(jnp.int32))[:, None] == 1
            held = word % group == me
            row = word // group
            parts = row[:, 1:, None] * SUB + jnp.arange(SUB)
            o_rows = tables[parts].reshape(row.shape[0], n_neg + 1, SUB * LANES)[:, :, :width]
            found = jnp.concatenate([table_in[row[:, :1]], o_rows], axis=1)
            found = lax.psum(jnp.where(held[:, :, None], found, 0.0), 'ep')
            u_vec, o_vec = found[:, 0], found[:, 1:]
            sign = jnp.where(is_ctx == 1, -1.0, 1.0)
            signed = sign * jnp.sum(u_vec[:, None, :] * o_vec, axis=-1)
            part = jnp.sum(jnp.where(left & (me == 0), -jax.nn.log_sigmoid(-signed), 0.0))
            gain = jnp.where(left, sign * jax.nn.sigmoid(signed), 0.0)
            goal = jnp.where(held & left, row, rows_dev)
            grad_u = jnp.sum(gain[:, :, None] * o_vec, axis=1)
            grad_o = gain[:, :, None] * u_vec[:, None, :]
            acc_in = acc_in.at[goal[:, 0]].add(-LEARN_RATE * grad_u, mode='drop')
            acc_out = acc_out.at[goal[:, 1:].reshape(-1)].add(-LEARN_RATE * grad_o.reshape(-1, width), mode='drop')
            return turn + 1, acc_in, acc_out, acc_loss + lax.psum(part, 'ep')

        _, new_in, new_out, total = lax.while_loop(more, again, (jnp.int32(0), new_in, new_out, sums[0]))
        return total / (n_pairs * group), new_in, new_out

    return jax.shard_map(device_step, mesh=mesh,
                         in_specs=(P('ep', None), P('ep', None), P('ep'), P('ep'), P('ep', None)),
                         out_specs=(P(), P('ep', None), P('ep', None)), check_vma=False)
```

```python
import functools

import jax
import jax.numpy as jnp
from jax import lax
from jax.experimental import pallas as pl
from jax.experimental.pallas import tpu as pltpu
from jax.sharding import PartitionSpec as P

LEARN_RATE = 0.5
LANES = 128
TILE = 8
SUB = 4
TAIL = 500 - 3 * LANES
CHUNK = 512
SLOTS = 1248
BATCH = 64
UNROLL = 16
STEP = 64
COLS = 256
TURNS = 4
UP, DOWN, LATE = range(3)
GATHER_PLAN = 'Z0P0Q0I0X0R0Z1J0P1X1Z2G0P2Q2X2Q1R2Z3P3G1X3X4Q3G2R1R3X5X6X7G3'
SCATTER_PLAN = 'O0N0N2E0A0E1N3N1L0X0O1L2X1F0E2L1A1A2F1X2O2L3X3O3A3F2M0F3'
ROOM = 768
LEFT = 32
ANY = pl.ANY
MESH = pl.DeviceIdType.MESH


def load_table(table, wide, stage, sems):
    rows = table.shape[0]
    n_chunks = rows // CHUNK

    def copy(k):
        return pltpu.make_async_copy(table.at[pl.ds(k * CHUNK, CHUNK)], stage.at[k % 2], sems.at[k % 2])

    copy(0).start()
    for k in range(n_chunks):
        if k + 1 < n_chunks:
            copy(k + 1).start()
        copy(k).wait()
        buf = stage.at[k % 2]

        @pl.loop(0, CHUNK // (TILE * SUB))
        def _(g):
            for i in range(SUB):
                r8 = pl.multiple_of((g * SUB + i) * TILE, TILE)
                w8 = pl.multiple_of((k * CHUNK + (g * SUB + i) * TILE) * SUB, (TILE * SUB))
                for j in range(SUB):
                    if j < SUB - 1:
                        wide[pl.ds(w8 + j, TILE, stride=SUB), :] = buf[pl.ds(r8, TILE), j * LANES:(j + 1) * LANES]
                    else:
                        wide[pl.ds(w8 + j, TILE, stride=SUB), :] = jnp.concatenate(
                            [buf[pl.ds(r8, TILE), j * LANES:j * LANES + TAIL], jnp.zeros((TILE, LANES - TAIL), jnp.float32)],
                            axis=1)


def store_table(out, stage, sems, value):
    rows = out.shape[0]
    n_chunks = rows // CHUNK

    def copy(k):
        return pltpu.make_async_copy(stage.at[k % 2], out.at[pl.ds(k * CHUNK, CHUNK)], sems.at[k % 2])

    for k in range(n_chunks):
        if k >= 2:
            copy(k - 2).wait()
        buf = stage.at[k % 2]

        @pl.loop(0, CHUNK // (TILE * SUB))
        def _(g):
            for i in range(SUB):
                r8 = pl.multiple_of((g * SUB + i) * TILE, TILE)
                w8 = pl.multiple_of((k * CHUNK + (g * SUB + i) * TILE) * SUB, (TILE * SUB))
                for j in range(SUB):
                    piece = value(w8, j)
                    if j < SUB - 1:
                        buf[pl.ds(r8, TILE), j * LANES:(j + 1) * LANES] = piece
                    else:
                        buf[pl.ds(r8, TILE), j * LANES:j * LANES + TAIL] = piece[:, :TAIL]

        copy(k).start()
    copy(n_chunks - 2).wait()
    copy(n_chunks - 1).wait()


def pick_kernel(rows4, table, out, wide, stage, sems):
    load_table(table, wide, stage, sems)

    @pl.loop(0, SLOTS // UNROLL)
    def _(g):
        for i in range(UNROLL):
            k = g * UNROLL + i
            r4 = pl.multiple_of(rows4[k], SUB)
            out[pl.ds(pl.multiple_of(k * SUB, SUB), SUB), :] = wide[pl.ds(r4, SUB), :]


def pick_rows(rows4, table):
    return pl.pallas_call(
        pick_kernel,
        out_shape=jax.ShapeDtypeStruct((SLOTS * SUB, LANES), jnp.float32),
        grid_spec=pltpu.PrefetchScalarGridSpec(
            num_scalar_prefetch=1, grid=(1,),
            in_specs=[pl.BlockSpec(memory_space=ANY)],
            out_specs=pl.BlockSpec((SLOTS * SUB, LANES), lambda i, *_: (0, 0)),
            scratch_shapes=[pltpu.VMEM((table.shape[0] * SUB, LANES), jnp.float32),
                            pltpu.VMEM((2, CHUNK, table.shape[1]), jnp.float32),
                            pltpu.SemaphoreType.DMA((2,))]),
        name='pick_rows')(rows4, table)


def add_kernel(rows4, table, grads, out, wide, stage, sems):
    load_table(table, wide, stage, sems)

    @pl.loop(0, SLOTS // UNROLL)
    def _(g):
        for i in range(UNROLL):
            k = g * UNROLL + i
            r4 = pl.multiple_of(rows4[k], SUB)
            wide[pl.ds(r4, SUB), :] = wide[pl.ds(r4, SUB), :] - LEARN_RATE * grads[pl.ds(pl.multiple_of(k * SUB, SUB), SUB), :]

    store_table(out, stage, sems, lambda w8, j: wide[pl.ds(w8 + j, 8, stride=SUB), :])


def add_rows(rows4, table, grads):
    return pl.pallas_call(
        add_kernel,
        out_shape=jax.ShapeDtypeStruct(table.shape, jnp.float32),
        grid_spec=pltpu.PrefetchScalarGridSpec(
            num_scalar_prefetch=1, grid=(1,),
            in_specs=[pl.BlockSpec(memory_space=ANY),
                      pl.BlockSpec((SLOTS * SUB, LANES), lambda i, *_: (0, 0))],
            out_specs=pl.BlockSpec(memory_space=ANY),
            scratch_shapes=[pltpu.VMEM((table.shape[0] * SUB, LANES), jnp.float32),
                            pltpu.VMEM((2, CHUNK, table.shape[1]), jnp.float32),
                            pltpu.SemaphoreType.DMA((2,))]),
        name='add_rows')(rows4, table, grads)


def score_kernel(bounds, row4s, slot4s, tables, u_blk, own_grad, other_grad, gu_blk, loss_blk,
                 wide, grad, sems, prods, coef):
    step = pl.program_id(0)

    @pl.when(step == 0)
    def _():
        whole = pltpu.make_async_copy(tables, wide, sems.at[0])
        whole.start()
        loss_blk[...] = jnp.zeros_like(loss_blk)

        @pl.loop(0, grad.shape[0] // COLS)
        def _(g):
            grad[pl.ds(pl.multiple_of(g * COLS, COLS), COLS), :] = jnp.zeros((COLS, LANES), jnp.float32)

        whole.wait()

    @pl.loop(0, SLOTS * SUB // 128)
    def _(g):
        gu_blk[pl.ds(pl.multiple_of(g * 128, 128), 128), :] = jnp.zeros((128, LANES), jnp.float32)

    begin, middle, end = bounds[2 * step], bounds[2 * step + 1], bounds[2 * step + 2]

    def spots(k):
        return pl.ds(pl.multiple_of(row4s[k], SUB), SUB), pl.ds(pl.multiple_of(slot4s[k], SUB), SUB)

    @pl.loop(0, (end - begin + BATCH - 1) // BATCH)
    def _(b):
        base = begin + b * BATCH

        @pl.loop(0, BATCH // UNROLL)
        def _(g):
            for i in range(UNROLL):
                k = g * UNROLL + i
                row, slot = spots(base + k)
                prods[pl.ds(pl.multiple_of(k * SUB, SUB), SUB), :] = u_blk[slot, :] * wide[row, :]

        part = prods[pl.ds(0, BATCH, stride=SUB), :]
        for j in range(1, SUB):
            part = part + prods[pl.ds(j, BATCH, stride=SUB), :]
        total = jnp.sum(part, axis=1, keepdims=True)
        number = lax.broadcasted_iota(jnp.int32, (BATCH, LANES), 0)
        sign = jnp.where(number < end - base, jnp.where(number < middle - base, 1.0, -1.0), 0.0)
        signed = sign * total
        small = jnp.exp(-jnp.abs(signed))
        loss = jnp.maximum(signed, 0.0) + jnp.log1p(small)
        loss_blk[...] += jnp.sum((jnp.abs(sign) * loss).reshape(BATCH // 8, 8, LANES), axis=0)
        gain = sign * jnp.where(signed >= 0, 1.0, small) / (1.0 + small)
        for j in range(SUB):
            coef[pl.ds(j, BATCH, stride=SUB), :] = gain

        @pl.loop(0, BATCH // UNROLL)
        def _(g):
            for i in range(0, UNROLL, 2):
                k = g * UNROLL + i
                row_a, slot_a = spots(base + k)
                row_b, slot_b = spots(base + k + 1)
                c_a = coef[pl.ds(pl.multiple_of(k * SUB, SUB), SUB), :]
                c_b = coef[pl.ds(pl.multiple_of((k + 1) * SUB, SUB), SUB), :]
                gu_a, gu_b = c_a * wide[row_a, :], c_b * wide[row_b, :]
                go_a, go_b = c_a * u_blk[slot_a, :], c_b * u_blk[slot_b, :]
                gu_b = gu_b + jnp.where(slot4s[base + k] == slot4s[base + k + 1], gu_a, 0.0)
                go_b = go_b + jnp.where(row4s[base + k] == row4s[base + k + 1], go_a, 0.0)
                gu_a, gu_b = gu_a + gu_blk[slot_a, :], gu_b + gu_blk[slot_b, :]
                go_a, go_b = go_a + grad[row_a, :], go_b + grad[row_b, :]
                gu_blk[slot_a, :] = gu_a
                grad[row_a, :] = go_a
                gu_blk[slot_b, :] = gu_b
                grad[row_b, :] = go_b

    @pl.when(step == pl.num_programs(0) - 1)
    def _():
        half = own_grad.shape[0]
        first = pltpu.make_async_copy(grad.at[pl.ds(0, half)], own_grad, sems.at[0])
        second = pltpu.make_async_copy(grad.at[pl.ds(half, half)], other_grad, sems.at[1])
        first.start()
        second.start()
        first.wait()
        second.wait()


def score_rows(bounds, row4s, slot4s, tables, u_all):
    n_blocks = u_all.shape[0] // (SLOTS * SUB)
    blk = pl.BlockSpec((SLOTS * SUB, LANES), lambda i, *_: (i, 0))
    half = jax.ShapeDtypeStruct((tables.shape[0] // 2, LANES), jnp.float32)
    return pl.pallas_call(
        score_kernel,
        out_shape=(half, half, jax.ShapeDtypeStruct(u_all.shape, jnp.float32),
                   jax.ShapeDtypeStruct((8, LANES), jnp.float32)),
        grid_spec=pltpu.PrefetchScalarGridSpec(
            num_scalar_prefetch=3, grid=(n_blocks,),
            in_specs=[pl.BlockSpec(memory_space=ANY), blk],
            out_specs=(pl.BlockSpec(memory_space=ANY), pl.BlockSpec(memory_space=ANY), blk,
                       pl.BlockSpec((8, LANES), lambda i, *_: (0, 0))),
            scratch_shapes=[*[pltpu.VMEM(tables.shape, jnp.float32)] * 2, pltpu.SemaphoreType.DMA((2,)),
                            pltpu.VMEM((BATCH * SUB, LANES), jnp.float32),
                            pltpu.VMEM((BATCH * SUB, LANES), jnp.float32)]),
        compiler_params=pltpu.CompilerParams(vmem_limit_bytes=60 * 1024 * 1024),
        name='score_rows')(bounds, row4s, slot4s, tables, u_all)


def place_of():
    me = lax.axis_index('ep')
    x, y, z = (me // 2) % 2, (me // 4) % 2, me // 8
    return me, x, y, z, 1 - x, 1 - y, me + 2 - 4 * x, me + 4 - 8 * y, z > 0, z < 3


def follow(plan, steps):
    for name, plane in zip(plan[::2], plan[1::2]):
        steps[name](int(plane))


def block_of(g, base=0):
    return pl.ds(pl.multiple_of(base + g * STEP, STEP), STEP)


def pair(sends, recvs, k):
    at = k if isinstance(k, tuple) else (k,)
    return sends.at[at], recvs.at[at]


def partner_of(me):
    return me + 1 - 2 * (me % 2)


def plane_order(z):
    far = 3 * (1 - z // 2)
    near = 1 + z % 2
    return z, near, 6 - far - near - z, far


def meet_neighbours(me, x_peer, y_peer, below, above, partner=None):
    barrier = pltpu.get_barrier_semaphore()
    extra = int(partner is not None)
    if extra:
        pl.semaphore_signal(barrier, inc=1, device_id=(partner,), device_id_type=MESH)
    pl.semaphore_signal(barrier, inc=1, device_id=(x_peer,), device_id_type=MESH)
    pl.semaphore_signal(barrier, inc=1, device_id=(y_peer,), device_id_type=MESH)

    @pl.when(above)
    def _():
        pl.semaphore_signal(barrier, inc=1, device_id=(me + 8,), device_id_type=MESH)

    @pl.when(below)
    def _():
        pl.semaphore_signal(barrier, inc=1, device_id=(me - 8,), device_id_type=MESH)

    @pl.when(below & above)
    def _():
        pl.semaphore_wait(barrier, 4 + extra)

    @pl.when(~(below & above))
    def _():
        pl.semaphore_wait(barrier, 3 + extra)


def remote(src, dst, send, recv, peer):
    return pltpu.make_async_remote_copy(src_ref=src, dst_ref=dst, send_sem=send, recv_sem=recv,
                                        device_id=(peer,), device_id_type=MESH)


def shares(rows):
    small = rows * 4 // 39 // STEP * STEP
    return rows // 2 - small, small


def gather_kernel(mine, own_t, out, tables, other_t, cols, rows, in_sem, out_sem, swap_s, swap_r,
                  zs, zr, xs, xr, ys, yr, gs, gr, local_sem):
    me, x, y, z, far_x, far_y, x_peer, y_peer, below, above = place_of()
    big, small = shares(mine.shape[0])
    low, high, both = pl.ds(0, big), pl.ds(big, big), pl.ds(0, 2 * big)
    late = pl.ds(2 * big, 2 * small)
    late_x, late_y = pl.ds(2 * big, small), pl.ds(2 * big + small, small)
    planes = plane_order(z)

    def up(p, src):
        return remote(src.at[both], out.at[p, y, x, both], zs.at[UP, p], zr.at[UP, p], me + 8)

    def down(p, src):
        return remote(src.at[both], out.at[p, y, x, both], zs.at[DOWN, p], zr.at[DOWN, p], me - 8)

    def late_up(p):
        piece = out.at[p, :, :, late]
        return remote(piece, piece, zs.at[2, p], zr.at[2, p], me + 8)

    def late_down(p):
        piece = out.at[p, :, :, late]
        return remote(piece, piece, zs.at[3, p], zr.at[3, p], me - 8)

    def held(p):
        return out.at[p, y, x]

    def to_x(k, m, src, row, part):
        return remote(src, out.at[planes[k], row, x, part], xs.at[m, k], xr.at[m, k], x_peer)

    def to_y(k, m, src, col, part):
        return remote(src, out.at[planes[k], y, col, part], ys.at[m, k], yr.at[m, k], y_peer)

    def own_pieces(k):
        src = mine if k == 0 else held(planes[k])
        return (to_y(k, 0, src.at[low], x, low), to_x(k, 0, src.at[high], y, high),
                to_y(k, 1, src.at[high], x, high), to_x(k, 1, src.at[low], y, low))

    def second_x(k):
        return to_x(k, 2, out.at[planes[k], far_y, x, low], far_y, low)

    def second_y(k):
        return to_y(k, 2, out.at[planes[k], y, far_x, high], far_x, high)

    def from_x(k, m, row, part):
        spot = out.at[planes[k], row, far_x, part]
        return remote(spot, spot, xs.at[m, k], xr.at[m, k], x_peer)

    def from_y(k, m, col, part):
        spot = out.at[planes[k], far_y, col, part]
        return remote(spot, spot, ys.at[m, k], yr.at[m, k], y_peer)

    def late1_x():
        return remote(mine.at[late_x], out.at[z, y, x, late_x], *pair(gs, gr, 0), x_peer)

    def late1_y():
        return remote(mine.at[late_y], out.at[z, y, x, late_y], *pair(gs, gr, 1), y_peer)

    def late2_y():
        piece = out.at[z, y, :, late_x]
        return remote(piece, piece, *pair(gs, gr, 2), y_peer)

    def late2_x():
        piece = out.at[z, :, x, late_y]
        return remote(piece, piece, *pair(gs, gr, 3), x_peer)

    partner = partner_of(me)
    meet_neighbours(me, x_peer, y_peer, below, above, partner)
    swap = remote(own_t, other_t, swap_s, swap_r, partner)
    keep = pltpu.make_async_copy(mine, out.at[z, y, x], local_sem)
    keep.start()

    def late_out(k):
        late1_x().start()
        late1_y().start()

    def late_on(k):
        keep.wait()
        late1_x().wait_recv()
        late2_y().start()
        late1_y().wait_recv()
        late2_x().start()

    def along_z(k):
        p = planes[k]
        src = mine if k == 0 else held(p)

        @pl.when(p <= z)
        def _():
            if k > 0:
                up(p, src).wait_recv()

            @pl.when(above)
            def _():
                up(p, src).start()

        @pl.when(p >= z)
        def _():
            if k > 0:
                down(p, src).wait_recv()

            @pl.when(below)
            def _():
                down(p, src).start()

    def early_pieces(k):
        for piece in own_pieces(k)[:2]:
            piece.start()

    def other_pieces(k):
        for piece in own_pieces(k)[2:]:
            piece.start()

    def relay(k):
        from_y(k, 0, x, low).wait_recv()
        second_x(k).start()
        from_x(k, 0, y, high).wait_recv()
        second_y(k).start()

    def late_along_z(k):
        p = planes[k]
        if k == 0:
            late2_y().wait_recv()
            late2_x().wait_recv()

        @pl.when(p <= z)
        def _():
            if k > 0:
                late_up(p).wait_recv()

            @pl.when(above)
            def _():
                late_up(p).start()

        @pl.when(p >= z)
        def _():
            if k > 0:
                late_down(p).wait_recv()

            @pl.when(below)
            def _():
                late_down(p).start()

    def convert(k):
        source, first = (own_t, k) if k < TURNS else (other_t, k - TURNS)
        if k == 1:
            swap.start()
        if k == TURNS:
            swap.wait_recv()

        def fetch(t):
            at = pl.ds(pl.multiple_of((first * TURNS + t) * COLS, COLS), COLS)
            return pltpu.make_async_copy(source.at[:, at], cols.at[t % 2], in_sem.at[t % 2])

        def put(t):
            at = pl.ds(pl.multiple_of((k * TURNS + t) * COLS * SUB, COLS), COLS * SUB)
            return pltpu.make_async_copy(rows.at[t % 2], tables.at[at], out_sem.at[t % 2])

        fetch(0).start()

        @pl.loop(0, TURNS)
        def _(t):
            fetch(t).wait()

            @pl.when(t + 1 < TURNS)
            def _():
                fetch(t + 1).start()

            @pl.when(t > 1)
            def _():
                put(t - 2).wait()

            for h in range(COLS // LANES):
                for j in range(SUB):
                    width = LANES if j < SUB - 1 else TAIL
                    turned = cols[t % 2, j * LANES:j * LANES + width, h * LANES:(h + 1) * LANES].T
                    if width < LANES:
                        turned = jnp.concatenate([turned, jnp.zeros((LANES, LANES - width), jnp.float32)], axis=1)
                    rows[t % 2, pl.ds(h * LANES * SUB + j, LANES, stride=SUB), :] = turned
            put(t).start()

        put(TURNS - 2).wait()
        put(TURNS - 1).wait()

    follow(GATHER_PLAN, {'X': convert, 'I': late_out, 'J': late_on, 'Z': along_z, 'P': early_pieces, 'Q': other_pieces,
                         'R': relay, 'G': late_along_z})
    for piece in (late1_x(), late1_y(), late2_x(), late2_y(), swap):
        piece.wait_send()
    for k in range(4):
        from_y(k, 1, x, high).wait_recv()
        from_x(k, 1, y, low).wait_recv()
        from_x(k, 2, far_y, low).wait_recv()
        from_y(k, 2, far_x, high).wait_recv()
        for piece in own_pieces(k):
            piece.wait_send()
        second_x(k).wait_send()
        second_y(k).wait_send()
        p = planes[k]

        @pl.when((p <= z) & above)
        def _():
            up(p, held(p)).wait_send()
            late_up(p).wait_send()

        @pl.when((p >= z) & below)
        def _():
            down(p, held(p)).wait_send()
            late_down(p).wait_send()


def gather_slots(mine, own_t):
    rows = mine.shape[0]
    width, words = own_t.shape
    dma = pltpu.SemaphoreType.DMA
    out, tables, _ = pl.pallas_call(
        gather_kernel,
        out_shape=(jax.ShapeDtypeStruct((4, 2, 2, rows, LANES), jnp.float32),
                   jax.ShapeDtypeStruct((2 * words * SUB, LANES), jnp.float32),
                   jax.ShapeDtypeStruct(own_t.shape, jnp.float32)),
        in_specs=[pl.BlockSpec(memory_space=pltpu.VMEM), pl.BlockSpec(memory_space=ANY)],
        out_specs=(pl.BlockSpec(memory_space=ANY),) * 3,
        scratch_shapes=[pltpu.VMEM((2, width, COLS), jnp.float32), pltpu.VMEM((2, COLS * SUB, LANES), jnp.float32),
                        dma((2,)), dma((2,)), dma, dma, dma((4, 4)), dma((4, 4)), *[dma((3, 4))] * 4,
                        dma((4,)), dma((4,)), dma],
        compiler_params=pltpu.CompilerParams(collective_id=1, has_side_effects=True),
        name='gather_slots')(mine, own_t)
    return out.reshape(16 * rows, LANES), tables


def scatter_kernel(parts, tables, own_grad, other_grad, out, new_table, back, terms, fresh, term_sem, fresh_sem, swap_s, swap_r, r1x, r1y, r2x, r2y, zu, zd, stage, lu, ld, held, ly2, lx1, lx2, ly1,
                   zs, zr, xs, xr, ys, yr, gs, gr, stage_sem, held_sem):
    me, x, y, z, far_x, far_y, x_peer, y_peer, below, above = place_of()
    half, small = shares(out.shape[0])
    low, high = pl.ds(0, half), pl.ds(half, half)
    late = pl.ds(2 * half, 2 * small)
    late_a, late_b = pl.ds(0, small), pl.ds(small, small)
    planes = plane_order(z)[::-1]

    def x1(k, h):
        row = far_y if h == 0 else y
        return remote(parts.at[planes[k], row, far_x, low], r1x.at[k, h], xs.at[h, k], xr.at[h, k], x_peer)

    def y1(k, h):
        col = far_x if h == 0 else x
        return remote(parts.at[planes[k], far_y, col, high], r1y.at[k, h], ys.at[h, k], yr.at[h, k], y_peer)

    def x2(k):
        return remote(r1y.at[k, 0], r2y.at[k], *pair(xs, xr, (LATE, k)), x_peer)

    def y2(k):
        return remote(r1x.at[k, 0], r2x.at[k], *pair(ys, yr, (LATE, k)), y_peer)

    def load(k, i):
        p = planes[k]
        src = (parts.at[p, far_y, x, low], parts.at[p, y, x, low],
               parts.at[p, y, far_x, high], parts.at[p, y, x, high])[i]
        return pltpu.make_async_copy(src, stage.at[i], stage_sem.at[i])

    def add(dst, *others):
        @pl.loop(0, half // STEP)
        def _(g):
            rows = block_of(g)
            value = dst[rows, :]
            for other in others:
                value = value + other[rows, :]
            dst[rows, :] = value

    def up(c, k, src):
        p = planes[k]
        return remote(src, zu.at[c, p - 1], zs.at[c, UP, p], zr.at[c, UP, p], me + 8)

    def down(c, k, src):
        p = planes[k]
        return remote(src, zd.at[c, p], zs.at[c, DOWN, p], zr.at[c, DOWN, p], me - 8)

    def late_load(p):
        return pltpu.make_async_copy(parts.at[p, :, :, late], held, held_sem)

    def late_up(p, src):
        return remote(src, lu.at[p - 1], zs.at[LATE, UP, p], zr.at[LATE, UP, p], me + 8)

    def late_down(p, src):
        return remote(src, ld.at[p], zs.at[LATE, DOWN, p], zr.at[LATE, DOWN, p], me - 8)

    def late_add(dst, src):
        @pl.loop(0, 2 * small // STEP)
        def _(g):
            rows = block_of(g)
            for i in range(2):
                for j in range(2):
                    dst[i, j, rows, :] = dst[i, j, rows, :] + src[i, j, rows, :]

    def small_add(dst, src):
        @pl.loop(0, small // STEP)
        def _(g):
            rows = block_of(g)
            dst[rows, :] = dst[rows, :] + src[rows, :]

    def late_stage(k):
        p = planes[k]
        if k < 3:
            @pl.when(below & above)
            def _():
                late_load(p).start()

            @pl.when((p > z) & below)
            def _():
                late_up(p, lu.at[p - 1]).wait_recv()
                late_load(p).wait()
                late_add(lu.at[p - 1], held)
                late_up(p, lu.at[p - 1]).start()

            @pl.when((p < z) & above)
            def _():
                late_down(p, ld.at[p]).wait_recv()
                late_load(p).wait()
                late_add(ld.at[p], held)
                late_down(p, ld.at[p]).start()
        else:
            late_load(p).start()
            late_load(p).wait()

            @pl.when(below)
            def _():
                late_up(p, lu.at[p - 1]).wait_recv()
                late_add(held, lu.at[p - 1])

            @pl.when(above)
            def _():
                late_down(p, ld.at[p]).wait_recv()
                late_add(held, ld.at[p])

            late_y1().start()
            late_x1().start()

    def late_y1():
        return remote(held.at[far_y, :, late_a], ly1, *pair(gs, gr, 0), y_peer)

    def late_x1():
        return remote(held.at[:, far_x, late_b], lx1, *pair(gs, gr, 1), x_peer)

    def late_x2():
        return remote(ly1.at[far_x], lx2, *pair(gs, gr, 2), x_peer)

    def late_y2():
        return remote(lx1.at[far_y], ly2, *pair(gs, gr, 3), y_peer)

    partner = partner_of(me)
    meet_neighbours(me, x_peer, y_peer, below, above, partner)
    swap = remote(other_grad, back, swap_s, swap_r, partner)
    swap.start()
    for i in range(4):
        load(0, i).start()

    def settle(c, k, total, first, i):
        p = planes[k]
        load(k, i).wait()
        add(total, first, stage.at[i])
        if k < 3:
            load(k + 1, i).start()

        @pl.when((p >= z) & below)
        def _():
            up(c, k, total).wait_recv()
            add(total, zu.at[c, p - 1])

        @pl.when((p <= z) & above)
        def _():
            down(c, k, total).wait_recv()
            add(total, zd.at[c, p])

    def move(c, k, total):
        p = planes[k]

        @pl.when(p > z)
        def _():
            up(c, k, total).start()

        @pl.when(p < z)
        def _():
            down(c, k, total).start()

    def finish(k):
        x1(k, 1).wait_recv()
        y2(k).wait_recv()
        settle(0, k, r2x.at[k], r1x.at[k, 1], 1)
        if k < 3:
            move(0, k, r2x.at[k])
        y1(k, 1).wait_recv()
        x2(k).wait_recv()
        settle(1, k, r2y.at[k], r1y.at[k, 1], 3)
        if k < 3:
            move(1, k, r2y.at[k])

    def late_ends(k):
        p = planes[k]

        @pl.when(~below)
        def _():
            late_up(p, parts.at[p, :, :, late]).start()

        @pl.when(~above)
        def _():
            late_down(p, parts.at[p, :, :, late]).start()

    def first_pieces(k):
        x1(k, 0).start()
        y1(k, 0).start()

    def other_pieces(k):
        x1(k, 1).start()
        y1(k, 1).start()

    def turn_corner(k):
        x1(k, 0).wait_recv()
        load(k, 0).wait()
        add(r1x.at[k, 0], stage.at[0])
        y1(k, 0).wait_recv()
        load(k, 2).wait()
        add(r1y.at[k, 0], stage.at[2])
        if k < 3:
            load(k + 1, 0).start()
            load(k + 1, 2).start()
        y2(k).start()
        x2(k).start()

    def late_corner(k):
        late_y1().wait_recv()
        late_x1().wait_recv()
        for i in range(2):
            small_add(ly1.at[i], held.at[y, i, late_a])
            small_add(lx1.at[i], held.at[i, x, late_b])
        late_x2().start()
        late_y2().start()

    def update(k):
        if k == 0:
            swap.wait_recv()

        def fetch(t):
            at = pl.ds(pl.multiple_of((k * TURNS + t) * COLS * SUB, COLS), COLS * SUB)
            return [pltpu.make_async_copy(ref.at[at], terms.at[i, t % 2], term_sem.at[i, t % 2])
                    for i, ref in enumerate((tables, own_grad, back))]

        def put(t):
            at = pl.ds(pl.multiple_of((k * TURNS + t) * COLS, COLS), COLS)
            return pltpu.make_async_copy(fresh.at[t % 2], new_table.at[at], fresh_sem.at[t % 2])

        for copy in fetch(0):
            copy.start()

        @pl.loop(0, TURNS)
        def _(t):
            for copy in fetch(t):
                copy.wait()

            @pl.when(t + 1 < TURNS)
            def _():
                for copy in fetch(t + 1):
                    copy.start()

            @pl.when(t > 1)
            def _():
                put(t - 2).wait()

            @pl.loop(0, COLS // TILE)
            def _(g):
                for j in range(SUB):
                    at = pl.ds(pl.multiple_of(g * TILE * SUB, TILE) + j, TILE, stride=SUB)
                    old, first, second = [terms[i, t % 2, at, :] for i in range(3)]
                    new = old - LEARN_RATE * (first + second)
                    width = LANES if j < SUB - 1 else TAIL
                    fresh[t % 2, pl.ds(pl.multiple_of(g * TILE, TILE), TILE), j * LANES:j * LANES + width] = new[:, :width]

            put(t).start()

        put(TURNS - 2).wait()
        put(TURNS - 1).wait()

    follow(SCATTER_PLAN, {'X': update, 'E': late_ends, 'N': first_pieces, 'O': other_pieces, 'A': turn_corner, 'F': finish,
                          'L': late_stage, 'M': late_corner})

    @pl.loop(0, half // STEP)
    def _(g):
        rows = block_of(g)
        out[rows, :] = r2x[3, rows, :]
        out[block_of(g, half), :] = r2y[3, rows, :]

    late_x2().wait_recv()
    late_y2().wait_recv()

    @pl.loop(0, small // STEP)
    def _(g):
        rows = block_of(g)
        out[block_of(g, 2 * half), :] = ly1[x, rows, :] + lx2[rows, :]
        out[block_of(g, 2 * half + small), :] = lx1[y, rows, :] + ly2[rows, :]

    for piece in (late_x1(), late_y1(), late_x2(), late_y2(), swap):
        piece.wait_send()

    for k in range(4):
        for h in range(2):
            x1(k, h).wait_send()
            y1(k, h).wait_send()
        x2(k).wait_send()
        y2(k).wait_send()
        if k < 3:
            p = planes[k]

            @pl.when(p > z)
            def _():
                late_up(p, lu.at[p - 1]).wait_send()

            @pl.when(p < z)
            def _():
                late_down(p, ld.at[p]).wait_send()

            for c, total in ((0, r2x.at[k]), (1, r2y.at[k])):
                @pl.when(p > z)
                def _():
                    up(c, k, total).wait_send()

                @pl.when(p < z)
                def _():
                    down(c, k, total).wait_send()


def scatter_slots(parts, tables, own_grad, other_grad, width):
    rows = parts.shape[0] // 16
    dma = pltpu.SemaphoreType.DMA
    half, small = shares(rows)
    f32 = jnp.float32
    return pl.pallas_call(
        scatter_kernel,
        out_shape=(jax.ShapeDtypeStruct((rows, LANES), f32),
                   jax.ShapeDtypeStruct((own_grad.shape[0] // SUB, width), f32),
                   jax.ShapeDtypeStruct(own_grad.shape, f32)),
        in_specs=[pl.BlockSpec(memory_space=ANY)] * 4,
        out_specs=(pl.BlockSpec(memory_space=pltpu.VMEM), *[pl.BlockSpec(memory_space=ANY)] * 2),
        scratch_shapes=[pltpu.VMEM((3, 2, COLS * SUB, LANES), f32), pltpu.VMEM((2, COLS, width), f32),
                        dma((3, 2)), dma((2,)), dma, dma, *[pltpu.VMEM((4, 2, half, LANES), f32)] * 2, *[pltpu.VMEM((4, half, LANES), f32)] * 2,
                        *[pltpu.VMEM((2, 3, half, LANES), f32)] * 2, pltpu.VMEM((4, half, LANES), f32),
                        *[pltpu.VMEM((3, 2, 2, 2 * small, LANES), f32)] * 2,
                        pltpu.VMEM((2, 2, 2 * small, LANES), f32),
                        *[pltpu.VMEM((small, LANES), f32), pltpu.VMEM((2, small, LANES), f32)] * 2,
                        *[dma((3, 2, 4))] * 2, *[dma((3, 4))] * 4,
                        *[dma((4,))] * 3, dma],
        compiler_params=pltpu.CompilerParams(collective_id=2, has_side_effects=True,
                                             vmem_limit_bytes=63 * 1024 * 1024),
        name='scatter_slots')(parts.reshape(4, 2, 2, rows, LANES), tables, own_grad, other_grad)[:2]


def trade(a):
    return lax.all_to_all(a, 'ep', 0, 0)


def solution(mesh):
    group = mesh.shape['ep']

    def device_step(table_in, table_out, centers, contexts, negatives):
        rows_dev, width = table_in.shape
        n_pairs, n_neg = negatives.shape
        n_ref = n_pairs * (n_neg + 1)
        me = lax.axis_index('ep')
        ids = jnp.arange(group, dtype=jnp.int32)

        all_centers = trade(jnp.broadcast_to(centers[None], (group, n_pairs))).reshape(-1)
        all_owner = all_centers % group
        counts = jnp.sum((all_owner.reshape(group, n_pairs)[:, None, :] == ids[None, :, None]).astype(jnp.int32), axis=2)
        totals = jnp.sum(counts, axis=0)
        before = jnp.sum(jnp.where(ids[:, None] < me, counts, 0), axis=0)
        owner_c = centers % group
        one_hot = (owner_c[:, None] == ids[None, :])
        tri = (jnp.arange(n_pairs)[:, None] > jnp.arange(n_pairs)[None, :]).astype(jnp.bfloat16)
        earlier = jnp.dot(tri, one_hot.astype(jnp.bfloat16), preferred_element_type=jnp.float32).astype(jnp.int32)
        rank = jnp.sum(jnp.where(one_hot, earlier + before[None, :], 0), axis=1)
        place = jnp.arange(group * n_pairs, dtype=jnp.int32)
        big = jnp.int32(2 ** 31 - 1)
        mine = jnp.where(all_owner == me, place * rows_dev + all_centers // group, big)
        rows4 = (lax.sort(mine, is_stable=False)[:SLOTS] % rows_dev) * SUB
        u_mine = pick_rows(rows4, table_in)

        words = jnp.concatenate([contexts[:, None], negatives], axis=1)
        owner_o = words % group
        core_u = (owner_c % 2)[:, None]
        row_o = words // group + (owner_o + core_u) % 2 * rows_dev
        is_ctx = (jnp.arange(n_neg + 1) == 0).astype(jnp.int32)[None, :]
        block = (owner_c // 2)[:, None] * 2 + is_ctx
        code = (block * SLOTS + rank[:, None]) * (2 * rows_dev) + row_o
        fits = rank < SLOTS
        dest = jnp.where(fits[:, None], owner_o // 2 * 2 + core_u, group)
        dest_count = jnp.sum((dest.reshape(1, n_ref) == ids[:, None]).astype(jnp.int32), axis=1)
        roomy = jnp.max(dest_count) <= ROOM
        fits = fits & roomy
        dest = jnp.where(roomy, dest, group)
        dest_count = jnp.where(roomy, dest_count, 0)
        spare_dest = jnp.where(jnp.arange(ROOM)[None, :] < ROOM - dest_count[:, None], ids[:, None], group)
        keys = jnp.concatenate([dest.reshape(n_ref), spare_dest.reshape(group * ROOM)])
        vals = jnp.concatenate([code.reshape(n_ref), jnp.full((group * ROOM,), big)])
        _, vals = lax.sort((keys, vals), num_keys=1, is_stable=False)
        got = trade(vals[:group * ROOM].reshape(group, ROOM))
        refs = lax.sort(got.reshape(group * ROOM), is_stable=False)
        edges = jnp.arange(group + 1, dtype=jnp.int32) * (SLOTS * rows_dev * 2)
        bounds = jnp.sum((refs[None, :] < edges[:, None]).astype(jnp.int32), axis=1)
        pad = jnp.zeros((BATCH,), jnp.int32)
        row4s = jnp.concatenate([refs % (2 * rows_dev) * SUB, pad])
        slot4s = jnp.concatenate([refs // (2 * rows_dev) % SLOTS * SUB, pad])

        u_all, tables = gather_slots(u_mine, table_out.T)
        own_grad, other_grad, gu, loss = score_rows(bounds, row4s, slot4s, tables, u_all)
        gu_mine, new_out = scatter_slots(gu, tables, own_grad, other_grad, width)
        new_in = add_rows(rows4, table_in, gu_mine)
        loss = jnp.sum(loss[:, 0])
        overflow = jnp.sum((~fits).astype(jnp.int32))
        both = jnp.where(jnp.arange(LANES) == 0, loss, overflow.astype(jnp.float32))
        sums = jnp.sum(trade(jnp.broadcast_to(both[None], (group, LANES))), axis=0)

        def more(state):
            return state[0] < jnp.where(sums[1] > 0.5, n_pairs // LEFT, 0)

        def again(state):
            turn, acc_in, acc_out, acc_loss = state

            def cut(a):
                return lax.all_gather(lax.dynamic_slice_in_dim(a, turn * LEFT, LEFT), 'ep', axis=0, tiled=True)

            word = jnp.concatenate([cut(centers)[:, None], cut(words)], axis=1)
            left = cut((~fits).astype(jnp.int32))[:, None] == 1
            held = word % group == me
            row = word // group
            parts = row[:, 1:, None] * SUB + jnp.arange(SUB)
            o_rows = tables[parts].reshape(row.shape[0], n_neg + 1, SUB * LANES)[:, :, :width]
            found = jnp.concatenate([table_in[row[:, :1]], o_rows], axis=1)
            found = lax.psum(jnp.where(held[:, :, None], found, 0.0), 'ep')
            u_vec, o_vec = found[:, 0], found[:, 1:]
            sign = jnp.where(is_ctx == 1, -1.0, 1.0)
            signed = sign * jnp.sum(u_vec[:, None, :] * o_vec, axis=-1)
            part = jnp.sum(jnp.where(left & (me == 0), -jax.nn.log_sigmoid(-signed), 0.0))
            gain = jnp.where(left, sign * jax.nn.sigmoid(signed), 0.0)
            goal = jnp.where(held & left, row, rows_dev)
            grad_u = jnp.sum(gain[:, :, None] * o_vec, axis=1)
            grad_o = gain[:, :, None] * u_vec[:, None, :]
            acc_in = acc_in.at[goal[:, 0]].add(-LEARN_RATE * grad_u, mode='drop')
            acc_out = acc_out.at[goal[:, 1:].reshape(-1)].add(-LEARN_RATE * grad_o.reshape(-1, width), mode='drop')
            return turn + 1, acc_in, acc_out, acc_loss + lax.psum(part, 'ep')

        _, new_in, new_out, total = lax.while_loop(more, again, (jnp.int32(0), new_in, new_out, sums[0]))
        return total / (n_pairs * group), new_in, new_out

    return jax.shard_map(device_step, mesh=mesh,
                         in_specs=(P('ep', None), P('ep', None), P('ep'), P('ep'), P('ep', None)),
                         out_specs=(P(), P('ep', None), P('ep', None)), check_vma=False)
```
